32 devices in a mesh: dp: 16 (over z, y, x), seq: 2 (over core).
Axes of the slice: x: 2, y: 2, z: 4, core: 2. Of those that a mesh axis runs over, the one named last changes fastest.
Arguments:
- content: bfloat16 [32, 512, 768], P('dp', 'seq'), may hold values from -6 to 6
- query_in: bfloat16 [32, 512, 768], P('dp', 'seq'), may hold values from -6 to 6
- content_cot: bfloat16 [32, 512, 768], P('dp', 'seq'), may hold values from -6 to 6
- query_cot: bfloat16 [32, 512, 768], P('dp', 'seq'), may hold values from -6 to 6
- lengths: int32 [32, 8], P('dp'), may hold values from 1 to 256, 512 in all within a row
- order: int32 [32, 512], P('dp'), may hold values from 0 to 511, each once within a row
- query_weight: bfloat16 [768, 768], P('dp'), may hold values from -0.21875 to 0.21875
- query_bias: bfloat16 [768], P('dp'), may hold values from -3 to 3
- key_weight: bfloat16 [768, 768], P('dp'), may hold values from -0.21875 to 0.21875
- value_weight: bfloat16 [768, 768], P('dp'), may hold values from -0.21875 to 0.21875
- value_bias: bfloat16 [768], P('dp'), may hold values from -3 to 3
- out_weight: bfloat16 [768, 768], P('dp'), may hold values from -0.875 to 0.875
- out_bias: bfloat16 [768], P('dp'), may hold values from -3 to 3
- mixer_gain: bfloat16 [768], P('dp'), may hold values from 0.5 to 1.5
- mixer_shift: bfloat16 [768], P('dp'), may hold values from -3 to 3
- up_weight: bfloat16 [768, 3072], P(None, 'dp'), may hold values from -0.21875 to 0.21875
- up_bias: bfloat16 [3072], P('dp'), may hold values from -3 to 3
- down_weight: bfloat16 [3072, 768], P('dp'), may hold values from -0.109375 to 0.109375
- down_bias: bfloat16 [768], P('dp'), may hold values from -3 to 3
- final_gain: bfloat16 [768], P('dp'), may hold values from 0.5 to 1.5
- final_shift: bfloat16 [768], P('dp'), may hold values from -3 to 3
- position_bias: bfloat16 [384], P('dp'), may hold values from -4 to 4
Outputs:
- content_out: bfloat16 [32, 512, 768], P('dp', 'seq')
- query_out: bfloat16 [32, 512, 768], P('dp', 'seq')
- content_grad: bfloat16 [32, 512, 768], P('dp', 'seq')
- query_grad: bfloat16 [32, 512, 768], P('dp', 'seq')
- query_weight_grad: float32 [768, 768], P('dp')
- query_bias_grad: float32 [768], P('dp')
- key_weight_grad: float32 [768, 768], P('dp')
- value_weight_grad: float32 [768, 768], P('dp')
- value_bias_grad: float32 [768], P('dp')
- out_weight_grad: float32 [768, 768], P('dp')
- out_bias_grad: float32 [768], P('dp')
- mixer_gain_grad: float32 [768], P('dp')
- mixer_shift_grad: float32 [768], P('dp')
- up_weight_grad: float32 [768, 3072], P(None, 'dp')
- up_bias_grad: float32 [3072], P('dp')
- down_weight_grad: float32 [3072, 768], P('dp')
- down_bias_grad: float32 [768], P('dp')
- final_gain_grad: float32 [768], P('dp')
- final_shift_grad: float32 [768], P('dp')
- position_bias_grad: float32 [384], P('dp')
The draws below stay inside these ranges and needn't reach their ends.
Inputs may be any that keep to these rules, and one draw needn't show every extreme that they name: Each row of order holds every position 0 to 511 once. Each row of lengths sums to 512, and its largest entry is 256.
All inputs are finite; a program needn't handle non-finite values.
Results may differ from the reference program's by a relative error of at most 0.013.
Values may be sent and summed in bfloat16 or wider, within the bound.
No kernel may reach another device: no remote copies, remote signals or barrier semaphores. Data moves between devices by JAX's collectives and lax.ppermute only.
A program may use at most 256 MiB of HBM per device.

```python
import math
import jax
import jax.numpy as jnp
import numpy as np
from jax import lax

D = 768
HEADS = 12
HEAD_DIM = 64
FF = 3072
BUCKETS = 32
L = 512
DOCS = 8
DOC_MOST = 256
ROWS = 32


def levels(stream_key, dims, shards, least, largest):
    def one(axis_at, parts):
        draws = jax.random.uniform(jax.random.fold_in(jax.random.fold_in(stream_key, 6), axis_at), (parts,), jnp.float32, least / len(shards), largest / len(shards))
        return jnp.repeat(jnp.exp(draws), dims[axis_at] // parts).reshape((-1,) + (1,) * (len(dims) - axis_at - 1))

    level = one(*shards[0])
    for cut in shards[1:]:
        level = level * one(*cut)
    return level


def split_up(count, total, most, lean):
    loads = [(1 << 20) // math.isqrt(grade ** lean) + 1 for grade in range(2, count + 1)]
    spare, holding = total - most - (count - 1), [1] * (count - 1)
    while spare > 0:
        movable = [i for i in range(count - 1) if holding[i] < most]
        mass, budget = sum([loads[i] for i in movable]), spare
        for i in movable:
            extra = min(most - holding[i], max(1, budget * loads[i] // mass), spare)
            holding[i] = holding[i] + extra
            spare = spare - extra
    return np.array([most] + holding)


def ragged(rng, number_of, total, most, skew):
    if number_of == 2:
        one = jax.random.randint(rng, (), max(1, total - most), min(most, total - 1) + 1)
        return jnp.stack([one, total - one])
    sizes = jnp.asarray(split_up(number_of, total, most, skew), jnp.int32)
    twos = (number_of - 1) // 2
    source_of, taker = sizes[1:1 + 2 * twos:2], sizes[2:2 + 2 * twos:2]
    room = jnp.minimum(source_of - 1, most - taker)
    shifted = jax.random.randint(jax.random.fold_in(rng, 1), (twos,), 0, 1 << 20) % (room + 1)
    sizes = sizes.at[1:1 + 2 * twos:2].set(source_of - shifted).at[2:2 + 2 * twos:2].set(taker + shifted)
    return sizes[jax.random.permutation(jax.random.fold_in(rng, 2), number_of)]


def scatter_about(key, shape, deviation, most, cuts=(), held_as=jnp.bfloat16):
    values = jax.random.normal(key, shape, jnp.float32) * deviation
    if len(cuts) > 0:
        values = levels(key, shape, cuts, -0.22, 0.18) * values
    return jnp.clip(values, min=-most, max=most).astype(held_as)


def setup_inputs(seed: int = 0) -> dict:
    key_of = jax.random.split(jax.random.key(seed), 23)
    content = scatter_about(key_of[0], (ROWS, L, D), 1.0, 6.0, ((0, 16), (1, 2)))
    query_in = scatter_about(key_of[1], (ROWS, L, D), 1.0, 6.0, ((0, 16), (1, 2)))
    content_cot = scatter_about(key_of[2], (ROWS, L, D), 1.0, 6.0, ((0, 16), (1, 2)))
    query_cot = scatter_about(key_of[3], (ROWS, L, D), 1.0, 6.0, ((0, 16), (1, 2)))
    lengths = jax.vmap(lambda own: ragged(own, DOCS, L, DOC_MOST, 2))(jax.random.split(key_of[4], ROWS)).reshape((ROWS, DOCS)).astype(jnp.int32)
    order = jax.vmap(lambda own: jax.random.permutation(own, L))(jax.random.split(key_of[5], ROWS)).reshape((ROWS, L)).astype(jnp.int32)
    query_weight = scatter_about(key_of[6], (D, D), D ** -0.5, 0.21875, ((0, 16),))
    query_bias = scatter_about(key_of[7], (D,), 0.5, 3.0, ((0, 16),))
    key_weight = scatter_about(key_of[8], (D, D), D ** -0.5, 0.21875, ((0, 16),))
    value_weight = scatter_about(key_of[9], (D, D), D ** -0.5, 0.21875, ((0, 16),))
    value_bias = scatter_about(key_of[10], (D,), 0.5, 3.0, ((0, 16),))
    out_weight = scatter_about(key_of[11], (D, D), (D // 16) ** -0.5, 0.875, ((0, 16),))
    out_bias = scatter_about(key_of[12], (D,), 0.5, 3.0, ((0, 16),))
    mixer_gain = jnp.clip(1.0 + 0.1 * jax.random.normal(key_of[13], (D,), jnp.float32), 0.5, 1.5).astype(jnp.bfloat16)
    mixer_shift = scatter_about(key_of[14], (D,), 0.5, 3.0, ((0, 16),))
    up_weight = scatter_about(key_of[15], (D, FF), D ** -0.5, 0.21875, ((1, 16),))
    up_bias = scatter_about(key_of[16], (FF,), 0.5, 3.0, ((0, 16),))
    down_weight = scatter_about(key_of[17], (FF, D), FF ** -0.5, 0.109375, ((0, 16),))
    down_bias = scatter_about(key_of[18], (D,), 0.5, 3.0, ((0, 16),))
    final_gain = jnp.clip(1.0 + 0.1 * jax.random.normal(key_of[19], (D,), jnp.float32), 0.5, 1.5).astype(jnp.bfloat16)
    final_shift = scatter_about(key_of[20], (D,), 0.5, 3.0, ((0, 16),))
    position_bias = scatter_about(key_of[21], (BUCKETS * HEADS,), 1.0, 4.0, ((0, 16),))
    return dict(content=content, query_in=query_in, content_cot=content_cot, query_cot=query_cot, lengths=lengths, order=order, query_weight=query_weight, query_bias=query_bias, key_weight=key_weight, value_weight=value_weight, value_bias=value_bias, out_weight=out_weight, out_bias=out_bias, mixer_gain=mixer_gain, mixer_shift=mixer_shift, up_weight=up_weight, up_bias=up_bias, down_weight=down_weight, down_bias=down_bias, final_gain=final_gain, final_shift=final_shift, position_bias=position_bias)


limits = (1, 2, 3, 4, 5, 6, 7, 8, 12, 16, 23, 32, 46, 64, 91)

@jax.custom_vjp
def low(v):
    return lax.optimization_barrier(v.astype(jnp.bfloat16)).astype(jnp.float32)

@jax.custom_vjp
def low_back(v):
    return v

def low_keep(v):
    return (low(v), None)

def low_pass(kept, grad):
    return (grad,)

def back_keep(v):
    return (v, None)

def back_low(kept, grad):
    return (low(grad),)
low.defvjp(low_keep, low_pass)
low_back.defvjp(back_keep, back_low)

def rounded(values):
    return low(low_back(values))

def matmul(left, right):
    return jnp.dot(left, right, precision=lax.Precision.HIGHEST)

def layer_norm(values, gain, shift):
    center = values - lax.optimization_barrier(jnp.mean(values, axis=-1, keepdims=True))
    spread = lax.optimization_barrier(jnp.mean(center * center, axis=-1, keepdims=True))
    return center * lax.rsqrt(spread + 1e-05) * gain + shift

def bucket_table(query_places, key_places):
    distance = key_places[None, :] - query_places[:, None]
    magnitude = jnp.abs(distance)
    counted = jnp.zeros(distance.shape, jnp.int32)
    for limit in limits:
        counted = counted + (magnitude >= limit).astype(jnp.int32)
    return counted + 16 * (distance > 0).astype(jnp.int32)

def row_forward(content, query_in, lengths_row, order_row, params):
    query_weight, query_bias, key_weight, value_weight, value_bias, out_weight, out_bias, mixer_gain, mixer_shift, up_weight, up_bias, down_weight, down_bias, final_gain, final_shift, position_bias = params
    bounds = jnp.cumsum(lengths_row)[:-1]
    segment = lax.optimization_barrier(jnp.sum((order_row[:, None] >= bounds[None, :]).astype(jnp.int32), axis=1))
    places = jnp.arange(L)
    same = segment[:, None] == segment[None, :]
    allowed_content = same & (places[None, :] <= places[:, None])
    allowed_query = same & (places[None, :] < places[:, None])
    bucket = bucket_table(order_row, order_row)
    table = position_bias.reshape(BUCKETS, HEADS)
    bias = jnp.transpose(table[bucket], (2, 0, 1))
    scale = 1.0 / math.sqrt(HEAD_DIM)
    keys = rounded(matmul(content, key_weight)).reshape(L, HEADS, HEAD_DIM)
    values = rounded(matmul(content, value_weight) + value_bias).reshape(L, HEADS, HEAD_DIM)

    def stream_out(stream, allowed):
        live = jnp.any(allowed, axis=-1).astype(jnp.float32)
        queries = rounded(matmul(stream, query_weight) + query_bias).reshape(L, HEADS, HEAD_DIM)
        scores = jnp.einsum('qhd,khd->hqk', queries, keys, precision=lax.Precision.HIGHEST) * scale + bias
        scores = jnp.where(allowed[None], low_back(scores), -1e+30)
        probs = jax.nn.softmax(scores, axis=-1) * live[None, :, None]
        mixed = jnp.einsum('hqk,khd->qhd', low(probs), values, precision=lax.Precision.HIGHEST)
        mixed = rounded(mixed.reshape(L, HEADS * HEAD_DIM))
        branch = low_back(matmul(mixed, out_weight) + out_bias)
        first = layer_norm(stream + branch, mixer_gain, mixer_shift)
        up = low_back(matmul(low(first), up_weight) + up_bias)
        act = low(jax.nn.gelu(up, approximate=False))
        down = low_back(matmul(act, down_weight) + down_bias)
        return layer_norm(first + down, final_gain, final_shift)
    return (stream_out(content, allowed_content), stream_out(query_in, allowed_query))

def reference(content, query_in, content_cot, query_cot, lengths, order, query_weight, query_bias, key_weight, value_weight, value_bias, out_weight, out_bias, mixer_gain, mixer_shift, up_weight, up_bias, down_weight, down_bias, final_gain, final_shift, position_bias):
    params = tuple((piece.astype(jnp.float32) for piece in (query_weight, query_bias, key_weight, value_weight, value_bias, out_weight, out_bias, mixer_gain, mixer_shift, up_weight, up_bias, down_weight, down_bias, final_gain, final_shift, position_bias)))
    checked = jax.checkpoint(row_forward)

    def forward(content_full, query_full, weights):

        def one(pieces):
            return checked(pieces[0], pieces[1], pieces[2], pieces[3], weights)
        return lax.map(one, (content_full, query_full, lengths, order))
    outputs, pullback = jax.vjp(forward, content.astype(jnp.float32), query_in.astype(jnp.float32), params)
    content_grad, query_grad, grads = pullback((content_cot.astype(jnp.float32), query_cot.astype(jnp.float32)))
    return (outputs[0].astype(jnp.bfloat16), outputs[1].astype(jnp.bfloat16), content_grad.astype(jnp.bfloat16), query_grad.astype(jnp.bfloat16), grads[0], grads[1], grads[2], grads[3], grads[4], grads[5], grads[6], grads[7], grads[8], grads[9], grads[10], grads[11], grads[12], grads[13], grads[14], grads[15])
```

```python
import functools
import math

import jax
import jax.numpy as jnp
from jax import lax
from jax.experimental import pallas as pl
from jax.experimental.pallas import tpu as pltpu
from jax.sharding import PartitionSpec as P

HEADS = 12
HEAD_DIM = 64
BUCKETS = 32
GROUP = 4
LANES = GROUP * HEAD_DIM
GROUPS = HEADS // GROUP
TILE = 128
NEG = -1e30
FLOOR = -1e29
EPS = 1e-05

limits = (1, 2, 3, 4, 5, 6, 7, 8, 12, 16, 23, 32, 46, 64, 91)

NN = (((1,), (0,)), ((), ()))
NT = (((1,), (1,)), ((), ()))
TN = (((0,), (0,)), ((), ()))
VMEM_SPEC = pl.BlockSpec(memory_space=pltpu.VMEM)
SMEM_SPEC = pl.BlockSpec(memory_space=pltpu.SMEM)
SDS = jax.ShapeDtypeStruct


def product(left, right, dims=NN):
    return lax.dot_general(left, right, dims, preferred_element_type=jnp.float32)


def params(semantics=None, limit=56):
    return pltpu.CompilerParams(dimension_semantics=semantics, vmem_limit_bytes=limit << 20)


def row_sum(values):
    return jnp.sum(values, axis=-1, keepdims=True)


def sort_kernel(bounds, content, query, ccot, qcot, order_row, order_col, pos_row, pos_col,
                xs_out, cs_out, mask_out):
    length = order_row.shape[1]
    down = lax.broadcasted_iota(jnp.int32, (length, length), 0)
    across = lax.broadcasted_iota(jnp.int32, (length, length), 1)
    forward = order_row[...] == down
    backward = order_col[...] == across
    rank_col = row_sum(jnp.where(forward, pos_row[...].astype(jnp.float32), 0.0))
    rank_row = jnp.sum(
        jnp.where(backward, pos_col[...].astype(jnp.float32), 0.0), axis=0, keepdims=True
    )
    place_col = lax.broadcasted_iota(jnp.int32, (length, 1), 0)
    place_row = lax.broadcasted_iota(jnp.int32, (1, length), 1)
    segment_col = jnp.zeros((length, 1), jnp.int32)
    segment_row = jnp.zeros((1, length), jnp.int32)
    for index in range(bounds.shape[0]):
        segment_col = segment_col + (place_col >= bounds[index]).astype(jnp.int32)
        segment_row = segment_row + (place_row >= bounds[index]).astype(jnp.int32)
    same = segment_col == segment_row
    mask_out[0] = jnp.where(same & (rank_row <= rank_col), 0.0, NEG)
    mask_out[1] = jnp.where(same & (rank_row < rank_col), 0.0, NEG)
    onehot = jnp.where(forward, 1.0, 0.0).astype(jnp.bfloat16)
    for source, target, at in (
        (content, xs_out, 0), (query, xs_out, 1), (ccot, cs_out, 0), (qcot, cs_out, 1),
    ):
        target[at * length : (at + 1) * length, :] = product(onehot, source[...]).astype(
            jnp.bfloat16
        )


def sort_rows(bounds, content, query, ccot, qcot, order, pos):
    length, width = content.shape
    return pl.pallas_call(
        sort_kernel,
        out_shape=(
            SDS((2 * length, width), jnp.bfloat16),
            SDS((2 * length, width), jnp.bfloat16),
            SDS((2, length, length), jnp.float32),
        ),
        in_specs=[SMEM_SPEC] + [VMEM_SPEC] * 8,
        out_specs=(VMEM_SPEC,) * 3,
        compiler_params=params(),
        name="sort_rows",
    )(bounds, content, query, ccot, qcot, order.reshape(1, length), order.reshape(length, 1),
      pos.reshape(1, length), pos.reshape(length, 1))


def unsort_kernel(order_col, values, out):
    length = order_col.shape[0]
    across = lax.broadcasted_iota(jnp.int32, (length, length), 1)
    onehot = jnp.where(order_col[...] == across, 1.0, 0.0).astype(jnp.bfloat16)
    for stream in range(2):
        out[stream] = product(
            onehot, values[stream * length : (stream + 1) * length, :]
        ).astype(jnp.bfloat16)


def unsort_rows(order, values):
    length = order.shape[0]
    width = values.shape[1]
    return pl.pallas_call(
        unsort_kernel,
        out_shape=SDS((2, length, width), jnp.bfloat16),
        in_specs=[VMEM_SPEC] * 2,
        out_specs=VMEM_SPEC,
        compiler_params=params(),
        name="unsort_rows",
    )(order.reshape(length, 1), values)


def bucket_onehot(length):
    distance = lax.broadcasted_iota(jnp.int32, (BUCKETS, 2 * length), 1) - (length - 1)
    magnitude = jnp.abs(distance)
    counted = jnp.zeros(distance.shape, jnp.int32)
    for limit in limits:
        counted = counted + (magnitude >= limit).astype(jnp.int32)
    bucket = counted + 16 * (distance > 0).astype(jnp.int32)
    return bucket == lax.broadcasted_iota(jnp.int32, distance.shape, 0)


def bias_kernel(table, out):
    length = 512
    onehot = jnp.where(bucket_onehot(length), 1.0, 0.0).astype(jnp.bfloat16)
    rows = product(table[...], onehot)
    for head in range(HEADS):
        spread = jnp.broadcast_to(rows[head : head + 1, :], (TILE, 2 * length))
        out[head] = pltpu.roll(
            spread, 2 * length - (TILE - 1), 1, stride=1, stride_axis=0
        )[:, : 2 * length - TILE]


def bias_table(table, length):
    return pl.pallas_call(
        bias_kernel,
        out_shape=SDS((HEADS, TILE, 2 * length - TILE), jnp.float32),
        in_specs=[VMEM_SPEC],
        out_specs=VMEM_SPEC,
        compiler_params=params(),
        name="bias_table",
    )(table)


def block_copies(spots, pieces, target, sems, tiles):
    count = sum(piece.shape[0] for piece in pieces)
    half = spots[count]
    copies = []
    for index, piece in enumerate(pieces):
        side = half if index < len(pieces) // 2 else 1 - half
        rows = piece.shape[2]
        for block in range(piece.shape[0]):
            at = len(copies)
            row = pl.multiple_of(spots[at] * rows, rows)
            copies.append(
                pltpu.make_async_copy(
                    piece.at[block, tiles],
                    target.at[side, :, pl.ds(row, rows), :],
                    sems.at[at],
                )
            )
    return copies


def block_stores(spots, source, outs, sems, tiles):
    count = sum(out.shape[0] for out in outs)
    half = spots[count]
    copies = []
    for index, out in enumerate(outs):
        side = half if index == 0 else 1 - half
        rows = out.shape[2]
        for block in range(out.shape[0]):
            at = len(copies)
            row = pl.multiple_of(spots[at] * rows, rows)
            copies.append(
                pltpu.make_async_copy(
                    source.at[side, :, pl.ds(row, rows), :],
                    out.at[block, tiles],
                    sems.at[at],
                )
            )
    return copies


def run_copies(copies):
    for copy in copies:
        copy.start()
    for copy in copies:
        copy.wait()


def joined(weights, index):
    return jnp.concatenate([weights[0, index], weights[1, index]], axis=1)


def head_lanes(head, shape):
    lane = lax.broadcasted_iota(jnp.int32, shape, 1)
    return (lane >= head * HEAD_DIM) & (lane < (head + 1) * HEAD_DIM)


def attend_kernel(spots, xs, mask, bias, bq, bv, *rest):
    pieces, rest = rest[:-7], rest[-7:]
    q_out, k_out, v_out, mixed_out, lse_out, weights_all, sems = rest
    length = mask.shape[1]
    group = pl.program_id(0)

    @pl.when(group == 0)
    def _():
        copies = block_copies(spots, pieces, weights_all, sems, slice(0, 3 * GROUPS))
        run_copies(copies)

    q = (product(xs[...], joined(weights_all, 3 * group)) + bq[...]).astype(jnp.bfloat16)
    q_out[...] = q
    k = product(xs[0:length, :], joined(weights_all, 3 * group + 1)).astype(jnp.bfloat16)
    k_out[...] = k
    v = product(xs[0:length, :], joined(weights_all, 3 * group + 2)) + bv[...]
    v = v.astype(jnp.bfloat16)
    v_out[...] = v
    low = jnp.bfloat16(0)
    heads_v = [jnp.where(head_lanes(h, v.shape), v, low) for h in range(GROUP)]
    for stream in range(2):
        for tile in range(length // TILE):
            at = stream * length + tile * TILE
            q_tile = q_out[at : at + TILE, :] * jnp.bfloat16(0.125)
            masked = mask[stream, tile * TILE : (tile + 1) * TILE, :]
            total = jnp.zeros((TILE, LANES), jnp.float32)
            for h in range(GROUP):
                q_head = jnp.where(head_lanes(h, q_tile.shape), q_tile, low)
                scores = product(q_head, k, NT)
                first = length - TILE - tile * TILE
                scores = scores + bias[h, :, first : first + length] + masked
                peak = jnp.maximum(jnp.max(scores, axis=-1, keepdims=True), FLOOR)
                weights = jnp.exp(scores - peak)
                summed = row_sum(weights)
                alive = summed > 0
                inverse = jnp.where(alive, 1.0 / summed, 0.0)
                probs = (weights * inverse).astype(jnp.bfloat16)
                total = total + product(probs, heads_v[h])
                lse_out[0, at : at + TILE, h : h + 1] = jnp.where(
                    alive, peak + jnp.log(summed), 0.0
                )
            mixed_out[at : at + TILE, :] = total.astype(jnp.bfloat16)


def attend(spots, xs, mask, bias, bq, bv, pieces):
    tokens, width = xs.shape
    blocks = sum(piece.shape[0] for piece in pieces)
    length = mask.shape[1]
    full = lambda g: (0, 0)
    column = lambda g: (0, g)
    return pl.pallas_call(
        attend_kernel,
        grid=(GROUPS,),
        out_shape=(
            SDS((tokens, width), jnp.bfloat16),
            SDS((length, width), jnp.bfloat16),
            SDS((length, width), jnp.bfloat16),
            SDS((tokens, width), jnp.bfloat16),
            SDS((GROUPS, tokens, 128), jnp.float32),
        ),
        in_specs=[
            SMEM_SPEC,
            pl.BlockSpec((tokens, width), full),
            pl.BlockSpec((2, length, length), lambda g: (0, 0, 0)),
            pl.BlockSpec((GROUP, TILE, bias.shape[2]), lambda g: (g, 0, 0)),
            pl.BlockSpec((1, LANES), column),
            pl.BlockSpec((1, LANES), column),
        ] + [pl.BlockSpec(memory_space=pl.ANY)] * len(pieces),
        out_specs=(
            pl.BlockSpec((tokens, LANES), column),
            pl.BlockSpec((length, LANES), column),
            pl.BlockSpec((length, LANES), column),
            pl.BlockSpec((tokens, LANES), column),
            pl.BlockSpec((1, tokens, 128), lambda g: (g, 0, 0)),
        ),
        scratch_shapes=[
            pltpu.VMEM((2, 3 * GROUPS, width, 128), jnp.bfloat16),
            pltpu.SemaphoreType.DMA((blocks,)),
        ],
        compiler_params=params(("arbitrary",)),
        name="attend",
    )(spots, xs, mask, bias, bq, bv, *pieces)


BLOCK = 256


def norm_parts(values):
    mean = jnp.mean(values, axis=-1, keepdims=True)
    center = values - mean
    spread = jnp.mean(center * center, axis=-1, keepdims=True)
    scale = lax.rsqrt(spread + EPS)
    return center * scale, scale


def norm_back(normal, scale, grad):
    mean = jnp.mean(grad, axis=-1, keepdims=True)
    inner = jnp.mean(grad * normal, axis=-1, keepdims=True)
    return scale * (grad - mean - normal * inner)


def column_sum(values):
    return jnp.sum(values, axis=0, keepdims=True)


def feed_kernel(spots, xs, mixed, cot, up_own, up_other, down_own, down_other, rows, up_bias,
                *rest):
    pieces, rest = rest[:-12], rest[-12:]
    (out, act_out, gup_out, first_out, gdown_out, gres_out, gbranch_out, gmixed_out,
     sums, up_sums, wo_all, sems) = rest
    step = pl.program_id(0)
    out_bias, mixer_gain, mixer_shift = rows[0:1, :], rows[1:2, :], rows[2:3, :]
    down_bias, final_gain, final_shift = rows[3:4, :], rows[4:5, :], rows[5:6, :]
    half = up_own.shape[0]

    @pl.when(step == 0)
    def _():
        sums[...] = jnp.zeros_like(sums)
        up_sums[...] = jnp.zeros_like(up_sums)
        tiles = slice(3 * GROUPS, 4 * GROUPS)
        run_copies(block_copies(spots, pieces, wo_all, sems, tiles))

    wo = jnp.concatenate([joined(wo_all, index) for index in range(GROUPS)], axis=1)
    branch = product(mixed[...], wo) + out_bias
    normal1, scale1 = norm_parts(xs[...].astype(jnp.float32) + branch)
    first = normal1 * mixer_gain + mixer_shift
    first_low = first.astype(jnp.bfloat16)
    first_out[...] = first_low
    slopes = []
    second = first + down_bias
    for index, (up_w, down_w) in enumerate(((up_own, down_own), (up_other, down_other))):
        lanes = slice(index * half, (index + 1) * half)
        up = product(first_low, up_w[...], NT) + up_bias[:, lanes]
        gate = 0.5 * (1.0 + lax.erf(up * math.sqrt(0.5)))
        act = (up * gate).astype(jnp.bfloat16)
        act_out[:, lanes] = act
        slopes.append(gate + up * jnp.exp(-0.5 * up * up) * (1.0 / math.sqrt(2.0 * math.pi)))
        second = second + product(act, down_w[...])
    normal2, scale2 = norm_parts(second)
    out[...] = (normal2 * final_gain + final_shift).astype(jnp.bfloat16)
    cots = cot[...].astype(jnp.float32)
    gsecond = norm_back(normal2, scale2, cots * final_gain)
    gdown = gsecond.astype(jnp.bfloat16)
    gdown_out[...] = gdown
    gfirst = gsecond
    for index, (up_w, down_w) in enumerate(((up_own, down_own), (up_other, down_other))):
        lanes = slice(index * half, (index + 1) * half)
        gup = (product(gdown, down_w[...], NT) * slopes[index]).astype(jnp.bfloat16)
        gup_out[:, lanes] = gup
        up_sums[:, lanes] += column_sum(gup.astype(jnp.float32))
        gfirst = gfirst + product(gup, up_w[...])
    gres = norm_back(normal1, scale1, gfirst * mixer_gain)
    gres_out[...] = gres
    gbranch = gres.astype(jnp.bfloat16)
    gbranch_out[...] = gbranch
    gmixed_out[...] = product(gbranch, wo, NT).astype(jnp.bfloat16)
    sums[0:1, :] += column_sum(gbranch.astype(jnp.float32))
    sums[1:2, :] += column_sum(gfirst * normal1)
    sums[2:3, :] += column_sum(gfirst)
    sums[3:4, :] += column_sum(gdown.astype(jnp.float32))
    sums[4:5, :] += column_sum(cots * normal2)
    sums[5:6, :] += column_sum(cots)


def feed(spots, xs, mixed, cot, up_own, up_other, down_own, down_other, rows, up_bias, pieces):
    tokens, width = xs.shape
    blocks = sum(piece.shape[0] for piece in pieces)
    half = up_own.shape[0]
    hidden = 2 * half
    token = pl.BlockSpec((BLOCK, width), lambda i: (i, 0))
    wide = pl.BlockSpec((BLOCK, hidden), lambda i: (i, 0))

    def whole(shape):
        return pl.BlockSpec(shape, lambda i: (0, 0), pipeline_mode=pl.Buffered(1))

    return pl.pallas_call(
        feed_kernel,
        grid=(tokens // BLOCK,),
        out_shape=(
            SDS((tokens, width), jnp.bfloat16),
            SDS((tokens, hidden), jnp.bfloat16),
            SDS((tokens, hidden), jnp.bfloat16),
            SDS((tokens, width), jnp.bfloat16),
            SDS((tokens, width), jnp.bfloat16),
            SDS((tokens, width), jnp.float32),
            SDS((tokens, width), jnp.bfloat16),
            SDS((tokens, width), jnp.bfloat16),
            SDS((8, width), jnp.float32),
            SDS((1, hidden), jnp.float32),
        ),
        in_specs=[SMEM_SPEC, token, token, token]
        + [whole((half, width))] * 4
        + [whole((8, width)), whole((1, hidden))]
        + [pl.BlockSpec(memory_space=pl.ANY)] * len(pieces),
        out_specs=(token, wide, wide, token, token, token, token, token,
                   pl.BlockSpec((8, width), lambda i: (0, 0)),
                   pl.BlockSpec((1, hidden), lambda i: (0, 0))),
        scratch_shapes=[
            pltpu.VMEM((2, GROUPS, width, 128), jnp.bfloat16),
            pltpu.SemaphoreType.DMA((blocks,)),
        ],
        compiler_params=params(("arbitrary",), 60),
        name="feed",
    )(spots, xs, mixed, cot, up_own, up_other, down_own, down_other, rows, up_bias, *pieces)


def weight_kernel(act, gup, first, gdown, down_out, up_out):
    down_out[...] = product(act[...], gdown[...], TN).astype(jnp.bfloat16)
    up_out[...] = product(gup[...], first[...], TN).astype(jnp.bfloat16)


def feed_weights(act, gup, first, gdown, start, count, chunk):
    tokens, width = first.shape
    base = start // chunk
    full = pl.BlockSpec((tokens, width), lambda i: (0, 0))
    return pl.pallas_call(
        weight_kernel,
        grid=(count // chunk,),
        out_shape=(SDS((count, width), jnp.bfloat16), SDS((count, width), jnp.bfloat16)),
        in_specs=[
            pl.BlockSpec((tokens, chunk), lambda i: (0, base + i)),
            pl.BlockSpec((tokens, chunk), lambda i: (0, base + i)),
            full, full,
        ],
        out_specs=(pl.BlockSpec((chunk, width), lambda i: (i, 0)),) * 2,
        compiler_params=params(("arbitrary",)),
        name="feed_weights",
    )(act, gup, first, gdown)


def out_weight_kernel(spots, mixed, gbranch, own, other, buffer, sems):
    grad = product(mixed[...], gbranch[...], TN).astype(jnp.bfloat16)
    for index in range(GROUPS):
        for half in range(2):
            first = index * LANES + half * 128
            buffer[half, index] = grad[:, first : first + 128]
    run_copies(block_stores(spots, buffer, (own, other), sems, slice(0, GROUPS)))


def out_weights(spots, mixed, gbranch, blocks):
    width = mixed.shape[1]
    shape = SDS((blocks, GROUPS, width // blocks, 128), jnp.bfloat16)
    return pl.pallas_call(
        out_weight_kernel,
        out_shape=(shape, shape),
        in_specs=[SMEM_SPEC] + [VMEM_SPEC] * 2,
        out_specs=(pl.BlockSpec(memory_space=pl.ANY),) * 2,
        scratch_shapes=[
            pltpu.VMEM((2, GROUPS, width, 128), jnp.bfloat16),
            pltpu.SemaphoreType.DMA((2 * blocks,)),
        ],
        compiler_params=params(),
        name="out_weights",
    )(spots, mixed, gbranch)


def attend_back_kernel(spots, xs, mask, bias, q, k, v, gmixed, lse, gres, *rest):
    pieces, rest = rest[:-14], rest[-14:]
    (gx_out, gw_own, gw_other, sums_out, gtable_out,
     probs_low, gscores_low, gdist, gx, gq, weights_all, buffer, sems, out_sems) = rest
    group = pl.program_id(0)
    length = mask.shape[1]
    low = jnp.bfloat16(0)

    @pl.when(group == 0)
    def _():
        gx[...] = gres[...]
        copies = block_copies(spots, pieces, weights_all, sems, slice(0, 3 * GROUPS))
        run_copies(copies)

    keys = k[...]
    values = v[...]
    gk = jnp.zeros((length, LANES), jnp.float32)
    gv = jnp.zeros((length, LANES), jnp.float32)
    for h in range(GROUP):
        gdist[h] = jnp.zeros(gdist.shape[1:], jnp.float32)
        for tile in range(length // TILE):
            first = length - TILE - tile * TILE
            both = None
            for stream in range(2):
                at = stream * length + tile * TILE
                rows = slice(at, at + TILE)
                q_tile = q[rows, :] * jnp.bfloat16(0.125)
                lanes = head_lanes(h, q_tile.shape)
                scores = product(jnp.where(lanes, q_tile, low), keys, NT)
                scores = scores + bias[h, :, first : first + length]
                scores = scores + mask[stream, tile * TILE : (tile + 1) * TILE, :]
                probs = jnp.exp(scores - lse[0, rows, h : h + 1])
                gprobs = product(jnp.where(lanes, gmixed[rows, :], low), values, NT)
                weighted = probs * gprobs
                gscores = weighted - probs * row_sum(weighted)
                probs_low[rows, :] = probs.astype(jnp.bfloat16)
                gscores_low[rows, :] = gscores.astype(jnp.bfloat16)
                both = gscores if both is None else both + gscores
            gdist[h, :, first : first + length] += both
        scaled = q[...] * jnp.bfloat16(0.125)
        lanes = head_lanes(h, scaled.shape)
        key_lanes = head_lanes(h, keys.shape)
        gq_head = product(gscores_low[...], jnp.where(key_lanes, keys, low))
        if h == 0:
            gq[...] = gq_head
        else:
            gq[...] += gq_head
        gk = gk + product(gscores_low[...], jnp.where(lanes, scaled, low), TN)
        gv = gv + product(probs_low[...], jnp.where(lanes, gmixed[...], low), TN)
    gq_low = (gq[...] * 0.125).astype(jnp.bfloat16)
    gk_low = gk.astype(jnp.bfloat16)
    gv_low = gv.astype(jnp.bfloat16)
    for index, grad in enumerate((
        product(xs[...], gq_low, TN),
        product(xs[0:length, :], gk_low, TN),
        product(xs[0:length, :], gv_low, TN),
    )):
        grad = grad.astype(jnp.bfloat16)
        buffer[0, index] = grad[:, :128]
        buffer[1, index] = grad[:, 128:]
    tiles = pl.ds(3 * group, 3)
    run_copies(block_stores(spots, buffer, (gw_own, gw_other), out_sems, tiles))
    sums_out[0:1, :] = column_sum(gq_low.astype(jnp.float32))
    sums_out[1:2, :] = column_sum(gv_low.astype(jnp.float32))
    gx[...] += product(gq_low, joined(weights_all, 3 * group), NT)
    gx[0:length, :] += product(gk_low, joined(weights_all, 3 * group + 1), NT) + product(
        gv_low, joined(weights_all, 3 * group + 2), NT
    )
    span = 2 * length
    pieces = []
    row_index = lax.broadcasted_iota(jnp.int32, (8, span), 0)
    for h in range(GROUP):
        wide = jnp.concatenate([gdist[h], jnp.zeros((TILE, TILE), jnp.float32)], axis=1)
        size = TILE // 2
        while size >= 8:
            wide = wide[size:, :] + pltpu.roll(wide[:size, :], size, 1)
            size //= 2
        for bit in (4, 2, 1):
            wide = jnp.where(row_index & bit == 0, pltpu.roll(wide, bit, 1), wide)
        pieces.append(column_sum(wide))
    pieces.append(jnp.zeros((8 - GROUP, span), jnp.float32))
    onehot = jnp.where(bucket_onehot(length), 1.0, 0.0)
    gtable_out[0] = lax.dot_general(
        jnp.concatenate(pieces, axis=0), onehot, NT, precision=lax.Precision.HIGHEST,
        preferred_element_type=jnp.float32,
    )

    @pl.when(group == GROUPS - 1)
    def _():
        gx_out[...] = gx[...].astype(jnp.bfloat16)


def attend_back(spots, xs, mask, bias, q, k, v, gmixed, lse, gres, pieces, blocks):
    tokens, width = xs.shape
    held = sum(piece.shape[0] for piece in pieces)
    shape = SDS((blocks, 3 * GROUPS, width // blocks, 128), jnp.bfloat16)
    anywhere = pl.BlockSpec(memory_space=pl.ANY)
    length = mask.shape[1]
    full = lambda g: (0, 0)
    column = lambda g: (0, g)
    once = pl.Buffered(1)
    return pl.pallas_call(
        attend_back_kernel,
        grid=(GROUPS,),
        out_shape=(
            SDS((tokens, width), jnp.bfloat16),
            shape,
            shape,
            SDS((8, width), jnp.float32),
            SDS((GROUPS, 8, BUCKETS), jnp.float32),
        ),
        in_specs=[
            SMEM_SPEC,
            pl.BlockSpec((tokens, width), full, pipeline_mode=once),
            pl.BlockSpec((2, length, length), lambda g: (0, 0, 0), pipeline_mode=once),
            pl.BlockSpec((GROUP, TILE, bias.shape[2]), lambda g: (g, 0, 0)),
            pl.BlockSpec((tokens, LANES), column),
            pl.BlockSpec((length, LANES), column),
            pl.BlockSpec((length, LANES), column),
            pl.BlockSpec((tokens, LANES), column),
            pl.BlockSpec((1, tokens, 128), lambda g: (g, 0, 0)),
            pl.BlockSpec((tokens, width), full, pipeline_mode=once),
        ] + [anywhere] * len(pieces),
        out_specs=(
            pl.BlockSpec((tokens, width), full),
            anywhere,
            anywhere,
            pl.BlockSpec((8, LANES), column),
            pl.BlockSpec((1, 8, BUCKETS), lambda g: (g, 0, 0)),
        ),
        scratch_shapes=[
            pltpu.VMEM((tokens, length), jnp.bfloat16),
            pltpu.VMEM((tokens, length), jnp.bfloat16),
            pltpu.VMEM((GROUP, TILE, bias.shape[2]), jnp.float32),
            pltpu.VMEM((tokens, width), jnp.float32),
            pltpu.VMEM((tokens, LANES), jnp.float32),
            pltpu.VMEM((2, 3 * GROUPS, width, 128), jnp.bfloat16),
            pltpu.VMEM((2, 3, width, 128), jnp.bfloat16),
            pltpu.SemaphoreType.DMA((held,)),
            pltpu.SemaphoreType.DMA((2 * blocks,)),
        ],
        compiler_params=params(("arbitrary",)),
        name="attend_back",
    )(spots, xs, mask, bias, q, k, v, gmixed, lse, gres, *pieces)


BOTH = ("dp", "seq")


def xor_pairs(count, by_half):
    halves = len(by_half)
    return [
        (device * halves + half, (device ^ flip) * halves + half)
        for device in range(count)
        for half, flip in enumerate(by_half)
    ]


def swap(value):
    return lax.ppermute(value, "seq", [(0, 1), (1, 0)])


def collect(value, count):
    parts = [value]
    for high in range(1, count // 4):
        parts.append(lax.ppermute(value, BOTH, xor_pairs(count, (4 * high, 4 * high))))
    near = jnp.stack(parts)
    second = lax.ppermute(near, BOTH, xor_pairs(count, (1, 2)))
    third = lax.ppermute(jnp.concatenate([near, second]), BOTH, xor_pairs(count, (2, 1)))
    return near, second, third


def offsets(count, half):
    first = jnp.where(half == 0, 1, 2)
    highs = 4 * jnp.arange(count // 4)
    near = jnp.concatenate([highs, highs ^ first])
    return jnp.concatenate([near, near ^ (3 - first)])


def spread(blocks, count):
    shape = blocks.shape[1:]
    blocks = blocks.reshape((2, 2, count // 4) + shape)
    low = jnp.bfloat16
    wide = jnp.float32
    came = lax.ppermute(blocks[1].astype(low), BOTH, xor_pairs(count, (2, 1)))
    blocks = blocks[0].astype(wide) + came.astype(wide)
    came = lax.ppermute(blocks[1].astype(low), BOTH, xor_pairs(count, (1, 2)))
    blocks = blocks[0].astype(wide) + came.astype(wide)
    total = blocks[0]
    for high in range(1, count // 4):
        came = lax.ppermute(
            blocks[high].astype(low), BOTH, xor_pairs(count, (4 * high, 4 * high))
        )
        total = total + came.astype(wide)
    return total


def reduce_blocks(own, other, count):
    total = spread(own.astype(jnp.float32) + swap(other).astype(jnp.float32), count)
    return total, swap(total)


def in_order(half, own, other):
    return jnp.where(half == 0, jnp.stack([own, other]), jnp.stack([other, own]))


def shards(count, content, query_in, content_cot, query_cot, lengths, order, query_weight,
           query_bias, key_weight, value_weight, value_bias, out_weight, out_bias, mixer_gain,
           mixer_shift, up_weight, up_bias, down_weight, down_bias, final_gain, final_shift,
           position_bias):
    low, wide = jnp.bfloat16, jnp.float32
    _, block, width = content.shape
    length = order.shape[1]
    half = lax.axis_index("seq")
    me = lax.axis_index("dp")
    rows = query_weight.shape[0]
    hidden = up_weight.shape[1]

    square = jnp.stack([query_weight, key_weight, value_weight, out_weight])
    square = square.reshape(4, rows, GROUPS, 2, 128)
    square = lax.dynamic_index_in_dim(square, half, 3, keepdims=False)
    square = jnp.transpose(square, (2, 0, 1, 3))
    square = jnp.concatenate(
        [square[:, :3].reshape(3 * GROUPS, rows, 128), square[:, 3]]
    )
    squares = collect(square, count)
    squares = squares + tuple(swap(piece) for piece in squares)

    vectors = (query_bias, value_bias, out_bias, mixer_gain, mixer_shift, down_bias, final_gain,
               final_shift, up_bias, position_bias)
    packed = jnp.concatenate(vectors)
    packed = lax.all_to_all(
        jnp.broadcast_to(packed[None], (count, packed.shape[0])), "dp", 0, 0, tiled=True
    )
    sizes = [vector.shape[0] for vector in vectors]
    starts = [sum(sizes[:index]) for index in range(len(sizes) + 1)]
    cut = [packed[:, starts[i] : starts[i + 1]] for i in range(len(sizes))]
    flat = [part.reshape(1, -1).astype(wide) for part in cut[:8]]
    table = cut[9].reshape(BUCKETS, HEADS)
    table = jnp.pad(jnp.transpose(table), ((0, 16 - HEADS), (0, 0)))

    mine = [lax.dynamic_index_in_dim(a, half, 0, keepdims=False)
            for a in (content, query_in, content_cot, query_cot)]
    theirs = [lax.dynamic_index_in_dim(a, 1 - half, 0, keepdims=False)
              for a in (content, query_in, content_cot, query_cot)]
    came = swap(jnp.stack(theirs))
    tokens = [jnp.concatenate([mine[i], came[i]]) for i in range(4)]
    pos = lax.rem(jnp.arange(length, dtype=jnp.int32) + half * block, length)
    order_row = lax.dynamic_index_in_dim(order, half, 0, keepdims=False)
    order_row = jnp.where(half == 0, order_row, jnp.roll(order_row, -block))
    bounds = jnp.cumsum(lax.dynamic_index_in_dim(lengths, half, 0, keepdims=False))[:-1]
    xs, cs, mask = sort_rows(bounds.astype(jnp.int32), *tokens, order_row, pos)
    bias = bias_table(table, length)

    flips = offsets(count, half)
    other_flips = offsets(count, 1 - half)
    chips, other_chips = me ^ flips, me ^ other_flips
    aligned = rows % 16 == 0
    if aligned:
        pieces = squares
        spots = jnp.concatenate([chips, other_chips, half[None]]).astype(jnp.int32)
        out_blocks = count
    else:
        pieces = []
        for side, places in ((squares[:3], chips), (squares[3:], other_chips)):
            joint = jnp.concatenate(side)
            ordered = jnp.take(joint, jnp.argsort(places), axis=0)
            ordered = jnp.transpose(ordered, (1, 0, 2, 3)).reshape(1, 4 * GROUPS, width, 128)
            pieces += [ordered, ordered[:0], ordered[:0]]
        pieces = tuple(piece for piece in pieces if piece.shape[0])
        spots = jnp.stack([0 * half, 0 * half, half]).astype(jnp.int32)
        out_blocks = 1

    q, k, v, mixed, lse = attend(spots, xs, mask, bias, flat[0], flat[1], pieces)

    middle = hidden // 2
    up_rows = jnp.transpose(up_weight)
    feed_own = jnp.stack([
        lax.dynamic_slice_in_dim(up_rows, half * middle, middle),
        lax.dynamic_slice_in_dim(down_weight, half * middle, middle),
    ])
    feeds = collect(feed_own, count)
    feeds = jnp.concatenate(feeds)
    feeds_other = swap(feeds)
    ups = [side[:, 0].reshape(count * middle, width) for side in (feeds, feeds_other)]
    downs = [side[:, 1].reshape(count * middle, width) for side in (feeds, feeds_other)]
    bias_parts = cut[8].reshape(count, 2, middle)
    ups_bias = []
    for side, places in ((half, chips), (1 - half, other_chips)):
        chosen = lax.dynamic_index_in_dim(bias_parts, side, 1, keepdims=False)
        pick = (places[:, None] == jnp.arange(count)[None, :]).astype(low)
        ups_bias.append(jnp.dot(pick, chosen, preferred_element_type=wide).reshape(1, -1))
    up_bias_all = jnp.concatenate(ups_bias, axis=1)
    vector_rows = jnp.concatenate(flat[2:8] + [jnp.zeros((2, width), wide)])
    out, act, gup, first, gdown, gres, gbranch, gmixed, sums, up_sums = feed(
        spots, xs, mixed, cs, ups[0], ups[1], downs[0], downs[1], vector_rows, up_bias_all, pieces
    )
    placed = unsort_rows(order_row, out)
    outs = place_rows(half, placed, block)

    share = count * middle
    gdown_other, gup_other = feed_weights(act, gup, first, gdown, share, share, share // 3)
    gdown_own, gup_own = feed_weights(act, gup, first, gdown, 0, share, share // 3)
    fshape = (count, middle, width)
    feed_grads = reduce_blocks(
        jnp.stack([gup_own.reshape(fshape), gdown_own.reshape(fshape)], axis=1),
        jnp.stack([gup_other.reshape(fshape), gdown_other.reshape(fshape)], axis=1),
        count,
    )
    feed_grads = in_order(half, *feed_grads)
    up_grad = jnp.transpose(feed_grads[:, 0].reshape(hidden, width))
    down_grad = feed_grads[:, 1].reshape(hidden, width)

    def by_device(grads):
        if aligned:
            return grads
        result = []
        for grad, places in zip(grads, (chips, other_chips)):
            parts = grad[0].reshape(grad.shape[1], count, rows, 128)
            result.append(jnp.take(jnp.transpose(parts, (1, 0, 2, 3)), places, axis=0))
        return result

    gwo = reduce_blocks(*by_device(out_weights(spots, mixed, gbranch, out_blocks)), count)
    gx, gw_own, gw_other, asums, gtable = attend_back(
        spots, xs, mask, bias, q, k, v, gmixed, lse, gres, pieces, out_blocks
    )
    grads = place_rows(half, unsort_rows(order_row, gx), block)
    gws = reduce_blocks(*by_device((gw_own, gw_other)), count)

    def square_grad(pair, tiles):
        both = in_order(half, pair[0][tiles], pair[1][tiles])
        return jnp.transpose(both, (2, 1, 0, 3)).reshape(rows, width)

    query_grad, key_grad, value_grad = (
        square_grad(gws, slice(index, None, 3)) for index in range(3)
    )
    out_grad = square_grad(gwo, slice(None))

    gtable = jnp.transpose(gtable[:, :GROUP].reshape(HEADS, BUCKETS))
    up_parts = []
    for side, places in ((half, chips), (1 - half, other_chips)):
        pick = (jnp.arange(count)[:, None] == places[None, :]).astype(wide)
        part = lax.dynamic_index_in_dim(
            up_sums.reshape(2, count, middle), jnp.where(side == half, 0, 1), 0, keepdims=False
        )
        up_parts.append(jnp.dot(pick, part, precision=lax.Precision.HIGHEST))
    up_parts = in_order(half, up_parts[0], up_parts[1])
    up_parts = jnp.transpose(up_parts, (1, 0, 2)).reshape(count, hidden)
    shares = [asums[0], asums[1], sums[0], sums[1], sums[2], sums[3], sums[4], sums[5]]
    packed = jnp.concatenate(
        [share.reshape(count, -1) for share in shares]
        + [up_parts, gtable.reshape(count, -1)],
        axis=1,
    )
    packed = jnp.sum(lax.all_to_all(packed, "dp", 0, 0, tiled=True), axis=0)
    packed = packed + swap(packed)
    ends = [packed[starts[i] : starts[i + 1]] for i in range(len(sizes))]
    return (
        outs[0], outs[1], grads[0], grads[1],
        query_grad, ends[0], key_grad, value_grad, ends[1], out_grad, ends[2], ends[3], ends[4],
        up_grad, ends[8], down_grad, ends[5], ends[6], ends[7], ends[9],
    )


def place_rows(half, placed, block):
    came = swap(placed[:, block:])
    own = placed[:, :block]
    return [
        jnp.where(half == 0, jnp.stack([own[i], came[i]]), jnp.stack([came[i], own[i]]))
        for i in range(2)
    ]


def solution(mesh):
    rows3 = P("dp", "seq", None)
    flat, first, last = P("dp"), P("dp", None), P(None, "dp")
    in_specs = (
        rows3, rows3, rows3, rows3, first, first, first, flat, first, first, flat, first, flat,
        flat, flat, last, flat, first, flat, flat, flat, flat,
    )
    out_specs = (
        rows3, rows3, rows3, rows3, first, flat, first, first, flat, first, flat, flat, flat,
        last, flat, first, flat, flat, flat, flat,
    )
    body = functools.partial(shards, mesh.shape["dp"])
    return jax.shard_map(
        body, mesh=mesh, in_specs=in_specs, out_specs=out_specs, check_vma=False
    )
```

```python
import functools
import math

import jax
import jax.numpy as jnp
from jax import lax
from jax.experimental import pallas as pl
from jax.experimental.pallas import tpu as pltpu
from jax.sharding import PartitionSpec as P

HEADS = 12
HEAD_DIM = 64
BUCKETS = 32
GROUP = 4
LANES = GROUP * HEAD_DIM
GROUPS = HEADS // GROUP
TILE = 128
TILES = 4
NEG = -1e30
FLOOR = -1e29
EPS = 1e-05

limits = (1, 2, 3, 4, 5, 6, 7, 8, 12, 16, 23, 32, 46, 64, 91)

NN = (((1,), (0,)), ((), ()))
NT = (((1,), (1,)), ((), ()))
TN = (((0,), (0,)), ((), ()))
VMEM_SPEC = pl.BlockSpec(memory_space=pltpu.VMEM)
HBM_SPEC = pl.BlockSpec(memory_space=pltpu.HBM)
SCALE = 1.6e6
SMEM_SPEC = pl.BlockSpec(memory_space=pltpu.SMEM)
SDS = jax.ShapeDtypeStruct


def cost(micros):
    return pl.CostEstimate(
        flops=0, bytes_accessed=int(micros * SCALE), transcendentals=0
    )


def product(left, right, dims=NN):
    return lax.dot_general(left, right, dims, preferred_element_type=jnp.float32)


def params(semantics=None, limit=56):
    return pltpu.CompilerParams(dimension_semantics=semantics, vmem_limit_bytes=limit << 20)


def row_sum(values):
    return jnp.sum(values, axis=-1, keepdims=True)


ME, HALF = 0, 1
VECTORS, UP_SLOT, TABLE_SLOT = 10, 8, 9
VECTOR_TILE = 4 * GROUPS
GRAD_TILES = VECTOR_TILE + 1
FULL = 60


def in_hbm(*values):
    return [pltpu.with_memory_space_constraint(value, pltpu.HBM) for value in values]


def run_copies(copies):
    for copy in copies:
        copy.start()
    for copy in copies:
        copy.wait()


def pack_kernel(ids, content, query, ccot, qcot, wq, wk, wv, wo, up, down, *rest):
    vectors, rest = rest[:VECTORS], rest[VECTORS:]
    (theirs, square, feed, slots, tokens, squares, feeds, turned, in_sems, out_sems) = rest
    half = ids[HALF]
    share = feed.shape[1]
    loads = []

    def load(source, target):
        copy = pltpu.make_async_copy(source, target, in_sems.at[len(loads)])
        copy.start()
        loads.append(copy)

    for index, weight in enumerate((wq, wk, wv, wo)):
        for group in range(GROUPS):
            lane = pl.multiple_of(group * LANES + half * 128, 128)
            place = 3 * group + index if index < 3 else 3 * GROUPS + group
            load(weight.at[:, pl.ds(lane, 128)], squares.at[place])
    for index, source in enumerate((content, query, ccot, qcot)):
        load(source.at[1 - half], tokens.at[index])
    rows = pl.ds(pl.multiple_of(half * share, share), share)
    load(down.at[rows, :], feeds)
    turned[...] = jnp.transpose(up[...].astype(jnp.float32)).astype(jnp.bfloat16)
    slots[...] = jnp.zeros_like(slots)
    for index, vector in enumerate(vectors):
        slots[index : index + 1, : vector.shape[1]] = vector[...]
    for copy in loads[: 4 * GROUPS]:
        copy.wait()
    stores = [
        pltpu.make_async_copy(squares, square, out_sems.at[0]),
        pltpu.make_async_copy(turned.at[rows, :], feed.at[0], out_sems.at[1]),
        pltpu.make_async_copy(tokens, theirs, out_sems.at[2]),
        pltpu.make_async_copy(feeds, feed.at[1], out_sems.at[3]),
    ]
    stores[0].start()
    stores[1].start()
    for copy in loads[4 * GROUPS :]:
        copy.wait()
    stores[2].start()
    stores[3].start()
    for copy in stores:
        copy.wait()


def pack(ids, content, query, ccot, qcot, wq, wk, wv, wo, up, down, vectors):
    _, block, width = content.shape
    rows = wq.shape[0]
    hidden = up.shape[1]
    return pl.pallas_call(
        pack_kernel,
        out_shape=(
            SDS((4, block, width), jnp.bfloat16),
            SDS((4 * GROUPS, rows, 128), jnp.bfloat16),
            SDS((2, hidden // 2, width), jnp.bfloat16),
            SDS((16, 256), jnp.bfloat16),
        ),
        in_specs=[SMEM_SPEC] + [HBM_SPEC] * 8 + [VMEM_SPEC, HBM_SPEC] + [VMEM_SPEC] * VECTORS,
        out_specs=(HBM_SPEC,) * 3 + (VMEM_SPEC,),
        scratch_shapes=[
            pltpu.VMEM((4, block, width), jnp.bfloat16),
            pltpu.VMEM((4 * GROUPS, rows, 128), jnp.bfloat16),
            pltpu.VMEM((hidden // 2, width), jnp.bfloat16),
            pltpu.VMEM((hidden, width), jnp.bfloat16),
            pltpu.SemaphoreType.DMA((4 * GROUPS + 5,)),
            pltpu.SemaphoreType.DMA((4,)),
        ],
        cost_estimate=cost(4),
        compiler_params=params(None, FULL),
        name="pack",
    )(ids, *in_hbm(content, query, ccot, qcot, wq, wk, wv, wo), up, *in_hbm(down),
      *(vector.reshape(1, -1) for vector in vectors))


def order_onehot(ids, order):
    length = order.shape[1]
    row = order[pl.ds(ids[HALF], 1), :]
    down = lax.broadcasted_iota(jnp.int32, (length, length), 0)
    return jnp.where(row == down, 1.0, 0.0).astype(jnp.bfloat16)


def sort_kernel(ids, lengths, content, query, ccot, qcot, came, order,
                xs_out, cs_out, mask_out, held, sems):
    length = order.shape[1]
    block = content.shape[1]
    half = ids[HALF]
    copies = []
    for index, source in enumerate((content, query, ccot, qcot)):
        for place, rows in ((half, source.at[half]), (1 - half, came.at[index])):
            here = pl.ds(pl.multiple_of(place * block, block), block)
            copies.append(
                pltpu.make_async_copy(rows, held.at[index, here], sems.at[len(copies)])
            )
    for copy in copies:
        copy.start()
    onehot = order_onehot(ids, order)
    lane = lax.broadcasted_iota(jnp.int32, (8, length), 1)
    line = lax.broadcasted_iota(jnp.int32, (8, length), 0)
    digits = jnp.where(line == 0, lane // 16, jnp.where(line == 1, lane % 16, 0))
    digits = product(digits.astype(jnp.float32).astype(jnp.bfloat16), onehot, NT)
    rank_row = digits[0:1, :] * 16.0 + digits[1:2, :]
    across = lax.broadcasted_iota(jnp.int32, (length, length), 1).astype(jnp.float32)
    rank_col = row_sum(onehot.astype(jnp.float32) * across)
    place_col = lax.broadcasted_iota(jnp.int32, (length, 1), 0)
    place_row = lax.broadcasted_iota(jnp.int32, (1, length), 1)
    segment_col = jnp.zeros((length, 1), jnp.int32)
    segment_row = jnp.zeros((1, length), jnp.int32)
    bound = jnp.int32(0)
    for index in range(lengths.shape[1] - 1):
        bound = bound + lengths[half, index]
        segment_col = segment_col + (place_col >= bound).astype(jnp.int32)
        segment_row = segment_row + (place_row >= bound).astype(jnp.int32)
    same = segment_col == segment_row
    mask_out[0] = jnp.where(same & (rank_row <= rank_col), 0.0, NEG).astype(jnp.bfloat16)
    mask_out[1] = jnp.where(same & (rank_row < rank_col), 0.0, NEG).astype(jnp.bfloat16)
    for copy in copies:
        copy.wait()
    for source, target, at in ((0, xs_out, 0), (1, xs_out, 1), (2, cs_out, 0), (3, cs_out, 1)):
        target[at * length : (at + 1) * length, :] = product(onehot, held[source]).astype(
            jnp.bfloat16
        )


def sort_rows(ids, lengths, tokens, came, order):
    length = order.shape[1]
    width = came.shape[2]
    return pl.pallas_call(
        sort_kernel,
        out_shape=(
            SDS((2 * length, width), jnp.bfloat16),
            SDS((2 * length, width), jnp.bfloat16),
            SDS((2, length, length), jnp.bfloat16),
        ),
        in_specs=[SMEM_SPEC] * 2 + [HBM_SPEC] * 5 + [VMEM_SPEC],
        out_specs=(VMEM_SPEC,) * 3,
        scratch_shapes=[
            pltpu.VMEM((4, length, width), jnp.bfloat16),
            pltpu.SemaphoreType.DMA((8,)),
        ],
        cost_estimate=cost(5),
        compiler_params=params(None, FULL),
        name="sort_rows",
    )(ids, lengths, *in_hbm(*tokens, came), order)


def put_back(ids, onehot, source, scratch, own, send, sems):
    length = onehot.shape[0]
    block = own.shape[1]
    for stream in range(2):
        rows = product(onehot, source(stream), TN).astype(jnp.bfloat16)
        scratch[0, stream] = rows[:block, :]
        scratch[1, stream] = rows[block:, :]
    run_copies([
        pltpu.make_async_copy(scratch.at[ids[HALF]], own, sems.at[0]),
        pltpu.make_async_copy(scratch.at[1 - ids[HALF]], send, sems.at[1]),
    ])


def unsort_kernel(ids, order, values, own, send, held, scratch, sems):
    length = order.shape[1]
    copy = pltpu.make_async_copy(values, held, sems.at[2])
    copy.start()
    onehot = order_onehot(ids, order)
    copy.wait()
    put_back(
        ids, onehot, lambda s: held[s * length : (s + 1) * length, :], scratch, own, send, sems
    )


def unsort_rows(ids, order, values):
    length = order.shape[1]
    width = values.shape[1]
    shape = SDS((2, length // 2, width), jnp.bfloat16)
    return pl.pallas_call(
        unsort_kernel,
        out_shape=(shape, shape),
        in_specs=[SMEM_SPEC, VMEM_SPEC, HBM_SPEC],
        out_specs=(HBM_SPEC, HBM_SPEC),
        scratch_shapes=[
            pltpu.VMEM((2 * length, width), jnp.bfloat16),
            pltpu.VMEM((2, 2, length // 2, width), jnp.bfloat16),
            pltpu.SemaphoreType.DMA((3,)),
        ],
        cost_estimate=cost(3),
        compiler_params=params(None, FULL),
        name="unsort_rows",
    )(ids, order, *in_hbm(values))


SPAN = 5 * TILE
TURN = 6 * TILE


def bucket_onehot():
    distance = lax.broadcasted_iota(jnp.int32, (BUCKETS, TURN), 1) - (3 * TILE - 1)
    magnitude = jnp.abs(distance)
    counted = jnp.zeros(distance.shape, jnp.int32)
    for limit in limits:
        counted = counted + (magnitude >= limit).astype(jnp.int32)
    bucket = counted + 16 * (distance > 0).astype(jnp.int32)
    return bucket == lax.broadcasted_iota(jnp.int32, distance.shape, 0)


def block_flip(ids, own, far, block, count):
    place = ids[HALF] if own else 1 - ids[HALF]
    first = jnp.where(place == 0, 1, 2)
    high = count // 2
    flip = jnp.int32(4 * (block % high))
    if block >= high:
        flip = flip ^ first
    return flip ^ (3 - first) if far else flip


def block_places(ids, pieces):
    places = []
    for index, piece in enumerate(pieces):
        own = index < len(pieces) // 2
        place = ids[HALF] if own else 1 - ids[HALF]
        for block in range(piece.shape[0]):
            if len(pieces) == 2:
                places.append((index, block, place, 0))
            else:
                flip = block_flip(ids, own, index % 2 == 1, block, piece.shape[0])
                places.append((index, block, place, ids[ME] ^ flip))
    return places


def block_copies(ids, pieces, target, sems, tiles):
    copies = []
    for index, block, place, chip in block_places(ids, pieces):
        rows = pieces[index].shape[2]
        here = pl.ds(pl.multiple_of(chip * rows, rows), rows)
        copies.append(
            pltpu.make_async_copy(
                pieces[index].at[block, tiles], target.at[place, :, here, :],
                sems.at[len(copies)],
            )
        )
    return copies


def block_stores(ids, source, outs, sems, tiles):
    copies = []
    for index, block, place, chip in block_places(ids, outs):
        rows = outs[index].shape[2]
        here = pl.ds(pl.multiple_of(chip * rows, rows), rows)
        copies.append(
            pltpu.make_async_copy(
                source.at[place, :, here, :], outs[index].at[block, tiles],
                sems.at[len(copies)],
            )
        )
    return copies


def joined(weights, index):
    return jnp.concatenate([weights[0, index], weights[1, index]], axis=1)


def store_shapes(pieces, tiles):
    return tuple(SDS((p.shape[0], tiles) + p.shape[2:], jnp.bfloat16) for p in pieces)


def vectors_kernel(width, sizes, ids, near, far, rows_out, up_out, bias_out):
    count = 2 * near.shape[0]
    half = ids[HALF]
    high = count // 4
    total = jnp.zeros((16, width), jnp.float32)
    table = jnp.zeros((16, width), jnp.float32)
    blank = jnp.zeros((16, width - 256), jnp.float32)
    slot = lax.broadcasted_iota(jnp.int32, (16, width), 0)
    blocks = [[], []]
    for side, part in enumerate((near, far)):
        for block in range(part.shape[0]):
            chip = ids[ME] ^ block_flip(ids, True, side == 1, block, part.shape[0])
            values = jnp.concatenate([part[block].astype(jnp.float32), blank], axis=1)
            blocks[side].append(values)
            total = total + pltpu.roll(
                jnp.where(slot < UP_SLOT, values, 0.0), chip * sizes[0], 1
            )
            table = table + pltpu.roll(
                jnp.where(slot == TABLE_SLOT, values, 0.0), chip * sizes[TABLE_SLOT], 1
            )
    rows_out[...] = total[2:10, :]
    rows_out[6:8, :] = total[0:2, :]
    share = sizes[UP_SLOT] // 2
    lane = lax.broadcasted_iota(jnp.int32, (16, width), 1)
    keep = (slot == UP_SLOT) & (lane < share)
    near_blocks, far_blocks = blocks
    order = (
        (half, near_blocks[:high] + near_blocks[high:]),
        (1 - half, near_blocks[:high] + far_blocks[:high]),
        (half, far_blocks[:high] + far_blocks[high:]),
        (1 - half, near_blocks[high:] + far_blocks[high:]),
    )
    for index, (place, parts) in enumerate(order):
        joint = jnp.zeros((16, width), jnp.float32)
        for block, values in enumerate(parts):
            values = pltpu.roll(values, lax.rem(width - place * share, width), 1)
            joint = joint + pltpu.roll(jnp.where(keep, values, 0.0), block * share, 1)
        up_out[:, index * width : (index + 1) * width] = joint[UP_SLOT : UP_SLOT + 1, :]
    flat = table[TABLE_SLOT : TABLE_SLOT + 1, : BUCKETS * HEADS]
    entry = lax.broadcasted_iota(jnp.int32, (16, BUCKETS * HEADS), 1)
    head = lax.broadcasted_iota(jnp.int32, (16, BUCKETS * HEADS), 0)
    spread_heads = jnp.where(entry % HEADS == head, flat, 0.0).astype(jnp.bfloat16)
    place = lax.broadcasted_iota(jnp.int32, (BUCKETS, BUCKETS * HEADS), 1) // HEADS
    bucket = lax.broadcasted_iota(jnp.int32, (BUCKETS, BUCKETS * HEADS), 0)
    folded = product(spread_heads, jnp.where(place == bucket, 1.0, 0.0).astype(jnp.bfloat16), NT)
    onehot = jnp.where(bucket_onehot(), 1.0, 0.0).astype(jnp.bfloat16)
    rows = product(folded.astype(jnp.bfloat16), onehot)
    for head in range(HEADS):
        spread = jnp.broadcast_to(rows[head : head + 1, :], (TILE, TURN))
        turned = pltpu.roll(spread, TURN - (TILE - 1), 1, stride=1, stride_axis=0)
        bias_out[head] = turned[:, :SPAN].astype(jnp.bfloat16)


def vectors_to_all(ids, near, far, width, sizes):
    return pl.pallas_call(
        functools.partial(vectors_kernel, width, sizes),
        out_shape=(
            SDS((8, width), jnp.float32),
            SDS((1, 4 * width), jnp.float32),
            SDS((HEADS, TILE, SPAN), jnp.bfloat16),
        ),
        in_specs=[SMEM_SPEC] + [VMEM_SPEC] * 2,
        out_specs=(VMEM_SPEC,) * 3,
        cost_estimate=cost(6),
        compiler_params=params(None, FULL),
        name="vectors",
    )(ids, near, far)


def head_lanes(head, shape):
    lane = lax.broadcasted_iota(jnp.int32, shape, 1)
    return (lane >= head * HEAD_DIM) & (lane < (head + 1) * HEAD_DIM)


def head_stack(values):
    low = jnp.zeros((), values.dtype)
    return jnp.concatenate(
        [jnp.where(head_lanes(h, values.shape), values, low) for h in range(GROUP)]
    )


def head_merge(stack, rows):
    total = stack[(GROUP - 1) * rows :, :]
    for h in range(GROUP - 1):
        part = stack[h * rows : (h + 1) * rows, :]
        total = jnp.where(head_lanes(h, part.shape), part, total)
    return total


def widen(values, lanes):
    return jnp.concatenate([values] * (lanes // 128), axis=1)


def by_width(ids, lengths, tile, body):
    half = ids[HALF]
    begin, end = tile * TILE, (tile + 1) * TILE
    bound = jnp.int32(0)
    low, high = jnp.int32(0), jnp.int32(TILES * TILE)
    for index in range(lengths.shape[1] - 1):
        bound = bound + lengths[half, index]
        low = jnp.where(bound <= begin, bound, low)
        high = jnp.where(bound >= end, jnp.minimum(bound, high), high)
    first = low // TILE
    width = jnp.maximum((high + TILE - 1) // TILE - first, 2)
    first = pl.multiple_of(jnp.minimum(first, TILES - width) * TILE, TILE)
    for count in range(2, TILES + 1):
        pl.when(width == count)(functools.partial(body, first, count * TILE))


def attend_kernel(ids, lengths, xs, mask, bias, rows, *rest):
    pieces, rest = rest[:-8], rest[-8:]
    q_out, k_out, v_out, mixed_out, lse_out, weights, values, sems = rest
    length = mask.shape[1]
    group = pl.program_id(0)

    def weight_copies(index):
        tiles = pl.ds(3 * index, 3)
        return block_copies(ids, pieces, weights.at[:, tiles], sems.at[index], tiles)

    @pl.when(group == 0)
    def _():
        for index in range(GROUPS):
            for copy in weight_copies(index):
                copy.start()

    for index in range(GROUPS):
        @pl.when(group == index)
        def _():
            for copy in weight_copies(index):
                copy.wait()

    q = product(xs[...], joined(weights, 3 * group)) + rows[6:7, :]
    q_out[...] = q.astype(jnp.bfloat16)
    k = product(xs[0:length, :], joined(weights, 3 * group + 1))
    k_out[...] = k.astype(jnp.bfloat16)
    v = product(xs[0:length, :], joined(weights, 3 * group + 2)) + rows[7:8, :]
    v_out[...] = v.astype(jnp.bfloat16)

    wide_lanes = lax.broadcasted_iota(jnp.int32, v.shape, 1) < 128
    one = jnp.ones((), jnp.bfloat16)
    values[0] = jnp.where(wide_lanes, v_out[...], one)
    values[1] = jnp.where(wide_lanes, one, v_out[...])

    def tile_step(tile, carry):
        def body(first, keys):
            there = pl.ds(first, keys)
            near = pl.ds(pl.multiple_of((2 - tile) * TILE + first, TILE), keys)
            here = pl.ds(pl.multiple_of(tile * TILE, TILE), TILE)
            key = k_out[there, :]
            for stream in range(2):
                at = pl.ds(pl.multiple_of(stream * length + tile * TILE, TILE), TILE)
                scores = product(head_stack(q_out[at, :] * jnp.bfloat16(0.125)), key, NT)
                masked = mask[stream, here, there].astype(jnp.float32)
                weights, peaks, logs = [], [], []
                for h in range(GROUP):
                    part = scores[h * TILE : (h + 1) * TILE, :] + bias[h, :, near].astype(jnp.float32) + masked
                    peak = jnp.maximum(jnp.max(part, axis=-1, keepdims=True), FLOOR)
                    weights.append(jnp.exp(part - peak).astype(jnp.bfloat16))
                    peaks.append(peak)
                for pair in range(2):
                    both = jnp.concatenate(weights[2 * pair : 2 * pair + 2])
                    both = product(both, values[pair, there, :])
                    top = slice(pair * 128, pair * 128 + 128)
                    low = slice(128 - pair * 128, 256 - pair * 128)
                    parts = []
                    for h in range(2):
                        rows = slice(h * TILE, (h + 1) * TILE)
                        summed = both[rows, low]
                        alive = summed > 0
                        inverse = jnp.where(alive, 1.0 / summed, 0.0)
                        parts.append(both[rows, top] * inverse)
                        logs.append(
                            jnp.where(alive, peaks[2 * pair + h] + jnp.log(summed), 0.0)
                        )
                    lane = lax.broadcasted_iota(jnp.int32, parts[0].shape, 1)
                    mixed = jnp.where(lane < HEAD_DIM, parts[0], parts[1])
                    mixed_out[at, top] = mixed.astype(jnp.bfloat16)
                packed = logs[0]
                for h in range(1, GROUP):
                    packed = jnp.where(lane == h, logs[h], packed)
                lse_out[0, at, :] = packed

        by_width(ids, lengths, tile, body)
        return carry

    lax.fori_loop(0, length // TILE, tile_step, 0)


def attend(ids, lengths, xs, mask, bias, rows, pieces):
    tokens, width = xs.shape
    length = mask.shape[1]
    blocks = sum(piece.shape[0] for piece in pieces)
    full = lambda g: (0, 0)
    column = lambda g: (0, g)
    once = pl.Buffered(1)
    return pl.pallas_call(
        attend_kernel,
        grid=(GROUPS,),
        out_shape=(
            SDS((tokens, width), jnp.bfloat16),
            SDS((length, width), jnp.bfloat16),
            SDS((length, width), jnp.bfloat16),
            SDS((tokens, width), jnp.bfloat16),
            SDS((GROUPS, tokens, 128), jnp.float32),
        ),
        in_specs=[
            SMEM_SPEC,
            SMEM_SPEC,
            pl.BlockSpec((tokens, width), full, pipeline_mode=once),
            pl.BlockSpec((2, length, length), lambda g: (0, 0, 0), pipeline_mode=once),
            pl.BlockSpec((GROUP, TILE, SPAN), lambda g: (g, 0, 0)),
            pl.BlockSpec((8, LANES), column),
        ] + [HBM_SPEC] * len(pieces),
        out_specs=(
            pl.BlockSpec((tokens, LANES), column),
            pl.BlockSpec((length, LANES), column),
            pl.BlockSpec((length, LANES), column),
            pl.BlockSpec((tokens, LANES), column),
            pl.BlockSpec((1, tokens, 128), lambda g: (g, 0, 0)),
        ),
        scratch_shapes=[
            pltpu.VMEM((2, 3 * GROUPS, width, 128), jnp.bfloat16),
            pltpu.VMEM((2, length, LANES), jnp.bfloat16),
            pltpu.SemaphoreType.DMA((GROUPS, blocks)),
        ],
        cost_estimate=cost(18),
        compiler_params=params(("arbitrary",), FULL),
        name="attend",
    )(ids, lengths, xs, mask, bias, rows, *in_hbm(*pieces))


def norm_parts(values):
    mean = jnp.mean(values, axis=-1, keepdims=True)
    center = values - mean
    spread = jnp.mean(center * center, axis=-1, keepdims=True)
    scale = lax.rsqrt(spread + EPS)
    return center * scale, scale


def norm_back(normal, scale, grad):
    mean = jnp.mean(grad, axis=-1, keepdims=True)
    inner = jnp.mean(grad * normal, axis=-1, keepdims=True)
    return scale * (grad - mean - normal * inner)


def column_sum(values):
    return jnp.sum(values, axis=0, keepdims=True)


BLOCK = 256


def feed_kernel(ids, xs, mixed, cot, rows, up_bias, near_own, near_other, far_own, far_other,
                *rest):
    pieces, rest = rest[:-14], rest[-14:]
    (out, act_out, gup_out, first_out, gdown_out, gres_out, gbranch_out, gmixed_out,
     sums, up_sums, up_all, down_all, wo_all, sems) = rest
    step = pl.program_id(0)
    units = up_all.shape[0] // 4
    parts = (near_own, near_other, far_own, far_other)

    @pl.when(step == 0)
    def _():
        sums[...] = jnp.zeros_like(sums)
        up_sums[...] = jnp.zeros_like(up_sums)
        copies = block_copies(ids, pieces, wo_all, sems, slice(3 * GROUPS, 4 * GROUPS))
        share = near_own.shape[2]
        for index, part in enumerate(parts):
            for block in range(part.shape[0]):
                here = slice(index * units + block * share, index * units + (block + 1) * share)
                for which, target in ((0, up_all), (1, down_all)):
                    copies.append(
                        pltpu.make_async_copy(
                            part.at[block, which], target.at[here, :], sems.at[len(copies)]
                        )
                    )
        run_copies(copies)

    wo = jnp.concatenate([joined(wo_all, index) for index in range(GROUPS)], axis=1)
    branch = product(mixed[...], wo) + rows[0:1, :]
    normal1, scale1 = norm_parts(xs[...].astype(jnp.float32) + branch)
    first = normal1 * rows[1:2, :] + rows[2:3, :]
    first_low = first.astype(jnp.bfloat16)
    first_out[...] = first_low
    slopes = []
    second = first + rows[3:4, :]
    for index in range(2):
        here = slice(2 * index * units, 2 * (index + 1) * units)
        up = product(first_low, up_all[here, :], NT) + up_bias[:, here]
        gate = 0.5 + 0.5 * lax.erf(up * math.sqrt(0.5))
        act = (up * gate).astype(jnp.bfloat16)
        act_out[:, here] = act
        slopes.append(gate + up * jnp.exp(-0.5 * up * up) * (1.0 / math.sqrt(2.0 * math.pi)))
        second = second + product(act, down_all[here, :])
    normal2, scale2 = norm_parts(second)
    gain = rows[4:5, :]
    out[...] = (normal2 * gain + rows[5:6, :]).astype(jnp.bfloat16)
    cots = cot[...].astype(jnp.float32)
    gsecond = norm_back(normal2, scale2, cots * gain)
    gdown = gsecond.astype(jnp.bfloat16)
    gdown_out[...] = gdown
    gfirst = gsecond
    for index in range(2):
        here = slice(2 * index * units, 2 * (index + 1) * units)
        gup = (product(gdown, down_all[here, :], NT) * slopes[index]).astype(jnp.bfloat16)
        gup_out[:, here] = gup
        up_sums[:, here] += column_sum(gup.astype(jnp.float32))
        gfirst = gfirst + product(gup, up_all[here, :])
    gres = norm_back(normal1, scale1, gfirst * rows[1:2, :])
    gres_out[...] = gres
    gbranch = gres.astype(jnp.bfloat16)
    gbranch_out[...] = gbranch
    gmixed_out[...] = product(gbranch, wo, NT).astype(jnp.bfloat16)
    sums[0:1, :] += column_sum(gbranch.astype(jnp.float32))
    sums[1:2, :] += column_sum(gfirst * normal1)
    sums[2:3, :] += column_sum(gfirst)
    sums[3:4, :] += column_sum(gdown.astype(jnp.float32))
    sums[4:5, :] += column_sum(cots * normal2)
    sums[5:6, :] += column_sum(cots)


def feed(ids, xs, mixed, cot, rows, up_bias, feeds, pieces):
    tokens, width = xs.shape
    hidden = up_bias.shape[1]
    token = pl.BlockSpec((BLOCK, width), lambda i: (i, 0))
    wide = pl.BlockSpec((BLOCK, hidden), lambda i: (i, 0))
    held = sum(piece.shape[0] for piece in pieces) + 2 * sum(part.shape[0] for part in feeds)
    low = SDS((tokens, width), jnp.bfloat16)
    return pl.pallas_call(
        feed_kernel,
        grid=(tokens // BLOCK,),
        out_shape=(
            low,
            SDS((tokens, hidden), jnp.bfloat16),
            SDS((tokens, hidden), jnp.bfloat16),
            low,
            low,
            SDS((tokens, width), jnp.float32),
            low,
            low,
            SDS((8, width), jnp.float32),
            SDS((1, hidden), jnp.float32),
        ),
        in_specs=[
            SMEM_SPEC, token, token, token,
            pl.BlockSpec((8, width), lambda i: (0, 0)),
            pl.BlockSpec((1, hidden), lambda i: (0, 0)),
        ] + [HBM_SPEC] * (4 + len(pieces)),
        out_specs=(token, wide, wide, token, token, token, token, token,
                   pl.BlockSpec((8, width), lambda i: (0, 0)),
                   pl.BlockSpec((1, hidden), lambda i: (0, 0))),
        scratch_shapes=[
            pltpu.VMEM((hidden, width), jnp.bfloat16),
            pltpu.VMEM((hidden, width), jnp.bfloat16),
            pltpu.VMEM((2, GROUPS, width, 128), jnp.bfloat16),
            pltpu.SemaphoreType.DMA((held,)),
        ],
        cost_estimate=cost(36),
        compiler_params=params(("arbitrary",), FULL),
        name="feed",
    )(ids, xs, mixed, cot, rows, up_bias, *in_hbm(*feeds, *pieces))


def feed_weights_kernel(act, gup, first, gdown, own, other):
    which = pl.program_id(1)

    def put(grad):
        share = own.shape[2]
        grad = grad.astype(jnp.bfloat16)

        def store(out):
            for block in range(out.shape[0]):
                out[block, 0] = grad[block * share : (block + 1) * share, :]

        pl.when(pl.program_id(0) == 0)(lambda: store(other))
        pl.when(pl.program_id(0) == 1)(lambda: store(own))

    pl.when(which == 0)(lambda: put(product(gup[...], first[...], TN)))
    pl.when(which == 1)(lambda: put(product(act[...], gdown[...], TN)))


def feed_weights(part, act, gup, first, gdown, shape):
    tokens, width = first.shape
    units = shape[0] * shape[2]
    full = pl.BlockSpec((tokens, width), lambda s, u: (0, 0), pipeline_mode=pl.Buffered(1))
    lanes = pl.BlockSpec((tokens, units), lambda s, u: (0, 2 * part + 1 - s))
    block = (shape[0], 1) + shape[2:]
    return pl.pallas_call(
        feed_weights_kernel,
        grid=(2, 2),
        out_shape=(SDS(shape, jnp.bfloat16),) * 2,
        in_specs=[lanes, lanes, full, full],
        out_specs=(
            pl.BlockSpec(block, lambda s, u: (0, s * u, 0, 0)),
            pl.BlockSpec(block, lambda s, u: (0, jnp.maximum(s, u), 0, 0)),
        ),
        cost_estimate=cost(9),
        compiler_params=params(("arbitrary", "arbitrary"), FULL),
        name="feed_weights",
    )(act, gup, first, gdown)


def out_weights_kernel(ids, mixed, gbranch, *rest):
    outs, (buffer, sems) = rest[:-2], rest[-2:]
    grad = product(mixed[...], gbranch[...], TN).astype(jnp.bfloat16)
    for index in range(GROUPS):
        for half in range(2):
            lane = index * LANES + half * 128
            buffer[half, index] = grad[:, lane : lane + 128]
    run_copies(block_stores(ids, buffer, outs, sems, slice(3 * GROUPS, 4 * GROUPS)))


def out_weights(ids, mixed, gbranch, pieces):
    tokens, width = mixed.shape
    blocks = sum(piece.shape[0] for piece in pieces)
    full = pl.BlockSpec((tokens, width), lambda i: (0, 0))
    return pl.pallas_call(
        out_weights_kernel,
        grid=(1,),
        out_shape=store_shapes(pieces, GRAD_TILES),
        in_specs=[SMEM_SPEC, full, full],
        out_specs=(HBM_SPEC,) * len(pieces),
        scratch_shapes=[
            pltpu.VMEM((2, GROUPS, width, 128), jnp.bfloat16),
            pltpu.SemaphoreType.DMA((blocks,)),
        ],
        cost_estimate=cost(4),
        compiler_params=params(("arbitrary",), FULL),
        name="out_weights",
    )(ids, mixed, gbranch)


def attend_back_kernel(ids_rows, ids, lengths, order, mask, bias, q, k, v, mixed, gmixed, lse, sums,
                       up_sums, xs_far, gres, *rest):
    scratch = rest[-17:]
    count = (len(rest) - 17 - 2) // 3
    pieces = rest[:count]
    own, send, *gw_outs = rest[2 * count : -17]
    (vectors, turned, vector_sems, gk, gv, gdist, gx, gq, inner, weights, buffer, xs, rows_out, sems, in_sems, out_sems,
     row_sems) = scratch
    group = pl.program_id(0)
    length = mask.shape[1]
    rows = xs.shape[1] // (2 * gw_outs[0].shape[0]) if count > 2 else ids_rows
    loads = block_copies(ids, pieces, weights, sems, slice(0, 3 * GROUPS)) + [
        pltpu.make_async_copy(xs_far, xs, in_sems.at[0]),
        pltpu.make_async_copy(gres, gx, in_sems.at[1]),
    ]

    def stores(index):
        slot = index % 2
        return block_stores(
            ids, buffer.at[slot], gw_outs, out_sems.at[slot], pl.ds(3 * index, 3)
        )

    @pl.when(group == 0)
    def _():
        for copy in loads:
            copy.start()

    gdist[...] = jnp.zeros_like(gdist)
    gk[...] = jnp.zeros_like(gk)
    gv[...] = jnp.zeros_like(gv)

    lane = lax.broadcasted_iota(jnp.int32, (LANES, GROUP * 128), 0) // HEAD_DIM
    head = lax.broadcasted_iota(jnp.int32, (LANES, GROUP * 128), 1) // 128
    adder = jnp.where(lane == head, 1.0, 0.0).astype(jnp.bfloat16)
    crossed = mixed[...].astype(jnp.float32) * gmixed[...].astype(jnp.float32)
    inner[...] = product(crossed.astype(jnp.bfloat16), adder)

    def tile_step(tile, carry):
        def body(first, keys):
            there = pl.ds(first, keys)
            near = pl.ds(pl.multiple_of((2 - tile) * TILE + first, TILE), keys)
            here = pl.ds(pl.multiple_of(tile * TILE, TILE), TILE)
            key = k[there, :]
            value = v[there, :]
            at = [
                pl.ds(pl.multiple_of(stream * length + tile * TILE, TILE), TILE)
                for stream in range(2)
            ]
            query = jnp.concatenate([head_stack(q[at[s], :] * jnp.bfloat16(0.125)) for s in range(2)])
            gmix = jnp.concatenate([head_stack(gmixed[at[s], :]) for s in range(2)])
            scores = product(query, key, NT)
            gprobs = product(gmix, value, NT)
            masked = [mask[s, here, there].astype(jnp.float32) for s in range(2)]
            probs_low = [None] * (2 * GROUP)
            gscores_low = [None] * (2 * GROUP)
            for h in range(GROUP):
                both = None
                near_bias = bias[h, :, near].astype(jnp.float32)
                for stream in range(2):
                    index = stream * GROUP + h
                    part = slice(index * TILE, (index + 1) * TILE)
                    score = scores[part, :] + near_bias + masked[stream]
                    probs = jnp.exp(score - lse[0, at[stream], h : h + 1])
                    lanes = slice(h * 128, (h + 1) * 128)
                    gscores = probs * (gprobs[part, :] - widen(inner[at[stream], lanes], keys))
                    probs_low[index] = probs.astype(jnp.bfloat16)
                    gscores_low[index] = gscores.astype(jnp.bfloat16)
                    both = gscores if both is None else both + gscores
                gdist[h, :, near] += both
            probs_low = jnp.concatenate(probs_low)
            gscores_low = jnp.concatenate(gscores_low)
            gv[there, :] += product(probs_low, gmix, TN)
            gk[there, :] += product(gscores_low, query, TN)
            back = product(gscores_low, key)
            for stream in range(2):
                part = slice(stream * GROUP * TILE, (stream + 1) * GROUP * TILE)
                gq[at[stream], :] = head_merge(back[part, :], TILE)

        by_width(ids, lengths, tile, body)
        return carry

    lax.fori_loop(0, length // TILE, tile_step, 0)
    gq_low = (gq[...] * 0.125).astype(jnp.bfloat16)
    gk_low = gk[...].astype(jnp.bfloat16)
    gv_low = gv[...].astype(jnp.bfloat16)

    @pl.when(group == 0)
    def _():
        for copy in loads:
            copy.wait()

    @pl.when(group == 2)
    def _():
        for copy in stores(0):
            copy.wait()

    slot = lax.rem(group, 2)
    for index, grad in enumerate((
        product(xs[...], gq_low, TN),
        product(xs[0:length, :], gk_low, TN),
        product(xs[0:length, :], gv_low, TN),
    )):
        grad = grad.astype(jnp.bfloat16)
        buffer[slot, 0, index] = grad[:, :128]
        buffer[slot, 1, index] = grad[:, 128:]
    for index in range(GROUPS):
        @pl.when(group == index)
        def _():
            for copy in stores(index):
                copy.start()

    gx[...] += product(gq_low, joined(weights, 3 * group), NT)
    gx[0:length, :] += product(gk_low, joined(weights, 3 * group + 1), NT) + product(
        gv_low, joined(weights, 3 * group + 2), NT
    )
    lanes = pl.ds(pl.multiple_of(group * LANES, LANES), LANES)
    vectors[0:1, lanes] = column_sum(gq_low.astype(jnp.float32))
    vectors[1:2, lanes] = column_sum(gv_low.astype(jnp.float32))
    span = TURN
    pieces_sum = []
    row_index = lax.broadcasted_iota(jnp.int32, (8, span), 0)
    for h in range(GROUP):
        wide = jnp.concatenate([gdist[h], jnp.zeros((TILE, TILE), jnp.float32)], axis=1)
        size = TILE // 2
        while size >= 8:
            wide = wide[size:, :] + pltpu.roll(wide[:size, :], size, 1)
            size //= 2
        for bit in (4, 2, 1):
            wide = jnp.where(row_index & bit == 0, pltpu.roll(wide, bit, 1), wide)
        pieces_sum.append(column_sum(wide))
    pieces_sum.append(jnp.zeros((8 - GROUP, span), jnp.float32))
    onehot = jnp.where(bucket_onehot(), 1.0, 0.0)
    by_bucket = lax.dot_general(
        jnp.concatenate(pieces_sum, axis=0), onehot, NT, precision=lax.Precision.HIGHEST,
        preferred_element_type=jnp.float32,
    )
    width = xs.shape[1]
    parts = width // rows
    each = BUCKETS * HEADS // parts
    lane = lax.broadcasted_iota(jnp.int32, (BUCKETS, width), 1)
    entry = lane // rows * each + lane % rows
    bucket = lax.broadcasted_iota(jnp.int32, (BUCKETS, width), 0)
    chosen = (entry // HEADS == bucket) & (lane % rows < each)
    table = lax.dot_general(
        by_bucket, jnp.where(chosen, 1.0, 0.0), NN, precision=lax.Precision.HIGHEST,
        preferred_element_type=jnp.float32,
    )
    head = lax.broadcasted_iota(jnp.int32, table.shape, 0)
    lane = lax.broadcasted_iota(jnp.int32, table.shape, 1)
    entry = lane // rows * each + lane % rows
    right = (head < GROUP) & (entry % HEADS == GROUP * group + head)
    table = column_sum(jnp.where(right, table, 0.0))

    @pl.when(group == 0)
    def _():
        vectors[12:13, :] = table

    @pl.when(group > 0)
    def _():
        vectors[12:13, :] += table

    @pl.when(group == GROUPS - 1)
    def _():
        put_back(
            ids, order_onehot(ids, order),
            lambda s: gx[s * length : (s + 1) * length, :].astype(jnp.bfloat16),
            rows_out, own, send, row_sems,
        )
        vectors[2:8, :] = sums[0:6, :]
        vectors[8:12, :] = up_slots(ids, up_sums, rows, parts // 2)
        vectors[13:, :] = jnp.zeros((128 - 13, width), jnp.float32)
        tile = jnp.transpose(vectors[...]).astype(jnp.bfloat16)
        turned[0, 0] = tile
        turned[1, 0] = tile
        last = block_stores(
            ids, turned, gw_outs, vector_sems, slice(VECTOR_TILE, VECTOR_TILE + 1)
        )
        for copy in last:
            copy.start()
        for copy in stores(1) + stores(2) + last:
            copy.wait()


def up_slots(ids, up_sums, rows, blocks):
    width = up_sums.shape[1] // 4
    share = 2 * rows
    slot = lax.broadcasted_iota(jnp.int32, (8, width), 0)
    lane = lax.broadcasted_iota(jnp.int32, (8, width), 1)
    total = jnp.zeros((8, width), jnp.float32)
    for index in range(4):
        own = index % 2 == 0
        place = ids[HALF] if own else 1 - ids[HALF]
        part = jnp.broadcast_to(up_sums[:, index * width : (index + 1) * width], (8, width))
        for block in range(blocks):
            chip = ids[ME] ^ block_flip(ids, own, index >= 2, block, blocks)
            for quarter in range(2):
                shift = (width - block * share - quarter * rows) % width
                values = pltpu.roll(part, shift, 1) if shift else part
                keep = (lane < rows) & (slot == 2 * place + quarter)
                total = total + pltpu.roll(jnp.where(keep, values, 0.0), chip * rows, 1)
    return total[0:4, :]


def attend_back(ids, lengths, order, xs, mask, bias, q, k, v, mixed, gmixed, lse, sums, up_sums,
                gres, pieces, grads, rows_each):
    tokens, width = xs.shape
    length = mask.shape[1]
    blocks = sum(piece.shape[0] for piece in pieces)
    column = lambda g: (0, g)
    rows = SDS((2, length // 2, width), jnp.bfloat16)
    first = 15 + len(pieces)
    return pl.pallas_call(
        functools.partial(attend_back_kernel, rows_each),
        grid=(GROUPS,),
        out_shape=(
            rows,
            rows,
        ) + store_shapes(pieces, GRAD_TILES),
        input_output_aliases={first + index: 2 + index for index in range(len(pieces))},
        in_specs=[
            SMEM_SPEC,
            SMEM_SPEC,
            VMEM_SPEC,
            pl.BlockSpec((2, length, length), lambda g: (0, 0, 0), pipeline_mode=pl.Buffered(1)),
            pl.BlockSpec((GROUP, TILE, SPAN), lambda g: (g, 0, 0)),
            pl.BlockSpec((tokens, LANES), column),
            pl.BlockSpec((length, LANES), column),
            pl.BlockSpec((length, LANES), column),
            pl.BlockSpec((tokens, LANES), column),
            pl.BlockSpec((tokens, LANES), column),
            pl.BlockSpec((1, tokens, 128), lambda g: (g, 0, 0)),
            pl.BlockSpec((8, width), lambda g: (0, 0)),
            pl.BlockSpec((1, 4 * width), lambda g: (0, 0)),
        ] + [HBM_SPEC] * (2 + 2 * len(pieces)),
        out_specs=(HBM_SPEC,) * (2 + len(pieces)),
        scratch_shapes=[
            pltpu.VMEM((128, width), jnp.float32),
            pltpu.VMEM((2, 1, width, 128), jnp.bfloat16),
            pltpu.SemaphoreType.DMA((blocks,)),
            pltpu.VMEM((length, LANES), jnp.float32),
            pltpu.VMEM((length, LANES), jnp.float32),
            pltpu.VMEM((GROUP, TILE, SPAN), jnp.float32),
            pltpu.VMEM((tokens, width), jnp.float32),
            pltpu.VMEM((tokens, LANES), jnp.float32),
            pltpu.VMEM((tokens, GROUP * 128), jnp.float32),
            pltpu.VMEM((2, 3 * GROUPS, width, 128), jnp.bfloat16),
            pltpu.VMEM((2, 2, 3, width, 128), jnp.bfloat16),
            pltpu.VMEM((tokens, width), jnp.bfloat16),
            pltpu.VMEM((2, 2, length // 2, width), jnp.bfloat16),
            pltpu.SemaphoreType.DMA((blocks,)),
            pltpu.SemaphoreType.DMA((2,)),
            pltpu.SemaphoreType.DMA((2, blocks)),
            pltpu.SemaphoreType.DMA((2,)),
        ],
        cost_estimate=cost(27),
        compiler_params=params(("arbitrary",), FULL),
        name="attend_back",
    )(ids, lengths, order, mask, bias, q, k, v, mixed, gmixed, lse, sums, up_sums,
      *in_hbm(xs, gres, *pieces, *grads))


def finish_kernel(ids, own, came, wq, wk, wv, wo, *vectors):
    half = ids[HALF]
    for place in range(2):
        mine = half == place
        for index, out in enumerate((wq, wk, wv, wo)):
            for group in range(GROUPS):
                tile = 3 * group + index if index < 3 else 3 * GROUPS + group
                lane = group * LANES + place * 128
                out[:, lane : lane + 128] = jnp.where(mine, own[tile], came[tile])
    turned = jnp.transpose(own[VECTOR_TILE])
    rows = own.shape[1]
    for index, out in enumerate(vectors):
        if index == UP_SLOT:
            for quarter in range(4):
                out[:, quarter * rows : (quarter + 1) * rows] = turned[8 + quarter : 9 + quarter, :]
        else:
            at = 12 if index == TABLE_SLOT else index
            out[...] = turned[at : at + 1, : out.shape[1]]


def finish(ids, own, came, sizes):
    rows = own.shape[1]
    width = LANES * GROUPS
    outs = (SDS((rows, width), jnp.float32),) * 4
    outs += tuple(SDS((1, size), jnp.float32) for size in sizes)
    return pl.pallas_call(
        finish_kernel,
        out_shape=outs,
        in_specs=[SMEM_SPEC, VMEM_SPEC, VMEM_SPEC],
        out_specs=(VMEM_SPEC,) * len(outs),
        cost_estimate=cost(2),
        compiler_params=params(None, FULL),
        name="finish",
    )(ids, own, came)


BOTH = ("dp", "seq")


def xor_pairs(count, by_half):
    halves = len(by_half)
    return [
        (device * halves + half, (device ^ flip) * halves + half)
        for device in range(count)
        for half, flip in enumerate(by_half)
    ]


def swap(value):
    return lax.ppermute(value, "seq", [(0, 1), (1, 0)])


def high_parts(value, count):
    return [
        lax.ppermute(value, BOTH, xor_pairs(count, (4 * high, 4 * high)))
        for high in range(1, count // 4)
    ]


def low_round(value, count):
    return jnp.concatenate([value, lax.ppermute(value, BOTH, xor_pairs(count, (1, 2)))])


def last_round(value, count):
    return lax.ppermute(value, BOTH, xor_pairs(count, (2, 1)))


def offsets(count, half):
    first = jnp.where(half == 0, 1, 2)
    highs = 4 * jnp.arange(count // 4)
    near = jnp.concatenate([highs, highs ^ first])
    return jnp.concatenate([near, near ^ (3 - first)])


def after(value, *others):
    return lax.optimization_barrier((value,) + others)[0]


def wide(value):
    return value.astype(jnp.float32)


def low(value):
    return value.astype(jnp.bfloat16)


def in_order(half, own, other):
    return jnp.where(half == 0, jnp.stack([own, other]), jnp.stack([other, own]))


def shards(count, content, query_in, content_cot, query_cot, lengths, order, query_weight,
           query_bias, key_weight, value_weight, value_bias, out_weight, out_bias, mixer_gain,
           mixer_shift, up_weight, up_bias, down_weight, down_bias, final_gain, final_shift,
           position_bias):
    _, block, width = content.shape
    length = order.shape[1]
    half = lax.axis_index("seq")
    me = lax.axis_index("dp")
    rows = query_weight.shape[0]
    hidden = up_weight.shape[1]
    share = hidden // 2
    near_count = count // 2

    ids = jnp.stack([me, half]).astype(jnp.int32)
    vectors = (query_bias, value_bias, out_bias, mixer_gain, mixer_shift, down_bias, final_gain,
               final_shift, up_bias, position_bias)
    sizes = [vector.shape[0] for vector in vectors]
    theirs, square, feed_own, slots = pack(
        ids, content, query_in, content_cot, query_cot, query_weight, key_weight, value_weight,
        out_weight, up_weight, down_weight, vectors,
    )

    square_parts = high_parts(square, count)
    slots_high = jnp.stack([slots] + high_parts(slots, count))
    came = swap(theirs)
    xs, cs, mask = sort_rows(
        ids, lengths, (content, query_in, content_cot, query_cot), came, order
    )
    square_parts = lax.optimization_barrier((square_parts, xs, slots_high))[0]
    square_near = low_round(jnp.stack([square] + square_parts), count)
    feed_own = after(feed_own, square_parts)
    feed_parts = high_parts(feed_own, count)
    slots_near = low_round(slots_high, count)
    square_near = after(square_near, slots_near)
    square_far = last_round(square_near, count)
    slots_far = last_round(slots_near, count)
    near_swapped = swap(square_near)
    square_far = after(square_far, slots_far, near_swapped)
    far_swapped = swap(square_far)
    feed_parts = lax.optimization_barrier((feed_parts, square_far))[0]
    feed_near = low_round(jnp.stack([feed_own] + feed_parts), count)
    vector_rows, up_biases, bias = vectors_to_all(ids, slots_near, slots_far, width, sizes)
    feed_near = after(feed_near, far_swapped, bias)
    pieces = (square_near, square_far, near_swapped, far_swapped)

    flips = offsets(count, half)
    other_flips = offsets(count, 1 - half)
    chips, other_chips = me ^ flips, me ^ other_flips
    aligned = rows % 16 == 0
    if not aligned:
        ordered = []
        for side, places in ((pieces[:2], chips), (pieces[2:], other_chips)):
            joint = jnp.take(jnp.concatenate(side), jnp.argsort(places), axis=0)
            ordered.append(
                jnp.transpose(joint, (1, 0, 2, 3)).reshape(1, 4 * GROUPS, width, 128)
            )
        pieces = tuple(ordered)

    q, k, v, mixed, lse = attend(ids, lengths, xs, mask, bias, vector_rows, pieces)
    feed_far = last_round(feed_near, count)
    feed_far = after(feed_far, mixed)

    feeds = (feed_near, swap(feed_near), feed_far, swap(feed_far))
    out, act, gup, first, gdown, gres, gbranch, gmixed, sums, up_sums = feed(
        ids, xs, mixed, cs, vector_rows, up_biases, feeds, pieces
    )
    shape = (near_count, 2, share, width)
    far_own, far_other = feed_weights(1, act, gup, first, gdown, shape)

    def by_device(grads):
        if aligned:
            return grads
        result = []
        for grad, places in zip(grads, (chips, other_chips)):
            parts = grad[0].reshape(grad.shape[1], count, rows, 128)
            parts = jnp.take(jnp.transpose(parts, (1, 0, 2, 3)), places, axis=0)
            result += [parts[:near_count], parts[near_count:]]
        return result

    def swapped_sum(own, other):
        return wide(own) + wide(swap(other))

    def halved(total):
        return total.reshape((2, total.shape[0] // 2) + total.shape[1:])

    def high_parts_of(total, count):
        return [
            lax.ppermute(low(total[high]), BOTH, xor_pairs(count, (4 * high, 4 * high)))
            for high in range(1, count // 4)
        ]

    def own_sum(total, parts):
        total = total[0]
        for part in parts:
            total = total + wide(part)
        return total

    gwo = out_weights(ids, after(mixed, far_own), gbranch, pieces)
    far = low(swapped_sum(far_own, far_other))
    gdown, far, _ = lax.optimization_barrier((gdown, far, gwo[0]))
    far = last_round(far, count)
    near_own, near_other = feed_weights(0, act, gup, first, gdown, shape)
    far, near_other = lax.optimization_barrier((far, near_other))
    near_came = swap(near_other)
    outs = unsort_rows(ids, order, after(out, far))
    near_came, near_own, far, _ = lax.optimization_barrier(
        (near_came, near_own, far, outs[0])
    )
    near = wide(near_own) + wide(near_came) + wide(far)
    gmixed, near = lax.optimization_barrier((gmixed, near))
    gfeed_came = lax.ppermute(low(halved(near)[1]), BOTH, xor_pairs(count, (1, 2)))
    grad_own, grad_send, *gws = attend_back(
        ids, lengths, order, xs, mask, bias, q, k, v, mixed, gmixed, lse, sums, up_sums, gres,
        pieces, gwo, rows,
    )
    gfeed_came, *gws = lax.optimization_barrier((gfeed_came, *gws))
    gfeed = halved(near)[0] + wide(gfeed_came)
    gfeed_parts = high_parts_of(gfeed, count)
    outs = place_rows(half, *outs)
    gws = by_device(gws)
    gw_far = last_round(low(swapped_sum(gws[1], gws[3])), count)
    near_came = swap(gws[2])
    gw_far, near_came = lax.optimization_barrier((gw_far, near_came))
    gw = wide(gws[0]) + wide(near_came) + wide(gw_far)
    gw_came = lax.ppermute(low(halved(gw)[1]), BOTH, xor_pairs(count, (1, 2)))
    gw_came, gfeed_parts = lax.optimization_barrier((gw_came, gfeed_parts))
    gw = halved(gw)[0] + wide(gw_came)
    gw_parts = high_parts_of(gw, count)
    gfeed = own_sum(gfeed, gfeed_parts)
    gfeed = in_order(half, gfeed, swap(gfeed))
    up_grad = jnp.transpose(gfeed[:, 0].reshape(hidden, width))
    down_grad = gfeed[:, 1].reshape(hidden, width)
    gw = own_sum(gw, gw_parts)
    query_grad, key_grad, value_grad, out_grad, *ends = finish(ids, gw, swap(gw), sizes)
    ends = [end.reshape(-1) for end in ends]
    grads = place_rows(half, grad_own, grad_send)

    return (
        outs[0], outs[1], grads[0], grads[1],
        query_grad, ends[0], key_grad, value_grad, ends[1], out_grad, ends[2], ends[3], ends[4],
        up_grad, ends[8], down_grad, ends[5], ends[6], ends[7], ends[9],
    )


def place_rows(half, own, send):
    came = swap(send)
    return [
        jnp.where(half == 0, jnp.stack([own[i], came[i]]), jnp.stack([came[i], own[i]]))
        for i in range(2)
    ]


def solution(mesh):
    rows3 = P("dp", "seq", None)
    flat, first, last = P("dp"), P("dp", None), P(None, "dp")
    in_specs = (
        rows3, rows3, rows3, rows3, first, first, first, flat, first, first, flat, first, flat,
        flat, flat, last, flat, first, flat, flat, flat, flat,
    )
    out_specs = (
        rows3, rows3, rows3, rows3, first, flat, first, first, flat, first, flat, flat, flat,
        last, flat, first, flat, flat, flat, flat,
    )
    body = functools.partial(shards, mesh.shape["dp"])
    return jax.shard_map(
        body, mesh=mesh, in_specs=in_specs, out_specs=out_specs, check_vma=False
    )
```

```python
import functools
import math

import jax
import jax.numpy as jnp
from jax import lax
from jax.experimental import pallas as pl
from jax.experimental.pallas import tpu as pltpu
from jax.sharding import PartitionSpec as P

HEADS = 12
HEAD_DIM = 64
BUCKETS = 32
GROUP = 4
LANES = GROUP * HEAD_DIM
GROUPS = HEADS // GROUP
TILE = 128
TILES = 4
NEG = -1e30
FLOOR = -1e29
EPS = 1e-05

limits = (1, 2, 3, 4, 5, 6, 7, 8, 12, 16, 23, 32, 46, 64, 91)

NN = (((1,), (0,)), ((), ()))
NT = (((1,), (1,)), ((), ()))
TN = (((0,), (0,)), ((), ()))
VMEM_SPEC = pl.BlockSpec(memory_space=pltpu.VMEM)
HBM_SPEC = pl.BlockSpec(memory_space=pltpu.HBM)
SCALE = 1.6e6
SMEM_SPEC = pl.BlockSpec(memory_space=pltpu.SMEM)
SDS = jax.ShapeDtypeStruct


def cost(micros):
    return pl.CostEstimate(
        flops=0, bytes_accessed=int(micros * SCALE), transcendentals=0
    )


def product(left, right, dims=NN):
    return lax.dot_general(left, right, dims, preferred_element_type=jnp.float32)


def params(semantics=None, limit=56):
    return pltpu.CompilerParams(dimension_semantics=semantics, vmem_limit_bytes=limit << 20)


def row_sum(values):
    return jnp.sum(values, axis=-1, keepdims=True)


ME, HALF = 0, 1
VECTORS, UP_SLOT, TABLE_SLOT = 10, 8, 9
FIRST_TILES, LAST_TILES = 3 * GROUPS, 4
FULL = 60


def in_hbm(*values):
    return [pltpu.with_memory_space_constraint(value, pltpu.HBM) for value in values]


def run_copies(copies):
    for copy in copies:
        copy.start()
    for copy in copies:
        copy.wait()


def pack_kernel(ids, content, query, ccot, qcot, wq, wk, wv, wo, up, down, *rest):
    vectors, rest = rest[:VECTORS], rest[VECTORS:]
    (theirs, square, feed, slots, tokens, squares, feeds, in_sems, out_sems) = rest
    half = ids[HALF]
    share = feed.shape[1]
    loads = []

    def load(source, target):
        copy = pltpu.make_async_copy(source, target, in_sems.at[len(loads)])
        copy.start()
        loads.append(copy)

    for index, weight in enumerate((wq, wk, wv, wo)):
        for group in range(GROUPS):
            lane = pl.multiple_of(group * LANES + half * 128, 128)
            place = 3 * group + index if index < 3 else 3 * GROUPS + group
            load(weight.at[:, pl.ds(lane, 128)], squares.at[place])
    for index, source in enumerate((content, query, ccot, qcot)):
        load(source.at[1 - half], tokens.at[index])
    rows = pl.ds(pl.multiple_of(half * share, share), share)
    load(up.at[rows, :], feeds.at[0])
    load(down.at[rows, :], feeds.at[1])
    slots[...] = jnp.zeros_like(slots)
    for index, vector in enumerate(vectors):
        slots[index : index + 1, : vector.shape[1]] = vector[...]
    for copy in loads[: 4 * GROUPS]:
        copy.wait()
    stores = [
        pltpu.make_async_copy(squares, square, out_sems.at[0]),
        pltpu.make_async_copy(tokens, theirs, out_sems.at[1]),
        pltpu.make_async_copy(feeds, feed, out_sems.at[2]),
    ]
    stores[0].start()
    for copy in loads[4 * GROUPS :]:
        copy.wait()
    stores[1].start()
    stores[2].start()
    for copy in stores:
        copy.wait()


def pack(ids, content, query, ccot, qcot, wq, wk, wv, wo, up, down, vectors):
    _, block, width = content.shape
    rows = wq.shape[0]
    hidden = up.shape[0]
    return pl.pallas_call(
        pack_kernel,
        out_shape=(
            SDS((4, block, width), jnp.bfloat16),
            SDS((4 * GROUPS, rows, 128), jnp.bfloat16),
            SDS((2, hidden // 2, width), jnp.bfloat16),
            SDS((16, 256), jnp.bfloat16),
        ),
        in_specs=[SMEM_SPEC] + [HBM_SPEC] * 10 + [VMEM_SPEC] * VECTORS,
        out_specs=(HBM_SPEC,) * 3 + (VMEM_SPEC,),
        scratch_shapes=[
            pltpu.VMEM((4, block, width), jnp.bfloat16),
            pltpu.VMEM((4 * GROUPS, rows, 128), jnp.bfloat16),
            pltpu.VMEM((2, hidden // 2, width), jnp.bfloat16),
            pltpu.SemaphoreType.DMA((4 * GROUPS + 6,)),
            pltpu.SemaphoreType.DMA((3,)),
        ],
        cost_estimate=cost(4),
        compiler_params=params(None, FULL),
        name="pack",
    )(ids, *in_hbm(content, query, ccot, qcot, wq, wk, wv, wo, up, down),
      *(vector.reshape(1, -1) for vector in vectors))


def order_onehot(ids, order):
    length = order.shape[1]
    row = order[pl.ds(ids[HALF], 1), :]
    down = lax.broadcasted_iota(jnp.int32, (length, length), 0)
    return jnp.where(row == down, 1.0, 0.0).astype(jnp.bfloat16)


def sort_kernel(ids, lengths, content, query, ccot, qcot, came, order,
                xs_out, cs_out, mask_out, held, sems):
    length = order.shape[1]
    block = content.shape[1]
    half = ids[HALF]
    copies = []
    for index, source in enumerate((content, query, ccot, qcot)):
        for place, rows in ((half, source.at[half]), (1 - half, came.at[index])):
            here = pl.ds(pl.multiple_of(place * block, block), block)
            copies.append(
                pltpu.make_async_copy(rows, held.at[index, here], sems.at[len(copies)])
            )
    for copy in copies:
        copy.start()
    onehot = order_onehot(ids, order)
    lane = lax.broadcasted_iota(jnp.int32, (8, length), 1)
    line = lax.broadcasted_iota(jnp.int32, (8, length), 0)
    digits = jnp.where(line == 0, lane // 16, jnp.where(line == 1, lane % 16, 0))
    digits = product(digits.astype(jnp.float32).astype(jnp.bfloat16), onehot, NT)
    rank_row = digits[0:1, :] * 16.0 + digits[1:2, :]
    across = lax.broadcasted_iota(jnp.int32, (length, length), 1).astype(jnp.float32)
    rank_col = row_sum(onehot.astype(jnp.float32) * across)
    place_col = lax.broadcasted_iota(jnp.int32, (length, 1), 0)
    place_row = lax.broadcasted_iota(jnp.int32, (1, length), 1)
    segment_col = jnp.zeros((length, 1), jnp.int32)
    segment_row = jnp.zeros((1, length), jnp.int32)
    bound = jnp.int32(0)
    for index in range(lengths.shape[1] - 1):
        bound = bound + lengths[half, index]
        segment_col = segment_col + (place_col >= bound).astype(jnp.int32)
        segment_row = segment_row + (place_row >= bound).astype(jnp.int32)
    same = segment_col == segment_row
    mask_out[0] = jnp.where(same & (rank_row <= rank_col), 0.0, NEG).astype(jnp.bfloat16)
    mask_out[1] = jnp.where(same & (rank_row < rank_col), 0.0, NEG).astype(jnp.bfloat16)
    for copy in copies:
        copy.wait()
    for source, target, at in ((0, xs_out, 0), (1, xs_out, 1), (2, cs_out, 0), (3, cs_out, 1)):
        target[at * length : (at + 1) * length, :] = product(onehot, held[source]).astype(
            jnp.bfloat16
        )


def sort_rows(ids, lengths, tokens, came, order):
    length = order.shape[1]
    width = came.shape[2]
    return pl.pallas_call(
        sort_kernel,
        out_shape=(
            SDS((2 * length, width), jnp.bfloat16),
            SDS((2 * length, width), jnp.bfloat16),
            SDS((2, length, length), jnp.bfloat16),
        ),
        in_specs=[SMEM_SPEC] * 2 + [HBM_SPEC] * 5 + [VMEM_SPEC],
        out_specs=(VMEM_SPEC,) * 3,
        scratch_shapes=[
            pltpu.VMEM((4, length, width), jnp.bfloat16),
            pltpu.SemaphoreType.DMA((8,)),
        ],
        cost_estimate=cost(5),
        compiler_params=params(None, FULL),
        name="sort_rows",
    )(ids, lengths, *in_hbm(*tokens, came), order)


def put_back(ids, onehot, source, scratch, own, send, sems):
    length = onehot.shape[0]
    block = own.shape[1]
    for stream in range(2):
        rows = product(onehot, source(stream), TN).astype(jnp.bfloat16)
        scratch[0, stream] = rows[:block, :]
        scratch[1, stream] = rows[block:, :]
    run_copies([
        pltpu.make_async_copy(scratch.at[ids[HALF]], own, sems.at[0]),
        pltpu.make_async_copy(scratch.at[1 - ids[HALF]], send, sems.at[1]),
    ])


def unsort_kernel(ids, order, values, own, send, held, scratch, sems):
    length = order.shape[1]
    copy = pltpu.make_async_copy(values, held, sems.at[2])
    copy.start()
    onehot = order_onehot(ids, order)
    copy.wait()
    put_back(
        ids, onehot, lambda s: held[s * length : (s + 1) * length, :], scratch, own, send, sems
    )


def unsort_rows(ids, order, values):
    length = order.shape[1]
    width = values.shape[1]
    shape = SDS((2, length // 2, width), jnp.bfloat16)
    return pl.pallas_call(
        unsort_kernel,
        out_shape=(shape, shape),
        in_specs=[SMEM_SPEC, VMEM_SPEC, HBM_SPEC],
        out_specs=(HBM_SPEC, HBM_SPEC),
        scratch_shapes=[
            pltpu.VMEM((2 * length, width), jnp.bfloat16),
            pltpu.VMEM((2, 2, length // 2, width), jnp.bfloat16),
            pltpu.SemaphoreType.DMA((3,)),
        ],
        cost_estimate=cost(3),
        compiler_params=params(None, FULL),
        name="unsort_rows",
    )(ids, order, *in_hbm(values))


SPAN = 5 * TILE
TURN = 6 * TILE


def bucket_onehot():
    distance = lax.broadcasted_iota(jnp.int32, (BUCKETS, TURN), 1) - (3 * TILE - 1)
    magnitude = jnp.abs(distance)
    counted = jnp.zeros(distance.shape, jnp.int32)
    for limit in limits:
        counted = counted + (magnitude >= limit).astype(jnp.int32)
    bucket = counted + 16 * (distance > 0).astype(jnp.int32)
    return bucket == lax.broadcasted_iota(jnp.int32, distance.shape, 0)


def block_flip(ids, own, far, block, count):
    place = ids[HALF] if own else 1 - ids[HALF]
    first = jnp.where(place == 0, 1, 2)
    high = count // 2
    flip = jnp.int32(4 * (block % high))
    if block >= high:
        flip = flip ^ first
    return flip ^ (3 - first) if far else flip


def block_places(ids, pieces):
    places = []
    for index, piece in enumerate(pieces):
        own = index < len(pieces) // 2
        place = ids[HALF] if own else 1 - ids[HALF]
        for block in range(piece.shape[0]):
            if len(pieces) == 2:
                places.append((index, block, place, 0))
            else:
                flip = block_flip(ids, own, index % 2 == 1, block, piece.shape[0])
                places.append((index, block, place, ids[ME] ^ flip))
    return places


def block_copies(ids, pieces, target, sems, tiles):
    copies = []
    for index, block, place, chip in block_places(ids, pieces):
        rows = pieces[index].shape[2]
        here = pl.ds(pl.multiple_of(chip * rows, rows), rows)
        copies.append(
            pltpu.make_async_copy(
                pieces[index].at[block, tiles], target.at[place, :, here, :],
                sems.at[len(copies)],
            )
        )
    return copies


def block_stores(ids, source, outs, sems, tiles):
    copies = []
    for index, block, place, chip in block_places(ids, outs):
        rows = outs[index].shape[2]
        here = pl.ds(pl.multiple_of(chip * rows, rows), rows)
        copies.append(
            pltpu.make_async_copy(
                source.at[place, :, here, :], outs[index].at[block, tiles],
                sems.at[len(copies)],
            )
        )
    return copies


def joined(weights, index):
    return jnp.concatenate([weights[0, index], weights[1, index]], axis=1)


def store_shapes(pieces, tiles):
    return tuple(SDS((p.shape[0], tiles) + p.shape[2:], jnp.bfloat16) for p in pieces)


def vectors_kernel(width, sizes, ids, near, far, rows_out, up_out, bias_out):
    count = 2 * near.shape[0]
    half = ids[HALF]
    high = count // 4
    total = jnp.zeros((16, width), jnp.float32)
    table = jnp.zeros((16, width), jnp.float32)
    blank = jnp.zeros((16, width - 256), jnp.float32)
    slot = lax.broadcasted_iota(jnp.int32, (16, width), 0)
    blocks = [[], []]
    for side, part in enumerate((near, far)):
        for block in range(part.shape[0]):
            chip = ids[ME] ^ block_flip(ids, True, side == 1, block, part.shape[0])
            values = jnp.concatenate([part[block].astype(jnp.float32), blank], axis=1)
            blocks[side].append(values)
            total = total + pltpu.roll(
                jnp.where(slot < UP_SLOT, values, 0.0), chip * sizes[0], 1
            )
            table = table + pltpu.roll(
                jnp.where(slot == TABLE_SLOT, values, 0.0), chip * sizes[TABLE_SLOT], 1
            )
    rows_out[...] = total[2:10, :]
    rows_out[6:8, :] = total[0:2, :]
    share = sizes[UP_SLOT] // 2
    lane = lax.broadcasted_iota(jnp.int32, (16, width), 1)
    keep = (slot == UP_SLOT) & (lane < share)
    near_blocks, far_blocks = blocks
    order = (
        (half, near_blocks[:high] + near_blocks[high:]),
        (1 - half, near_blocks[:high] + far_blocks[:high]),
        (half, far_blocks[:high] + far_blocks[high:]),
        (1 - half, near_blocks[high:] + far_blocks[high:]),
    )
    for index, (place, parts) in enumerate(order):
        joint = jnp.zeros((16, width), jnp.float32)
        for block, values in enumerate(parts):
            values = pltpu.roll(values, lax.rem(width - place * share, width), 1)
            joint = joint + pltpu.roll(jnp.where(keep, values, 0.0), block * share, 1)
        up_out[:, index * width : (index + 1) * width] = joint[UP_SLOT : UP_SLOT + 1, :]
    flat = table[TABLE_SLOT : TABLE_SLOT + 1, : BUCKETS * HEADS]
    entry = lax.broadcasted_iota(jnp.int32, (16, BUCKETS * HEADS), 1)
    head = lax.broadcasted_iota(jnp.int32, (16, BUCKETS * HEADS), 0)
    spread_heads = jnp.where(entry % HEADS == head, flat, 0.0).astype(jnp.bfloat16)
    place = lax.broadcasted_iota(jnp.int32, (BUCKETS, BUCKETS * HEADS), 1) // HEADS
    bucket = lax.broadcasted_iota(jnp.int32, (BUCKETS, BUCKETS * HEADS), 0)
    folded = product(spread_heads, jnp.where(place == bucket, 1.0, 0.0).astype(jnp.bfloat16), NT)
    onehot = jnp.where(bucket_onehot(), 1.0, 0.0).astype(jnp.bfloat16)
    rows = product(folded.astype(jnp.bfloat16), onehot)
    for head in range(HEADS):
        spread = jnp.broadcast_to(rows[head : head + 1, :], (TILE, TURN))
        turned = pltpu.roll(spread, TURN - (TILE - 1), 1, stride=1, stride_axis=0)
        bias_out[head] = turned[:, :SPAN].astype(jnp.bfloat16)


def vectors_to_all(ids, near, far, width, sizes):
    return pl.pallas_call(
        functools.partial(vectors_kernel, width, sizes),
        out_shape=(
            SDS((8, width), jnp.float32),
            SDS((1, 4 * width), jnp.float32),
            SDS((HEADS, TILE, SPAN), jnp.bfloat16),
        ),
        in_specs=[SMEM_SPEC] + [VMEM_SPEC] * 2,
        out_specs=(VMEM_SPEC,) * 3,
        cost_estimate=cost(6),
        compiler_params=params(None, FULL),
        name="vectors",
    )(ids, near, far)


def head_lanes(head, shape):
    lane = lax.broadcasted_iota(jnp.int32, shape, 1)
    return (lane >= head * HEAD_DIM) & (lane < (head + 1) * HEAD_DIM)


def head_stack(values):
    low = jnp.zeros((), values.dtype)
    return jnp.concatenate(
        [jnp.where(head_lanes(h, values.shape), values, low) for h in range(GROUP)]
    )


def head_merge(stack, rows):
    total = stack[(GROUP - 1) * rows :, :]
    for h in range(GROUP - 1):
        part = stack[h * rows : (h + 1) * rows, :]
        total = jnp.where(head_lanes(h, part.shape), part, total)
    return total


def widen(values, lanes):
    return jnp.concatenate([values] * (lanes // 128), axis=1)


def by_width(ids, lengths, tile, body):
    half = ids[HALF]
    begin, end = tile * TILE, (tile + 1) * TILE
    bound = jnp.int32(0)
    low, high = jnp.int32(0), jnp.int32(TILES * TILE)
    for index in range(lengths.shape[1] - 1):
        bound = bound + lengths[half, index]
        low = jnp.where(bound <= begin, bound, low)
        high = jnp.where(bound >= end, jnp.minimum(bound, high), high)
    first = low // TILE
    width = jnp.maximum((high + TILE - 1) // TILE - first, 2)
    first = pl.multiple_of(jnp.minimum(first, TILES - width) * TILE, TILE)
    for count in range(2, TILES + 1):
        pl.when(width == count)(functools.partial(body, first, count * TILE))


def attend_kernel(ids, lengths, xs, mask, bias, rows, *rest):
    pieces, rest = rest[:-8], rest[-8:]
    q_out, k_out, v_out, mixed_out, lse_out, weights, values, sems = rest
    length = mask.shape[1]
    group = pl.program_id(0)

    def weight_copies(index):
        tiles = pl.ds(3 * index, 3)
        return block_copies(ids, pieces, weights.at[:, tiles], sems.at[index], tiles)

    @pl.when(group == 0)
    def _():
        for index in range(GROUPS):
            for copy in weight_copies(index):
                copy.start()

    for index in range(GROUPS):
        @pl.when(group == index)
        def _():
            for copy in weight_copies(index):
                copy.wait()

    q = product(xs[...], joined(weights, 3 * group)) + rows[6:7, :]
    q_out[...] = q.astype(jnp.bfloat16)
    k = product(xs[0:length, :], joined(weights, 3 * group + 1))
    k_out[...] = k.astype(jnp.bfloat16)
    v = product(xs[0:length, :], joined(weights, 3 * group + 2)) + rows[7:8, :]
    v_out[...] = v.astype(jnp.bfloat16)

    wide_lanes = lax.broadcasted_iota(jnp.int32, v.shape, 1) < 128
    one = jnp.ones((), jnp.bfloat16)
    values[0] = jnp.where(wide_lanes, v_out[...], one)
    values[1] = jnp.where(wide_lanes, one, v_out[...])

    def tile_step(tile, carry):
        def body(first, keys):
            there = pl.ds(first, keys)
            near = pl.ds(pl.multiple_of((2 - tile) * TILE + first, TILE), keys)
            here = pl.ds(pl.multiple_of(tile * TILE, TILE), TILE)
            key = k_out[there, :]
            for stream in range(2):
                at = pl.ds(pl.multiple_of(stream * length + tile * TILE, TILE), TILE)
                scores = product(head_stack(q_out[at, :] * jnp.bfloat16(0.125)), key, NT)
                masked = mask[stream, here, there].astype(jnp.float32)
                weights, peaks, logs = [], [], []
                for h in range(GROUP):
                    part = scores[h * TILE : (h + 1) * TILE, :] + bias[h, :, near].astype(jnp.float32) + masked
                    peak = jnp.maximum(jnp.max(part, axis=-1, keepdims=True), FLOOR)
                    weights.append(jnp.exp(part - peak).astype(jnp.bfloat16))
                    peaks.append(peak)
                for pair in range(2):
                    both = jnp.concatenate(weights[2 * pair : 2 * pair + 2])
                    both = product(both, values[pair, there, :])
                    top = slice(pair * 128, pair * 128 + 128)
                    low = slice(128 - pair * 128, 256 - pair * 128)
                    parts = []
                    for h in range(2):
                        rows = slice(h * TILE, (h + 1) * TILE)
                        summed = both[rows, low]
                        alive = summed > 0
                        inverse = jnp.where(alive, 1.0 / summed, 0.0)
                        parts.append(both[rows, top] * inverse)
                        logs.append(
                            jnp.where(alive, peaks[2 * pair + h] + jnp.log(summed), 0.0)
                        )
                    lane = lax.broadcasted_iota(jnp.int32, parts[0].shape, 1)
                    mixed = jnp.where(lane < HEAD_DIM, parts[0], parts[1])
                    mixed_out[at, top] = mixed.astype(jnp.bfloat16)
                packed = logs[0]
                for h in range(1, GROUP):
                    packed = jnp.where(lane == h, logs[h], packed)
                lse_out[0, at, :] = packed

        by_width(ids, lengths, tile, body)
        return carry

    lax.fori_loop(0, length // TILE, tile_step, 0)


def attend(ids, lengths, xs, mask, bias, rows, pieces):
    tokens, width = xs.shape
    length = mask.shape[1]
    blocks = sum(piece.shape[0] for piece in pieces)
    full = lambda g: (0, 0)
    column = lambda g: (0, g)
    once = pl.Buffered(1)
    return pl.pallas_call(
        attend_kernel,
        grid=(GROUPS,),
        out_shape=(
            SDS((tokens, width), jnp.bfloat16),
            SDS((length, width), jnp.bfloat16),
            SDS((length, width), jnp.bfloat16),
            SDS((tokens, width), jnp.bfloat16),
            SDS((GROUPS, tokens, 128), jnp.float32),
        ),
        in_specs=[
            SMEM_SPEC,
            SMEM_SPEC,
            pl.BlockSpec((tokens, width), full, pipeline_mode=once),
            pl.BlockSpec((2, length, length), lambda g: (0, 0, 0), pipeline_mode=once),
            pl.BlockSpec((GROUP, TILE, SPAN), lambda g: (g, 0, 0)),
            pl.BlockSpec((8, LANES), column),
        ] + [HBM_SPEC] * len(pieces),
        out_specs=(
            pl.BlockSpec((tokens, LANES), column),
            pl.BlockSpec((length, LANES), column),
            pl.BlockSpec((length, LANES), column),
            pl.BlockSpec((tokens, LANES), column),
            pl.BlockSpec((1, tokens, 128), lambda g: (g, 0, 0)),
        ),
        scratch_shapes=[
            pltpu.VMEM((2, 3 * GROUPS, width, 128), jnp.bfloat16),
            pltpu.VMEM((2, length, LANES), jnp.bfloat16),
            pltpu.SemaphoreType.DMA((GROUPS, blocks)),
        ],
        cost_estimate=cost(18),
        compiler_params=params(("arbitrary",), FULL),
        name="attend",
    )(ids, lengths, xs, mask, bias, rows, *in_hbm(*pieces))


def norm_parts(values):
    mean = jnp.mean(values, axis=-1, keepdims=True)
    center = values - mean
    spread = jnp.mean(center * center, axis=-1, keepdims=True)
    scale = lax.rsqrt(spread + EPS)
    return center * scale, scale


def norm_back(normal, scale, grad):
    mean = jnp.mean(grad, axis=-1, keepdims=True)
    inner = jnp.mean(grad * normal, axis=-1, keepdims=True)
    return scale * (grad - mean - normal * inner)


def column_sum(values):
    return jnp.sum(values, axis=0, keepdims=True)


BLOCK = 256


def feed_kernel(ids, xs, mixed, cot, rows, up_bias, near_own, near_other, far_own, far_other,
                *rest):
    pieces, rest = rest[:-14], rest[-14:]
    (out, act_out, gup_out, first_out, gdown_out, gres_out, gbranch_out, gmixed_out,
     sums, up_sums, up_all, down_all, wo_all, sems) = rest
    step = pl.program_id(0)
    units = up_all.shape[0] // 4
    parts = (near_own, near_other, far_own, far_other)
    held = sum(piece.shape[0] for piece in pieces)

    def weight_copies():
        copies = []
        share = near_own.shape[2]
        for index, part in enumerate(parts):
            for block in range(part.shape[0]):
                here = slice(index * units + block * share, index * units + (block + 1) * share)
                for which, target in ((0, up_all), (1, down_all)):
                    copies.append(
                        pltpu.make_async_copy(
                            part.at[block, which], target.at[here, :],
                            sems.at[held + len(copies)],
                        )
                    )
        return copies

    @pl.when(step == 0)
    def _():
        sums[...] = jnp.zeros_like(sums)
        up_sums[...] = jnp.zeros_like(up_sums)
        copies = block_copies(ids, pieces, wo_all, sems, slice(3 * GROUPS, 4 * GROUPS))
        copies += weight_copies()
        run_copies(copies)

    wo = jnp.concatenate([joined(wo_all, index) for index in range(GROUPS)], axis=1)
    branch = product(mixed[...], wo) + rows[0:1, :]

    normal1, scale1 = norm_parts(xs[...].astype(jnp.float32) + branch)
    first = normal1 * rows[1:2, :] + rows[2:3, :]
    first_low = first.astype(jnp.bfloat16)
    first_out[...] = first_low
    slopes = []
    second = first + rows[3:4, :]
    for index in range(2):
        here = slice(2 * index * units, 2 * (index + 1) * units)
        up = product(first_low, up_all[here, :], NT) + up_bias[:, here]
        gate = 0.5 + 0.5 * lax.erf(up * math.sqrt(0.5))
        act = (up * gate).astype(jnp.bfloat16)
        act_out[:, here] = act
        slopes.append(gate + up * jnp.exp(-0.5 * up * up) * (1.0 / math.sqrt(2.0 * math.pi)))
        second = second + product(act, down_all[here, :])
    normal2, scale2 = norm_parts(second)
    gain = rows[4:5, :]
    out[...] = (normal2 * gain + rows[5:6, :]).astype(jnp.bfloat16)
    cots = cot[...].astype(jnp.float32)
    gsecond = norm_back(normal2, scale2, cots * gain)
    gdown = gsecond.astype(jnp.bfloat16)
    gdown_out[...] = gdown
    gfirst = gsecond
    for index in range(2):
        here = slice(2 * index * units, 2 * (index + 1) * units)
        gup = (product(gdown, down_all[here, :], NT) * slopes[index]).astype(jnp.bfloat16)
        gup_out[:, here] = gup
        up_sums[:, here] += column_sum(gup.astype(jnp.float32))
        gfirst = gfirst + product(gup, up_all[here, :])
    gres = norm_back(normal1, scale1, gfirst * rows[1:2, :])
    gres_out[...] = gres
    gbranch = gres.astype(jnp.bfloat16)
    gbranch_out[...] = gbranch
    gmixed_out[...] = product(gbranch, wo, NT).astype(jnp.bfloat16)
    sums[0:1, :] += column_sum(gbranch.astype(jnp.float32))
    sums[1:2, :] += column_sum(gfirst * normal1)
    sums[2:3, :] += column_sum(gfirst)
    sums[3:4, :] += column_sum(gdown.astype(jnp.float32))
    sums[4:5, :] += column_sum(cots * normal2)
    sums[5:6, :] += column_sum(cots)


def feed(ids, xs, mixed, cot, rows, up_bias, feeds, pieces):
    tokens, width = xs.shape
    hidden = up_bias.shape[1]
    token = pl.BlockSpec((BLOCK, width), lambda i: (i, 0))
    wide = pl.BlockSpec((BLOCK, hidden), lambda i: (i, 0))
    held = sum(piece.shape[0] for piece in pieces) + 2 * sum(part.shape[0] for part in feeds)
    low = SDS((tokens, width), jnp.bfloat16)
    return pl.pallas_call(
        feed_kernel,
        grid=(tokens // BLOCK,),
        out_shape=(
            low,
            SDS((tokens, hidden), jnp.bfloat16),
            SDS((tokens, hidden), jnp.bfloat16),
            low,
            low,
            SDS((tokens, width), jnp.float32),
            low,
            low,
            SDS((8, width), jnp.float32),
            SDS((1, hidden), jnp.float32),
        ),
        in_specs=[
            SMEM_SPEC, token, token, token,
            pl.BlockSpec((8, width), lambda i: (0, 0)),
            pl.BlockSpec((1, hidden), lambda i: (0, 0)),
        ] + [HBM_SPEC] * (4 + len(pieces)),
        out_specs=(token, wide, wide, token, token, token, token, token,
                   pl.BlockSpec((8, width), lambda i: (0, 0)),
                   pl.BlockSpec((1, hidden), lambda i: (0, 0))),
        scratch_shapes=[
            pltpu.VMEM((hidden, width), jnp.bfloat16),
            pltpu.VMEM((hidden, width), jnp.bfloat16),
            pltpu.VMEM((2, GROUPS, width, 128), jnp.bfloat16),
            pltpu.SemaphoreType.DMA((held,)),
        ],
        cost_estimate=cost(36),
        compiler_params=params(("arbitrary",), FULL),
        name="feed",
    )(ids, xs, mixed, cot, rows, up_bias, *in_hbm(*feeds, *pieces))


def feed_weights_kernel(act, gup, first, gdown, own, other):
    which = pl.program_id(1)

    def put(grad):
        share = own.shape[2]
        grad = grad.astype(jnp.bfloat16)

        def store(out):
            for block in range(out.shape[0]):
                out[block, 0] = grad[block * share : (block + 1) * share, :]

        pl.when(pl.program_id(0) == 0)(lambda: store(other))
        pl.when(pl.program_id(0) == 1)(lambda: store(own))

    pl.when(which == 0)(lambda: put(product(gup[...], first[...], TN)))
    pl.when(which == 1)(lambda: put(product(act[...], gdown[...], TN)))


def feed_weights(part, act, gup, first, gdown, shape):
    tokens, width = first.shape
    units = shape[0] * shape[2]
    full = pl.BlockSpec((tokens, width), lambda s, u: (0, 0), pipeline_mode=pl.Buffered(1))
    lanes = pl.BlockSpec((tokens, units), lambda s, u: (0, 2 * part + 1 - s))
    block = (shape[0], 1) + shape[2:]
    return pl.pallas_call(
        feed_weights_kernel,
        grid=(2, 2),
        out_shape=(SDS(shape, jnp.bfloat16),) * 2,
        in_specs=[lanes, lanes, full, full],
        out_specs=(
            pl.BlockSpec(block, lambda s, u: (0, s * u, 0, 0)),
            pl.BlockSpec(block, lambda s, u: (0, jnp.maximum(s, u), 0, 0)),
        ),
        cost_estimate=cost(9),
        compiler_params=params(("arbitrary", "arbitrary"), FULL),
        name="feed_weights",
    )(act, gup, first, gdown)


def out_weights_kernel(ids, mixed, gbranch, *rest):
    outs, (buffer, sems) = rest[:-2], rest[-2:]
    grad = product(mixed[...], gbranch[...], TN).astype(jnp.bfloat16)
    for index in range(GROUPS):
        for half in range(2):
            lane = index * LANES + half * 128
            buffer[half, index] = grad[:, lane : lane + 128]
    run_copies(block_stores(ids, buffer, outs, sems, slice(2 * GROUPS, 3 * GROUPS)))


def out_weights(ids, mixed, gbranch, pieces):
    tokens, width = mixed.shape
    blocks = sum(piece.shape[0] for piece in pieces)
    full = pl.BlockSpec((tokens, width), lambda i: (0, 0))
    return pl.pallas_call(
        out_weights_kernel,
        grid=(1,),
        out_shape=store_shapes(pieces, FIRST_TILES),
        in_specs=[SMEM_SPEC, full, full],
        out_specs=(HBM_SPEC,) * len(pieces),
        scratch_shapes=[
            pltpu.VMEM((2, GROUPS, width, 128), jnp.bfloat16),
            pltpu.SemaphoreType.DMA((blocks,)),
        ],
        cost_estimate=cost(4),
        compiler_params=params(("arbitrary",), FULL),
        name="out_weights",
    )(ids, mixed, gbranch)


def attend_back_kernel(ids_rows, base, steps, ids, lengths, order, mask, bias, q, k, v, mixed, gmixed, lse, sums,
                       up_sums, xs_far, gres, *rest):
    scratch = rest[-17:]
    done = base + steps == GROUPS
    count = (len(rest) - 17 - 2) // (2 if done else 3)
    pieces = rest[:count]
    if done:
        own, send, *gw_outs = rest[count:-17]
    else:
        gx_out, vectors_out, *gw_outs = rest[2 * count : -17]
    (vectors, turned, vector_sems, gk, gv, gdist, gx, gq, inner, weights, buffer, xs, rows_out, sems, in_sems, out_sems,
     row_sems) = scratch
    step = pl.program_id(0)
    group = base + step
    tiles = slice(3 * base, 3 * (base + steps))
    length = mask.shape[1]
    rows = xs.shape[1] // (2 * gw_outs[0].shape[0]) if count > 2 else ids_rows
    loads = block_copies(ids, pieces, weights, sems, tiles) + [
        pltpu.make_async_copy(xs_far, xs, in_sems.at[0]),
        pltpu.make_async_copy(gres, gx, in_sems.at[1]),
    ]

    def stores(index):
        return block_stores(
            ids, buffer.at[index], gw_outs, out_sems.at[index],
            slice(0, 3) if done else pl.ds(3 * (base + index), 3),
        )

    @pl.when(step == 0)
    def _():
        for copy in loads:
            copy.start()
        if base:
            vectors[0:16, :] = sums[8:24, :]

    gdist[...] = jnp.zeros_like(gdist)
    gk[...] = jnp.zeros_like(gk)
    gv[...] = jnp.zeros_like(gv)

    lane = lax.broadcasted_iota(jnp.int32, (LANES, GROUP * 128), 0) // HEAD_DIM
    head = lax.broadcasted_iota(jnp.int32, (LANES, GROUP * 128), 1) // 128
    adder = jnp.where(lane == head, 1.0, 0.0).astype(jnp.bfloat16)
    crossed = mixed[...].astype(jnp.float32) * gmixed[...].astype(jnp.float32)
    inner[...] = product(crossed.astype(jnp.bfloat16), adder)

    def tile_step(tile, carry):
        def body(first, keys):
            there = pl.ds(first, keys)
            near = pl.ds(pl.multiple_of((2 - tile) * TILE + first, TILE), keys)
            here = pl.ds(pl.multiple_of(tile * TILE, TILE), TILE)
            key = k[there, :]
            value = v[there, :]
            at = [
                pl.ds(pl.multiple_of(stream * length + tile * TILE, TILE), TILE)
                for stream in range(2)
            ]
            query = jnp.concatenate([head_stack(q[at[s], :] * jnp.bfloat16(0.125)) for s in range(2)])
            gmix = jnp.concatenate([head_stack(gmixed[at[s], :]) for s in range(2)])
            scores = product(query, key, NT)
            gprobs = product(gmix, value, NT)
            masked = [mask[s, here, there].astype(jnp.float32) for s in range(2)]
            probs_low = [None] * (2 * GROUP)
            gscores_low = [None] * (2 * GROUP)
            for h in range(GROUP):
                both = None
                near_bias = bias[h, :, near].astype(jnp.float32)
                for stream in range(2):
                    index = stream * GROUP + h
                    part = slice(index * TILE, (index + 1) * TILE)
                    score = scores[part, :] + near_bias + masked[stream]
                    probs = jnp.exp(score - lse[0, at[stream], h : h + 1])
                    lanes = slice(h * 128, (h + 1) * 128)
                    gscores = probs * (gprobs[part, :] - widen(inner[at[stream], lanes], keys))
                    probs_low[index] = probs.astype(jnp.bfloat16)
                    gscores_low[index] = gscores.astype(jnp.bfloat16)
                    both = gscores if both is None else both + gscores
                gdist[h, :, near] += both
            probs_low = jnp.concatenate(probs_low)
            gscores_low = jnp.concatenate(gscores_low)
            gv[there, :] += product(probs_low, gmix, TN)
            gk[there, :] += product(gscores_low, query, TN)
            back = product(gscores_low, key)
            for stream in range(2):
                part = slice(stream * GROUP * TILE, (stream + 1) * GROUP * TILE)
                gq[at[stream], :] = head_merge(back[part, :], TILE)

        by_width(ids, lengths, tile, body)
        return carry

    lax.fori_loop(0, length // TILE, tile_step, 0)
    gq_low = (gq[...] * 0.125).astype(jnp.bfloat16)
    gk_low = gk[...].astype(jnp.bfloat16)
    gv_low = gv[...].astype(jnp.bfloat16)

    @pl.when(step == 0)
    def _():
        for copy in loads:
            copy.wait()

    for index, grad in enumerate((
        product(xs[...], gq_low, TN),
        product(xs[0:length, :], gk_low, TN),
        product(xs[0:length, :], gv_low, TN),
    )):
        grad = grad.astype(jnp.bfloat16)
        buffer[step, 0, index] = grad[:, :128]
        buffer[step, 1, index] = grad[:, 128:]
    for index in range(steps):
        @pl.when(step == index)
        def _():
            for copy in stores(index):
                copy.start()

    gx[...] += product(gq_low, joined(weights, 3 * step), NT)
    gx[0:length, :] += product(gk_low, joined(weights, 3 * step + 1), NT) + product(
        gv_low, joined(weights, 3 * step + 2), NT
    )
    lanes = pl.ds(pl.multiple_of(group * LANES, LANES), LANES)
    vectors[0:1, lanes] = column_sum(gq_low.astype(jnp.float32))
    vectors[1:2, lanes] = column_sum(gv_low.astype(jnp.float32))
    span = TURN
    pieces_sum = []
    row_index = lax.broadcasted_iota(jnp.int32, (8, span), 0)
    for h in range(GROUP):
        wide = jnp.concatenate([gdist[h], jnp.zeros((TILE, TILE), jnp.float32)], axis=1)
        size = TILE // 2
        while size >= 8:
            wide = wide[size:, :] + pltpu.roll(wide[:size, :], size, 1)
            size //= 2
        for bit in (4, 2, 1):
            wide = jnp.where(row_index & bit == 0, pltpu.roll(wide, bit, 1), wide)
        pieces_sum.append(column_sum(wide))
    pieces_sum.append(jnp.zeros((8 - GROUP, span), jnp.float32))
    onehot = jnp.where(bucket_onehot(), 1.0, 0.0)
    by_bucket = lax.dot_general(
        jnp.concatenate(pieces_sum, axis=0), onehot, NT, precision=lax.Precision.HIGHEST,
        preferred_element_type=jnp.float32,
    )
    width = xs.shape[1]
    parts = width // rows
    each = BUCKETS * HEADS // parts
    lane = lax.broadcasted_iota(jnp.int32, (BUCKETS, width), 1)
    entry = lane // rows * each + lane % rows
    bucket = lax.broadcasted_iota(jnp.int32, (BUCKETS, width), 0)
    chosen = (entry // HEADS == bucket) & (lane % rows < each)
    table = lax.dot_general(
        by_bucket, jnp.where(chosen, 1.0, 0.0), NN, precision=lax.Precision.HIGHEST,
        preferred_element_type=jnp.float32,
    )
    head = lax.broadcasted_iota(jnp.int32, table.shape, 0)
    lane = lax.broadcasted_iota(jnp.int32, table.shape, 1)
    entry = lane // rows * each + lane % rows
    right = (head < GROUP) & (entry % HEADS == GROUP * group + head)
    table = column_sum(jnp.where(right, table, 0.0))

    if base:
        vectors[12:13, :] += table
    else:
        vectors[12:13, :] = table

    if not done:
        for copy in stores(0):
            copy.wait()
        vectors_out[...] = vectors[0:16, :]
        run_copies([pltpu.make_async_copy(gx, gx_out, in_sems.at[0])])
        return

    @pl.when(step == steps - 1)
    def _():
        put_back(
            ids, order_onehot(ids, order),
            lambda s: gx[s * length : (s + 1) * length, :].astype(jnp.bfloat16),
            rows_out, own, send, row_sems,
        )
        vectors[2:8, :] = sums[0:6, :]
        vectors[8:12, :] = up_slots(ids, up_sums, rows, parts // 2)
        vectors[13:, :] = jnp.zeros((128 - 13, width), jnp.float32)
        tile = jnp.transpose(vectors[...]).astype(jnp.bfloat16)
        turned[0, 0] = tile
        turned[1, 0] = tile
        last = block_stores(
            ids, turned, gw_outs, vector_sems, slice(3, LAST_TILES)
        )
        for copy in last:
            copy.start()
        waits = [copy for index in range(steps) for copy in stores(index)]
        for copy in waits + last:
            copy.wait()


def up_slots(ids, up_sums, rows, blocks):
    width = up_sums.shape[1] // 4
    share = 2 * rows
    slot = lax.broadcasted_iota(jnp.int32, (8, width), 0)
    lane = lax.broadcasted_iota(jnp.int32, (8, width), 1)
    total = jnp.zeros((8, width), jnp.float32)
    for index in range(4):
        own = index % 2 == 0
        place = ids[HALF] if own else 1 - ids[HALF]
        part = jnp.broadcast_to(up_sums[:, index * width : (index + 1) * width], (8, width))
        for block in range(blocks):
            chip = ids[ME] ^ block_flip(ids, own, index >= 2, block, blocks)
            for quarter in range(2):
                shift = (width - block * share - quarter * rows) % width
                values = pltpu.roll(part, shift, 1) if shift else part
                keep = (lane < rows) & (slot == 2 * place + quarter)
                total = total + pltpu.roll(jnp.where(keep, values, 0.0), chip * rows, 1)
    return total[0:4, :]


def attend_back(base, steps, ids, lengths, order, xs, mask, bias, q, k, v, mixed, gmixed, lse,
                sums, up_sums, gres, pieces, grads, rows_each):
    tokens, width = xs.shape
    length = mask.shape[1]
    blocks = sum(piece.shape[0] for piece in pieces)
    done = base + steps == GROUPS
    column = lambda g: (0, base + g)
    rows = SDS((2, length // 2, width), jnp.bfloat16)
    first = 15 + len(pieces)
    if done:
        outs, out_specs = (rows, rows), (HBM_SPEC, HBM_SPEC)
    else:
        outs = (SDS((tokens, width), jnp.float32), SDS((16, width), jnp.float32))
        out_specs = (HBM_SPEC, pl.BlockSpec((16, width), lambda g: (0, 0)))
    return pl.pallas_call(
        functools.partial(attend_back_kernel, rows_each, base, steps),
        grid=(steps,),
        out_shape=outs + store_shapes(pieces, LAST_TILES if done else FIRST_TILES),
        input_output_aliases={first + index: 2 + index for index in range(len(grads))},
        in_specs=[
            SMEM_SPEC,
            SMEM_SPEC,
            VMEM_SPEC,
            pl.BlockSpec((2, length, length), lambda g: (0, 0, 0), pipeline_mode=pl.Buffered(1)),
            pl.BlockSpec((GROUP, TILE, SPAN), lambda g: (base + g, 0, 0)),
            pl.BlockSpec((tokens, LANES), column),
            pl.BlockSpec((length, LANES), column),
            pl.BlockSpec((length, LANES), column),
            pl.BlockSpec((tokens, LANES), column),
            pl.BlockSpec((tokens, LANES), column),
            pl.BlockSpec((1, tokens, 128), lambda g: (base + g, 0, 0)),
            pl.BlockSpec(sums.shape, lambda g: (0, 0)),
            pl.BlockSpec((1, 4 * width), lambda g: (0, 0)),
        ] + [HBM_SPEC] * (2 + len(pieces) + len(grads)),
        out_specs=out_specs + (HBM_SPEC,) * len(pieces),
        scratch_shapes=[
            pltpu.VMEM((128, width), jnp.float32),
            pltpu.VMEM((2, 1, width, 128), jnp.bfloat16),
            pltpu.SemaphoreType.DMA((blocks,)),
            pltpu.VMEM((length, LANES), jnp.float32),
            pltpu.VMEM((length, LANES), jnp.float32),
            pltpu.VMEM((GROUP, TILE, SPAN), jnp.float32),
            pltpu.VMEM((tokens, width), jnp.float32),
            pltpu.VMEM((tokens, LANES), jnp.float32),
            pltpu.VMEM((tokens, GROUP * 128), jnp.float32),
            pltpu.VMEM((2, 3 * steps, width, 128), jnp.bfloat16),
            pltpu.VMEM((steps, 2, 3, width, 128), jnp.bfloat16),
            pltpu.VMEM((tokens, width), jnp.bfloat16),
            pltpu.VMEM((2, 2, length // 2, width), jnp.bfloat16),
            pltpu.SemaphoreType.DMA((blocks,)),
            pltpu.SemaphoreType.DMA((2,)),
            pltpu.SemaphoreType.DMA((steps, blocks)),
            pltpu.SemaphoreType.DMA((2,)),
        ],
        cost_estimate=cost(14 * steps),
        compiler_params=params(("arbitrary",), FULL),
        name="attend_back",
    )(ids, lengths, order, mask, bias, q, k, v, mixed, gmixed, lse, sums, up_sums,
      *in_hbm(xs, gres, *pieces, *grads))


def grad_tile(index, group):
    if index == 3:
        return 2 * GROUPS + group
    return index + (3 * group if group < GROUPS - 1 else FIRST_TILES)


def finish_kernel(ids, own, came, wq, wk, wv, wo, *vectors):
    half = ids[HALF]
    for place in range(2):
        mine = half == place
        for index, out in enumerate((wq, wk, wv, wo)):
            for group in range(GROUPS):
                tile = grad_tile(index, group)
                lane = group * LANES + place * 128
                out[:, lane : lane + 128] = jnp.where(mine, own[tile], came[tile])
    turned = jnp.transpose(own[FIRST_TILES + 3])
    rows = own.shape[1]
    for index, out in enumerate(vectors):
        if index == UP_SLOT:
            for quarter in range(4):
                out[:, quarter * rows : (quarter + 1) * rows] = turned[8 + quarter : 9 + quarter, :]
        else:
            at = 12 if index == TABLE_SLOT else index
            out[...] = turned[at : at + 1, : out.shape[1]]


def finish(ids, own, came, sizes):
    rows = own.shape[1]
    width = LANES * GROUPS
    outs = (SDS((rows, width), jnp.float32),) * 4
    outs += tuple(SDS((1, size), jnp.float32) for size in sizes)
    return pl.pallas_call(
        finish_kernel,
        out_shape=outs,
        in_specs=[SMEM_SPEC, VMEM_SPEC, VMEM_SPEC],
        out_specs=(VMEM_SPEC,) * len(outs),
        cost_estimate=cost(2),
        compiler_params=params(None, FULL),
        name="finish",
    )(ids, own, came)


BOTH = ("dp", "seq")


def xor_pairs(count, by_half):
    halves = len(by_half)
    return [
        (device * halves + half, (device ^ flip) * halves + half)
        for device in range(count)
        for half, flip in enumerate(by_half)
    ]


def swap(value):
    return lax.ppermute(value, "seq", [(0, 1), (1, 0)])


def high_part(value, high, count):
    return lax.ppermute(value, BOTH, xor_pairs(count, (4 * high, 4 * high)))


def high_parts(value, count):
    return [high_part(value, high, count) for high in range(1, count // 4)]


def low_round(value, count):
    return jnp.concatenate([value, lax.ppermute(value, BOTH, xor_pairs(count, (1, 2)))])


def last_round(value, count):
    return lax.ppermute(value, BOTH, xor_pairs(count, (2, 1)))


def offsets(count, half):
    first = jnp.where(half == 0, 1, 2)
    highs = 4 * jnp.arange(count // 4)
    near = jnp.concatenate([highs, highs ^ first])
    return jnp.concatenate([near, near ^ (3 - first)])


def after(value, *others):
    return lax.optimization_barrier((value,) + others)[0]


def wide(value):
    return value.astype(jnp.float32)


def low(value):
    return value.astype(jnp.bfloat16)


def in_order(half, own, other):
    return jnp.where(half == 0, jnp.stack([own, other]), jnp.stack([other, own]))


def shards(count, content, query_in, content_cot, query_cot, lengths, order, query_weight,
           query_bias, key_weight, value_weight, value_bias, out_weight, out_bias, mixer_gain,
           mixer_shift, up_weight, up_bias, down_weight, down_bias, final_gain, final_shift,
           position_bias):
    _, block, width = content.shape
    length = order.shape[1]
    half = lax.axis_index("seq")
    me = lax.axis_index("dp")
    rows = query_weight.shape[0]
    hidden = up_weight.shape[1]
    share = hidden // 2
    near_count = count // 2

    ids = jnp.stack([me, half]).astype(jnp.int32)
    vectors = (query_bias, value_bias, out_bias, mixer_gain, mixer_shift, down_bias, final_gain,
               final_shift, up_bias, position_bias)
    sizes = [vector.shape[0] for vector in vectors]
    theirs, square, feed_own, slots = pack(
        ids, content, query_in, content_cot, query_cot, query_weight, key_weight, value_weight,
        out_weight, jnp.transpose(up_weight), down_weight, vectors,
    )

    square_parts = high_parts(square, count)
    came = swap(theirs)
    slots = after(slots, came)
    slots_high = jnp.stack([slots] + high_parts(slots, count))
    xs, cs, mask = sort_rows(
        ids, lengths, (content, query_in, content_cot, query_cot), came, order
    )
    feed_early = high_part(after(feed_own, came), 2, count)
    square_parts, xs, slots_high = lax.optimization_barrier((square_parts, xs, slots_high))
    square_near = low_round(jnp.stack([square] + square_parts), count)
    slots_near = low_round(slots_high, count)
    square_near, slots_near, feed_early = lax.optimization_barrier(
        (square_near, slots_near, feed_early)
    )
    square_far = last_round(square_near, count)
    slots_far = last_round(slots_near, count)
    near_swapped = swap(square_near)
    square_far = after(square_far, slots_far, near_swapped)
    far_swapped = swap(square_far)
    feed_later = after(feed_own, square_near)
    feed_parts = [
        feed_early if high == 2 else high_part(feed_later, high, count)
        for high in range(1, count // 4)
    ]
    feed_parts = lax.optimization_barrier((feed_parts, square_far))[0]
    feed_near = low_round(jnp.stack([feed_own] + feed_parts), count)
    vector_rows, up_biases, bias = vectors_to_all(ids, slots_near, slots_far, width, sizes)
    feed_near = after(feed_near, far_swapped, bias)
    pieces = (square_near, square_far, near_swapped, far_swapped)

    flips = offsets(count, half)
    other_flips = offsets(count, 1 - half)
    chips, other_chips = me ^ flips, me ^ other_flips
    aligned = rows % 16 == 0
    if not aligned:
        ordered = []
        for side, places in ((pieces[:2], chips), (pieces[2:], other_chips)):
            joint = jnp.take(jnp.concatenate(side), jnp.argsort(places), axis=0)
            ordered.append(
                jnp.transpose(joint, (1, 0, 2, 3)).reshape(1, 4 * GROUPS, width, 128)
            )
        pieces = tuple(ordered)

    q, k, v, mixed, lse = attend(ids, lengths, xs, mask, bias, vector_rows, pieces)
    feed_far = last_round(feed_near, count)
    feed_far = after(feed_far, mixed)

    feeds = (feed_near, swap(feed_near), feed_far, swap(feed_far))
    out, act, gup, first, gdown, gres, gbranch, gmixed, sums, up_sums = feed(
        ids, xs, mixed, cs, vector_rows, up_biases, feeds, pieces
    )
    shape = (near_count, 2, share, width)
    far_own, far_other = feed_weights(1, act, gup, first, gdown, shape)

    def by_device(grads):
        if aligned:
            return grads
        result = []
        for grad, places in zip(grads, (chips, other_chips)):
            parts = grad[0].reshape(grad.shape[1], count, rows, 128)
            parts = jnp.take(jnp.transpose(parts, (1, 0, 2, 3)), places, axis=0)
            result += [parts[:near_count], parts[near_count:]]
        return result

    def swapped_sum(own, other):
        return wide(own) + wide(swap(other))

    def halved(total):
        return total.reshape((2, total.shape[0] // 2) + total.shape[1:])

    def high_parts_of(total, count):
        return [
            lax.ppermute(low(total[high]), BOTH, xor_pairs(count, (4 * high, 4 * high)))
            for high in range(1, count // 4)
        ]

    def own_sum(total, parts):
        total = total[0]
        for part in parts:
            total = total + wide(part)
        return total

    gwo = out_weights(ids, after(mixed, far_own), gbranch, pieces)
    far_came, _ = lax.optimization_barrier((swap(far_other), gwo[0]))
    far_first, far_second = (
        low(wide(halved(far_own)[part]) + wide(halved(far_came)[part])) for part in range(2)
    )
    gmixed, far_first, far_second = lax.optimization_barrier((gmixed, far_first, far_second))
    far_first = last_round(far_first, count)
    heads = functools.partial(
        attend_back, ids=ids, lengths=lengths, order=order, xs=xs, mask=mask, bias=bias, q=q, k=k,
        v=v, mixed=mixed, lse=lse, up_sums=up_sums, pieces=pieces, rows_each=rows,
    )
    gx, head_sums, *gws = heads(0, 1, gmixed=gmixed, sums=sums, gres=gres, grads=gwo)
    gdown, far_first, far_second, gx = lax.optimization_barrier(
        (gdown, far_first, far_second, gx)
    )
    far_second = last_round(far_second, count)
    near_own, near_other = feed_weights(0, act, gup, first, gdown, shape)
    far_second, near_own, near_other = lax.optimization_barrier(
        (far_second, near_own, near_other)
    )
    near_came = swap(near_other)
    outs = unsort_rows(ids, order, after(out, far_second))
    near_came, near_own, _ = lax.optimization_barrier((near_came, near_own, outs[0]))
    far_halves = (far_first, far_second)
    near_halves = [
        wide(halved(near_own)[part]) + wide(halved(near_came)[part]) + wide(far_halves[part])
        for part in range(2)
    ]
    gx, to_send = lax.optimization_barrier((gx, low(near_halves[1])))
    gfeed_came = lax.ppermute(to_send, BOTH, xor_pairs(count, (1, 2)))
    gx, head_sums, *gws = result = heads(
        1, 1, gmixed=gmixed, sums=jnp.concatenate([sums, head_sums]), gres=gx, grads=gws
    )
    gfeed_came, gx = lax.optimization_barrier((gfeed_came, gx))
    gfeed = near_halves[0] + wide(gfeed_came)
    gfeed_low = [low(gfeed[high]) for high in range(1, count // 4)]
    gx, gfeed_low = lax.optimization_barrier((gx, gfeed_low))
    early = high_part(gfeed_low[1], 2, count)
    most = by_device(result[2:])
    most_came = [swap(part) for part in most[2:]]
    grad_own, grad_send, *gws = heads(
        2, 1, gmixed=gmixed, sums=jnp.concatenate([sums, head_sums]), gres=gx, grads=()
    )
    early, most_came, gws = lax.optimization_barrier((early, most_came, gws))
    last = by_device(gws)
    most_far = last_round(low(wide(most[1]) + wide(most_came[1])), count)
    last_came = [swap(part) for part in last[2:]]
    last_far = last_round(low(wide(last[1]) + wide(last_came[1])), count)
    gfeed_parts = [
        early if high == 2 else high_part(gfeed_low[high - 1], high, count)
        for high in range(1, count // 4)
    ]
    outs = place_rows(half, *outs)
    grads = place_rows(half, grad_own, grad_send)
    most_far, last_far, last_came, gfeed_parts = lax.optimization_barrier(
        (most_far, last_far, last_came, gfeed_parts)
    )
    gw = jnp.concatenate([
        wide(most[0]) + wide(most_came[0]) + wide(most_far),
        wide(last[0]) + wide(last_came[0]) + wide(last_far),
    ], axis=1)
    gw_came = lax.ppermute(low(halved(gw)[1]), BOTH, xor_pairs(count, (1, 2)))
    gw = halved(gw)[0] + wide(gw_came)
    gw_parts = high_parts_of(gw, count)
    gfeed = own_sum(gfeed, gfeed_parts)
    gfeed = in_order(half, gfeed, swap(gfeed))
    up_grad = jnp.transpose(gfeed[:, 0].reshape(hidden, width))
    down_grad = gfeed[:, 1].reshape(hidden, width)
    gw = own_sum(gw, gw_parts)
    query_grad, key_grad, value_grad, out_grad, *ends = finish(ids, gw, swap(gw), sizes)
    ends = [end.reshape(-1) for end in ends]
    return (
        outs[0], outs[1], grads[0], grads[1],
        query_grad, ends[0], key_grad, value_grad, ends[1], out_grad, ends[2], ends[3], ends[4],
        up_grad, ends[8], down_grad, ends[5], ends[6], ends[7], ends[9],
    )


def place_rows(half, own, send):
    came = swap(send)
    return [
        jnp.where(half == 0, jnp.stack([own[i], came[i]]), jnp.stack([came[i], own[i]]))
        for i in range(2)
    ]


def solution(mesh):
    rows3 = P("dp", "seq", None)
    flat, first, last = P("dp"), P("dp", None), P(None, "dp")
    in_specs = (
        rows3, rows3, rows3, rows3, first, first, first, flat, first, first, flat, first, flat,
        flat, flat, last, flat, first, flat, flat, flat, flat,
    )
    out_specs = (
        rows3, rows3, rows3, rows3, first, flat, first, first, flat, first, flat, flat, flat,
        last, flat, first, flat, flat, flat, flat,
    )
    body = functools.partial(shards, mesh.shape["dp"])
    return jax.shard_map(
        body, mesh=mesh, in_specs=in_specs, out_specs=out_specs, check_vma=False
    )
```

```python
import functools
import math

import jax
import jax.numpy as jnp
from jax import lax
from jax.experimental import pallas as pl
from jax.experimental.pallas import tpu as pltpu
from jax.sharding import PartitionSpec as P

HEADS = 12
HEAD_DIM = 64
BUCKETS = 32
GROUP = 4
LANES = GROUP * HEAD_DIM
GROUPS = HEADS // GROUP
TILE = 128
TILES = 4
NEG = -1e30
FLOOR = -1e29
EPS = 1e-05

limits = (1, 2, 3, 4, 5, 6, 7, 8, 12, 16, 23, 32, 46, 64, 91)

NN = (((1,), (0,)), ((), ()))
NT = (((1,), (1,)), ((), ()))
TN = (((0,), (0,)), ((), ()))
VMEM_SPEC = pl.BlockSpec(memory_space=pltpu.VMEM)
ANY_SPEC = pl.BlockSpec(memory_space=pl.ANY)
HBM_SPEC = pl.BlockSpec(memory_space=pltpu.HBM)
SCALE = 1.6e6
SMEM_SPEC = pl.BlockSpec(memory_space=pltpu.SMEM)
SDS = jax.ShapeDtypeStruct


def cost(micros):
    return pl.CostEstimate(
        flops=0, bytes_accessed=int(micros * SCALE), transcendentals=0
    )


def product(left, right, dims=NN):
    return lax.dot_general(left, right, dims, preferred_element_type=jnp.float32)


def params(semantics=None, limit=56):
    return pltpu.CompilerParams(dimension_semantics=semantics, vmem_limit_bytes=limit << 20)


def row_sum(values):
    return jnp.sum(values, axis=-1, keepdims=True)


ME, HALF = 0, 1
VECTORS, UP_SLOT, TABLE_SLOT = 10, 8, 9
FIRST_TILES, LAST_TILES = 3 * GROUPS, 4
FULL = 60


def in_hbm(*values):
    return [pltpu.with_memory_space_constraint(value, pltpu.HBM) for value in values]


def run_copies(copies):
    for copy in copies:
        copy.start()
    for copy in copies:
        copy.wait()


def pack_kernel(ids, content, query, ccot, qcot, wq, wk, wv, wo, up, down, *rest):
    vectors, rest = rest[:VECTORS], rest[VECTORS:]
    (theirs, square, feed, slots, tokens, squares, feeds, in_sems, out_sems) = rest
    half = ids[HALF]
    share = feed.shape[1]
    loads = []

    def load(source, target):
        copy = pltpu.make_async_copy(source, target, in_sems.at[len(loads)])
        copy.start()
        loads.append(copy)

    for index, weight in enumerate((wq, wk, wv, wo)):
        for group in range(GROUPS):
            lane = pl.multiple_of(group * LANES + half * 128, 128)
            place = 3 * group + index if index < 3 else 3 * GROUPS + group
            load(weight.at[:, pl.ds(lane, 128)], squares.at[place])
    for index, source in enumerate((content, query, ccot, qcot)):
        load(source.at[1 - half], tokens.at[index])
    rows = pl.ds(pl.multiple_of(half * share, share), share)
    load(up.at[rows, :], feeds.at[0])
    load(down.at[rows, :], feeds.at[1])
    slots[...] = jnp.zeros_like(slots)
    for index, vector in enumerate(vectors):
        slots[index : index + 1, : vector.shape[1]] = vector[...]
    for copy in loads[: 4 * GROUPS]:
        copy.wait()
    stores = [
        pltpu.make_async_copy(squares, square, out_sems.at[0]),
        pltpu.make_async_copy(tokens, theirs, out_sems.at[1]),
        pltpu.make_async_copy(feeds, feed, out_sems.at[2]),
    ]
    stores[0].start()
    for copy in loads[4 * GROUPS :]:
        copy.wait()
    stores[1].start()
    stores[2].start()
    for copy in stores:
        copy.wait()


def pack(ids, content, query, ccot, qcot, wq, wk, wv, wo, up, down, vectors):
    _, block, width = content.shape
    rows = wq.shape[0]
    hidden = up.shape[0]
    return pl.pallas_call(
        pack_kernel,
        out_shape=(
            SDS((4, block, width), jnp.bfloat16),
            SDS((4 * GROUPS, rows, 128), jnp.bfloat16),
            SDS((2, hidden // 2, width), jnp.bfloat16),
            SDS((16, 256), jnp.bfloat16),
        ),
        in_specs=[SMEM_SPEC] + [HBM_SPEC] * 10 + [VMEM_SPEC] * VECTORS,
        out_specs=(HBM_SPEC,) * 3 + (VMEM_SPEC,),
        scratch_shapes=[
            pltpu.VMEM((4, block, width), jnp.bfloat16),
            pltpu.VMEM((4 * GROUPS, rows, 128), jnp.bfloat16),
            pltpu.VMEM((2, hidden // 2, width), jnp.bfloat16),
            pltpu.SemaphoreType.DMA((4 * GROUPS + 6,)),
            pltpu.SemaphoreType.DMA((3,)),
        ],
        cost_estimate=cost(4),
        compiler_params=params(None, FULL),
        name="pack",
    )(ids, *in_hbm(content, query, ccot, qcot, wq, wk, wv, wo, up, down),
      *(vector.reshape(1, -1) for vector in vectors))


def order_onehot(ids, order):
    length = order.shape[1]
    row = order[pl.ds(ids[HALF], 1), :]
    down = lax.broadcasted_iota(jnp.int32, (length, length), 0)
    return jnp.where(row == down, 1.0, 0.0).astype(jnp.bfloat16)


def sort_kernel(ids, lengths, content, query, ccot, qcot, came, order,
                xs_out, cs_out, mask_out, held, sems):
    length = order.shape[1]
    block = content.shape[1]
    half = ids[HALF]
    copies = []
    for index, source in enumerate((content, query, ccot, qcot)):
        for place, rows in ((half, source.at[half]), (1 - half, came.at[index])):
            here = pl.ds(pl.multiple_of(place * block, block), block)
            copies.append(
                pltpu.make_async_copy(rows, held.at[index, here], sems.at[len(copies)])
            )
    for copy in copies:
        copy.start()
    onehot = order_onehot(ids, order)
    lane = lax.broadcasted_iota(jnp.int32, (8, length), 1)
    line = lax.broadcasted_iota(jnp.int32, (8, length), 0)
    digits = jnp.where(line == 0, lane // 16, jnp.where(line == 1, lane % 16, 0))
    digits = product(digits.astype(jnp.float32).astype(jnp.bfloat16), onehot, NT)
    rank_row = digits[0:1, :] * 16.0 + digits[1:2, :]
    across = lax.broadcasted_iota(jnp.int32, (length, length), 1).astype(jnp.float32)
    rank_col = row_sum(onehot.astype(jnp.float32) * across)
    place_col = lax.broadcasted_iota(jnp.int32, (length, 1), 0)
    place_row = lax.broadcasted_iota(jnp.int32, (1, length), 1)
    segment_col = jnp.zeros((length, 1), jnp.int32)
    segment_row = jnp.zeros((1, length), jnp.int32)
    bound = jnp.int32(0)
    for index in range(lengths.shape[1] - 1):
        bound = bound + lengths[half, index]
        segment_col = segment_col + (place_col >= bound).astype(jnp.int32)
        segment_row = segment_row + (place_row >= bound).astype(jnp.int32)
    same = segment_col == segment_row
    mask_out[0] = jnp.where(same & (rank_row <= rank_col), 0.0, NEG).astype(jnp.bfloat16)
    mask_out[1] = jnp.where(same & (rank_row < rank_col), 0.0, NEG).astype(jnp.bfloat16)
    for copy in copies:
        copy.wait()
    for source, target, at in ((0, xs_out, 0), (1, xs_out, 1), (2, cs_out, 0), (3, cs_out, 1)):
        target[at * length : (at + 1) * length, :] = product(onehot, held[source]).astype(
            jnp.bfloat16
        )


def sort_rows(ids, lengths, tokens, came, order):
    length = order.shape[1]
    width = came.shape[2]
    return pl.pallas_call(
        sort_kernel,
        out_shape=(
            SDS((2 * length, width), jnp.bfloat16),
            SDS((2 * length, width), jnp.bfloat16),
            SDS((2, length, length), jnp.bfloat16),
        ),
        in_specs=[SMEM_SPEC] * 2 + [HBM_SPEC] * 5 + [VMEM_SPEC],
        out_specs=(VMEM_SPEC,) * 3,
        scratch_shapes=[
            pltpu.VMEM((4, length, width), jnp.bfloat16),
            pltpu.SemaphoreType.DMA((8,)),
        ],
        cost_estimate=cost(5),
        compiler_params=params(None, FULL),
        name="sort_rows",
    )(ids, lengths, *in_hbm(*tokens, came), order)


def put_back(ids, onehot, source, scratch, own, send, sems):
    length = onehot.shape[0]
    block = own.shape[1]
    for stream in range(2):
        rows = product(onehot, source(stream), TN).astype(jnp.bfloat16)
        scratch[0, stream] = rows[:block, :]
        scratch[1, stream] = rows[block:, :]
    return [
        pltpu.make_async_copy(scratch.at[ids[HALF]], own, sems.at[0]),
        pltpu.make_async_copy(scratch.at[1 - ids[HALF]], send, sems.at[1]),
    ]


def unsort_kernel(ids, order, values, own, send, held, scratch, sems):
    length = order.shape[1]
    copy = pltpu.make_async_copy(values, held, sems.at[2])
    copy.start()
    onehot = order_onehot(ids, order)
    copy.wait()
    run_copies(put_back(
        ids, onehot, lambda s: held[s * length : (s + 1) * length, :], scratch, own, send, sems
    ))


def unsort_rows(ids, order, values):
    length = order.shape[1]
    width = values.shape[1]
    shape = SDS((2, length // 2, width), jnp.bfloat16)
    return pl.pallas_call(
        unsort_kernel,
        out_shape=(shape, shape),
        in_specs=[SMEM_SPEC, VMEM_SPEC, HBM_SPEC],
        out_specs=(HBM_SPEC, HBM_SPEC),
        scratch_shapes=[
            pltpu.VMEM((2 * length, width), jnp.bfloat16),
            pltpu.VMEM((2, 2, length // 2, width), jnp.bfloat16),
            pltpu.SemaphoreType.DMA((3,)),
        ],
        cost_estimate=cost(3),
        compiler_params=params(None, FULL),
        name="unsort_rows",
    )(ids, order, *in_hbm(values))


SPAN = 5 * TILE
TURN = 6 * TILE


def bucket_onehot():
    distance = lax.broadcasted_iota(jnp.int32, (BUCKETS, TURN), 1) - (3 * TILE - 1)
    magnitude = jnp.abs(distance)
    counted = jnp.zeros(distance.shape, jnp.int32)
    for limit in limits:
        counted = counted + (magnitude >= limit).astype(jnp.int32)
    bucket = counted + 16 * (distance > 0).astype(jnp.int32)
    return bucket == lax.broadcasted_iota(jnp.int32, distance.shape, 0)


def block_flip(ids, own, far, block, count):
    place = ids[HALF] if own else 1 - ids[HALF]
    first = jnp.where(place == 0, 1, 2)
    high = count // 2
    flip = jnp.int32(4 * (block % high))
    if block >= high:
        flip = flip ^ first
    return flip ^ (3 - first) if far else flip


def block_places(ids, pieces):
    places = []
    for index, piece in enumerate(pieces):
        own = index < len(pieces) // 2
        place = ids[HALF] if own else 1 - ids[HALF]
        for block in range(piece.shape[0]):
            if len(pieces) == 2:
                places.append((index, block, place, 0))
            else:
                flip = block_flip(ids, own, index % 2 == 1, block, piece.shape[0])
                places.append((index, block, place, ids[ME] ^ flip))
    return places


def block_copies(ids, pieces, target, sems, tiles):
    copies = []
    for index, block, place, chip in block_places(ids, pieces):
        rows = pieces[index].shape[2]
        here = pl.ds(pl.multiple_of(chip * rows, rows), rows)
        copies.append(
            pltpu.make_async_copy(
                pieces[index].at[block, tiles], target.at[place, :, here, :],
                sems.at[len(copies)],
            )
        )
    return copies


def block_stores(ids, source, outs, sems, tiles):
    copies = []
    for index, block, place, chip in block_places(ids, outs):
        rows = outs[index].shape[2]
        here = pl.ds(pl.multiple_of(chip * rows, rows), rows)
        copies.append(
            pltpu.make_async_copy(
                source.at[place, :, here, :], outs[index].at[block, tiles],
                sems.at[len(copies)],
            )
        )
    return copies


def joined(weights, index):
    return jnp.concatenate([weights[0, index], weights[1, index]], axis=1)


def store_shapes(pieces, tiles):
    return tuple(SDS((p.shape[0], tiles) + p.shape[2:], jnp.bfloat16) for p in pieces)


def vectors_kernel(width, sizes, ids, near, far, rows_out, up_out, bias_out):
    count = 2 * near.shape[0]
    half = ids[HALF]
    high = count // 4
    total = jnp.zeros((16, width), jnp.float32)
    table = jnp.zeros((16, width), jnp.float32)
    blank = jnp.zeros((16, width - 256), jnp.float32)
    slot = lax.broadcasted_iota(jnp.int32, (16, width), 0)
    blocks = [[], []]
    for side, part in enumerate((near, far)):
        for block in range(part.shape[0]):
            chip = ids[ME] ^ block_flip(ids, True, side == 1, block, part.shape[0])
            values = jnp.concatenate([part[block].astype(jnp.float32), blank], axis=1)
            blocks[side].append(values)
            total = total + pltpu.roll(
                jnp.where(slot < UP_SLOT, values, 0.0), chip * sizes[0], 1
            )
            table = table + pltpu.roll(
                jnp.where(slot == TABLE_SLOT, values, 0.0), chip * sizes[TABLE_SLOT], 1
            )
    rows_out[...] = total[2:10, :]
    rows_out[6:8, :] = total[0:2, :]
    share = sizes[UP_SLOT] // 2
    lane = lax.broadcasted_iota(jnp.int32, (16, width), 1)
    keep = (slot == UP_SLOT) & (lane < share)
    near_blocks, far_blocks = blocks
    order = (
        (half, near_blocks[:high] + near_blocks[high:]),
        (1 - half, near_blocks[:high] + far_blocks[:high]),
        (half, far_blocks[:high] + far_blocks[high:]),
        (1 - half, near_blocks[high:] + far_blocks[high:]),
    )
    for index, (place, parts) in enumerate(order):
        joint = jnp.zeros((16, width), jnp.float32)
        for block, values in enumerate(parts):
            values = pltpu.roll(values, lax.rem(width - place * share, width), 1)
            joint = joint + pltpu.roll(jnp.where(keep, values, 0.0), block * share, 1)
        up_out[:, index * width : (index + 1) * width] = joint[UP_SLOT : UP_SLOT + 1, :]
    flat = table[TABLE_SLOT : TABLE_SLOT + 1, : BUCKETS * HEADS]
    entry = lax.broadcasted_iota(jnp.int32, (16, BUCKETS * HEADS), 1)
    head = lax.broadcasted_iota(jnp.int32, (16, BUCKETS * HEADS), 0)
    spread_heads = jnp.where(entry % HEADS == head, flat, 0.0).astype(jnp.bfloat16)
    place = lax.broadcasted_iota(jnp.int32, (BUCKETS, BUCKETS * HEADS), 1) // HEADS
    bucket = lax.broadcasted_iota(jnp.int32, (BUCKETS, BUCKETS * HEADS), 0)
    folded = product(spread_heads, jnp.where(place == bucket, 1.0, 0.0).astype(jnp.bfloat16), NT)
    onehot = jnp.where(bucket_onehot(), 1.0, 0.0).astype(jnp.bfloat16)
    rows = product(folded.astype(jnp.bfloat16), onehot)
    for head in range(HEADS):
        spread = jnp.broadcast_to(rows[head : head + 1, :], (TILE, TURN))
        turned = pltpu.roll(spread, TURN - (TILE - 1), 1, stride=1, stride_axis=0)
        bias_out[head] = turned[:, :SPAN].astype(jnp.bfloat16)


def vectors_to_all(ids, near, far, width, sizes):
    return pl.pallas_call(
        functools.partial(vectors_kernel, width, sizes),
        out_shape=(
            SDS((8, width), jnp.float32),
            SDS((1, 4 * width), jnp.float32),
            SDS((HEADS, TILE, SPAN), jnp.bfloat16),
        ),
        in_specs=[SMEM_SPEC] + [VMEM_SPEC] * 2,
        out_specs=(VMEM_SPEC,) * 3,
        cost_estimate=cost(6),
        compiler_params=params(None, FULL),
        name="vectors",
    )(ids, near, far)


def head_lanes(head, shape):
    lane = lax.broadcasted_iota(jnp.int32, shape, 1)
    return (lane >= head * HEAD_DIM) & (lane < (head + 1) * HEAD_DIM)


def head_stack(values):
    low = jnp.zeros((), values.dtype)
    return jnp.concatenate(
        [jnp.where(head_lanes(h, values.shape), values, low) for h in range(GROUP)]
    )


def head_merge(stack, rows):
    total = stack[(GROUP - 1) * rows :, :]
    for h in range(GROUP - 1):
        part = stack[h * rows : (h + 1) * rows, :]
        total = jnp.where(head_lanes(h, part.shape), part, total)
    return total


def widen(values, lanes):
    return jnp.concatenate([values] * (lanes // 128), axis=1)


def by_width(ids, lengths, tile, body):
    half = ids[HALF]
    begin, end = tile * TILE, (tile + 1) * TILE
    bound = jnp.int32(0)
    low, high = jnp.int32(0), jnp.int32(TILES * TILE)
    for index in range(lengths.shape[1] - 1):
        bound = bound + lengths[half, index]
        low = jnp.where(bound <= begin, bound, low)
        high = jnp.where(bound >= end, jnp.minimum(bound, high), high)
    first = low // TILE
    width = jnp.maximum((high + TILE - 1) // TILE - first, 2)
    first = pl.multiple_of(jnp.minimum(first, TILES - width) * TILE, TILE)
    for count in range(2, TILES + 1):
        pl.when(width == count)(functools.partial(body, first, count * TILE))


def attend_kernel(ids, lengths, xs, mask, bias, rows, *rest):
    pieces, rest = rest[:-8], rest[-8:]
    q_out, k_out, v_out, mixed_out, lse_out, weights, values, sems = rest
    length = mask.shape[1]
    group = pl.program_id(0)

    def weight_copies(index):
        tiles = pl.ds(3 * index, 3)
        return block_copies(ids, pieces, weights.at[:, tiles], sems.at[index], tiles)

    @pl.when(group == 0)
    def _():
        for index in range(GROUPS):
            for copy in weight_copies(index):
                copy.start()

    for index in range(GROUPS):
        @pl.when(group == index)
        def _():
            for copy in weight_copies(index):
                copy.wait()

    q = product(xs[...], joined(weights, 3 * group)) + rows[6:7, :]
    q_out[...] = q.astype(jnp.bfloat16)
    k = product(xs[0:length, :], joined(weights, 3 * group + 1))
    k_out[...] = k.astype(jnp.bfloat16)
    v = product(xs[0:length, :], joined(weights, 3 * group + 2)) + rows[7:8, :]
    v_out[...] = v.astype(jnp.bfloat16)

    wide_lanes = lax.broadcasted_iota(jnp.int32, v.shape, 1) < 128
    one = jnp.ones((), jnp.bfloat16)
    values[0] = jnp.where(wide_lanes, v_out[...], one)
    values[1] = jnp.where(wide_lanes, one, v_out[...])

    def tile_step(tile, carry):
        def body(first, keys):
            there = pl.ds(first, keys)
            near = pl.ds(pl.multiple_of((2 - tile) * TILE + first, TILE), keys)
            here = pl.ds(pl.multiple_of(tile * TILE, TILE), TILE)
            key = k_out[there, :]
            for stream in range(2):
                at = pl.ds(pl.multiple_of(stream * length + tile * TILE, TILE), TILE)
                scores = product(head_stack(q_out[at, :] * jnp.bfloat16(0.125)), key, NT)
                masked = mask[stream, here, there].astype(jnp.float32)
                weights, peaks, logs = [], [], []
                for h in range(GROUP):
                    part = scores[h * TILE : (h + 1) * TILE, :] + bias[h, :, near].astype(jnp.float32) + masked
                    peak = jnp.maximum(jnp.max(part, axis=-1, keepdims=True), FLOOR)
                    weights.append(jnp.exp(part - peak).astype(jnp.bfloat16))
                    peaks.append(peak)
                for pair in range(2):
                    both = jnp.concatenate(weights[2 * pair : 2 * pair + 2])
                    both = product(both, values[pair, there, :])
                    top = slice(pair * 128, pair * 128 + 128)
                    low = slice(128 - pair * 128, 256 - pair * 128)
                    parts = []
                    for h in range(2):
                        rows = slice(h * TILE, (h + 1) * TILE)
                        summed = both[rows, low]
                        alive = summed > 0
                        inverse = jnp.where(alive, 1.0 / summed, 0.0)
                        parts.append(both[rows, top] * inverse)
                        logs.append(
                            jnp.where(alive, peaks[2 * pair + h] + jnp.log(summed), 0.0)
                        )
                    lane = lax.broadcasted_iota(jnp.int32, parts[0].shape, 1)
                    mixed = jnp.where(lane < HEAD_DIM, parts[0], parts[1])
                    mixed_out[at, top] = mixed.astype(jnp.bfloat16)
                packed = logs[0]
                for h in range(1, GROUP):
                    packed = jnp.where(lane == h, logs[h], packed)
                lse_out[0, at, :] = packed

        by_width(ids, lengths, tile, body)
        return carry

    lax.fori_loop(0, length // TILE, tile_step, 0)


def attend(ids, lengths, xs, mask, bias, rows, pieces):
    tokens, width = xs.shape
    length = mask.shape[1]
    blocks = sum(piece.shape[0] for piece in pieces)
    full = lambda g: (0, 0)
    column = lambda g: (0, g)
    once = pl.Buffered(1)
    return pl.pallas_call(
        attend_kernel,
        grid=(GROUPS,),
        out_shape=(
            SDS((tokens, width), jnp.bfloat16),
            SDS((length, width), jnp.bfloat16),
            SDS((length, width), jnp.bfloat16),
            SDS((tokens, width), jnp.bfloat16),
            SDS((GROUPS, tokens, 128), jnp.float32),
        ),
        in_specs=[
            SMEM_SPEC,
            SMEM_SPEC,
            pl.BlockSpec((tokens, width), full, pipeline_mode=once),
            pl.BlockSpec((2, length, length), lambda g: (0, 0, 0), pipeline_mode=once),
            pl.BlockSpec((GROUP, TILE, SPAN), lambda g: (g, 0, 0)),
            pl.BlockSpec((8, LANES), column),
        ] + [HBM_SPEC] * len(pieces),
        out_specs=(
            pl.BlockSpec((tokens, LANES), column),
            pl.BlockSpec((length, LANES), column),
            pl.BlockSpec((length, LANES), column),
            pl.BlockSpec((tokens, LANES), column),
            pl.BlockSpec((1, tokens, 128), lambda g: (g, 0, 0)),
        ),
        scratch_shapes=[
            pltpu.VMEM((2, 3 * GROUPS, width, 128), jnp.bfloat16),
            pltpu.VMEM((2, length, LANES), jnp.bfloat16),
            pltpu.SemaphoreType.DMA((GROUPS, blocks)),
        ],
        cost_estimate=cost(18),
        compiler_params=params(("arbitrary",), FULL),
        name="attend",
    )(ids, lengths, xs, mask, bias, rows, *in_hbm(*pieces))


def norm_parts(values):
    mean = jnp.mean(values, axis=-1, keepdims=True)
    center = values - mean
    spread = jnp.mean(center * center, axis=-1, keepdims=True)
    scale = lax.rsqrt(spread + EPS)
    return center * scale, scale


def norm_back(normal, scale, grad):
    mean = jnp.mean(grad, axis=-1, keepdims=True)
    inner = jnp.mean(grad * normal, axis=-1, keepdims=True)
    return scale * (grad - mean - normal * inner)


def column_sum(values):
    return jnp.sum(values, axis=0, keepdims=True)


BLOCK = 256


def feed_kernel(ids, xs, mixed, cot, rows, up_bias, near_own, near_other, far_own, far_other,
                *rest):
    pieces, rest = rest[:-14], rest[-14:]
    (out, act_out, gup_out, first_out, gdown_out, gres_out, gbranch_out, gmixed_out,
     sums, up_sums, up_all, down_all, wo_all, sems) = rest
    step = pl.program_id(0)
    units = up_all.shape[0] // 4
    parts = (near_own, near_other, far_own, far_other)
    held = sum(piece.shape[0] for piece in pieces)

    def weight_copies():
        copies = []
        share = near_own.shape[2]
        for index, part in enumerate(parts):
            for block in range(part.shape[0]):
                here = slice(index * units + block * share, index * units + (block + 1) * share)
                for which, target in ((0, up_all), (1, down_all)):
                    copies.append(
                        pltpu.make_async_copy(
                            part.at[block, which], target.at[here, :],
                            sems.at[held + len(copies)],
                        )
                    )
        return copies

    @pl.when(step == 0)
    def _():
        sums[...] = jnp.zeros_like(sums)
        up_sums[...] = jnp.zeros_like(up_sums)
        copies = block_copies(ids, pieces, wo_all, sems, slice(3 * GROUPS, 4 * GROUPS))
        copies += weight_copies()
        run_copies(copies)

    wo = jnp.concatenate([joined(wo_all, index) for index in range(GROUPS)], axis=1)
    branch = product(mixed[...], wo) + rows[0:1, :]

    normal1, scale1 = norm_parts(xs[...].astype(jnp.float32) + branch)
    first = normal1 * rows[1:2, :] + rows[2:3, :]
    first_low = first.astype(jnp.bfloat16)
    first_out[...] = first_low
    slopes = []
    second = first + rows[3:4, :]
    for index in range(2):
        here = slice(2 * index * units, 2 * (index + 1) * units)
        up = product(first_low, up_all[here, :], NT) + up_bias[:, here]
        gate = 0.5 + 0.5 * lax.erf(up * math.sqrt(0.5))
        act = (up * gate).astype(jnp.bfloat16)
        act_out[:, here] = act
        slopes.append(gate + up * jnp.exp(-0.5 * up * up) * (1.0 / math.sqrt(2.0 * math.pi)))
        second = second + product(act, down_all[here, :])
    normal2, scale2 = norm_parts(second)
    gain = rows[4:5, :]
    out[...] = (normal2 * gain + rows[5:6, :]).astype(jnp.bfloat16)
    cots = cot[...].astype(jnp.float32)
    gsecond = norm_back(normal2, scale2, cots * gain)
    gdown = gsecond.astype(jnp.bfloat16)
    gdown_out[...] = gdown
    gfirst = gsecond
    for index in range(2):
        here = slice(2 * index * units, 2 * (index + 1) * units)
        gup = (product(gdown, down_all[here, :], NT) * slopes[index]).astype(jnp.bfloat16)
        gup_out[:, here] = gup
        up_sums[:, here] += column_sum(gup.astype(jnp.float32))
        gfirst = gfirst + product(gup, up_all[here, :])
    gres = norm_back(normal1, scale1, gfirst * rows[1:2, :])
    gres_out[...] = gres
    gbranch = gres.astype(jnp.bfloat16)
    gbranch_out[...] = gbranch
    gmixed_out[...] = product(gbranch, wo, NT).astype(jnp.bfloat16)
    sums[0:1, :] += column_sum(gbranch.astype(jnp.float32))
    sums[1:2, :] += column_sum(gfirst * normal1)
    sums[2:3, :] += column_sum(gfirst)
    sums[3:4, :] += column_sum(gdown.astype(jnp.float32))
    sums[4:5, :] += column_sum(cots * normal2)
    sums[5:6, :] += column_sum(cots)


def feed(ids, xs, mixed, cot, rows, up_bias, feeds, pieces):
    tokens, width = xs.shape
    hidden = up_bias.shape[1]
    token = pl.BlockSpec((BLOCK, width), lambda i: (i, 0))
    wide = pl.BlockSpec((BLOCK, hidden), lambda i: (i, 0))
    held = sum(piece.shape[0] for piece in pieces) + 2 * sum(part.shape[0] for part in feeds)
    low = SDS((tokens, width), jnp.bfloat16)
    return pl.pallas_call(
        feed_kernel,
        grid=(tokens // BLOCK,),
        out_shape=(
            low,
            SDS((tokens, hidden), jnp.bfloat16),
            SDS((tokens, hidden), jnp.bfloat16),
            low,
            low,
            SDS((tokens, width), jnp.float32),
            low,
            low,
            SDS((8, width), jnp.float32),
            SDS((1, hidden), jnp.float32),
        ),
        in_specs=[
            SMEM_SPEC, token, token, token,
            pl.BlockSpec((8, width), lambda i: (0, 0)),
            pl.BlockSpec((1, hidden), lambda i: (0, 0)),
        ] + [ANY_SPEC] * 4 + [HBM_SPEC] * len(pieces),
        out_specs=(token, wide, wide, token, token, token, token, token,
                   pl.BlockSpec((8, width), lambda i: (0, 0)),
                   pl.BlockSpec((1, hidden), lambda i: (0, 0))),
        scratch_shapes=[
            pltpu.VMEM((hidden, width), jnp.bfloat16),
            pltpu.VMEM((hidden, width), jnp.bfloat16),
            pltpu.VMEM((2, GROUPS, width, 128), jnp.bfloat16),
            pltpu.SemaphoreType.DMA((held,)),
        ],
        cost_estimate=cost(36),
        compiler_params=params(("arbitrary",), FULL),
        name="feed",
    )(ids, xs, mixed, cot, rows, up_bias, *feeds, *in_hbm(*pieces))


def feed_weights_kernel(act, gup, first, gdown, own, other):
    which = pl.program_id(1)

    def put(grad):
        share = own.shape[2]
        grad = grad.astype(jnp.bfloat16)

        def store(out):
            for block in range(out.shape[0]):
                out[block, 0] = grad[block * share : (block + 1) * share, :]

        pl.when(pl.program_id(0) == 0)(lambda: store(other))
        pl.when(pl.program_id(0) == 1)(lambda: store(own))

    pl.when(which == 0)(lambda: put(product(gup[...], first[...], TN)))
    pl.when(which == 1)(lambda: put(product(act[...], gdown[...], TN)))


def feed_weights(part, act, gup, first, gdown, shape):
    tokens, width = first.shape
    units = shape[0] * shape[2]
    full = pl.BlockSpec((tokens, width), lambda s, u: (0, 0), pipeline_mode=pl.Buffered(1))
    lanes = pl.BlockSpec((tokens, units), lambda s, u: (0, 2 * part + 1 - s))
    block = (shape[0], 1) + shape[2:]
    return pl.pallas_call(
        feed_weights_kernel,
        grid=(2, 2),
        out_shape=(SDS(shape, jnp.bfloat16),) * 2,
        in_specs=[lanes, lanes, full, full],
        out_specs=(
            pl.BlockSpec(block, lambda s, u: (0, s * u, 0, 0)),
            pl.BlockSpec(block, lambda s, u: (0, jnp.maximum(s, u), 0, 0)),
        ),
        cost_estimate=cost(9),
        compiler_params=params(("arbitrary", "arbitrary"), FULL),
        name="feed_weights",
    )(act, gup, first, gdown)


def out_weights_kernel(ids, mixed, gbranch, *rest):
    outs, (buffer, sems) = rest[:-2], rest[-2:]
    grad = product(mixed[...], gbranch[...], TN).astype(jnp.bfloat16)
    for index in range(GROUPS):
        for half in range(2):
            lane = index * LANES + half * 128
            buffer[half, index] = grad[:, lane : lane + 128]
    run_copies(block_stores(ids, buffer, outs, sems, slice(2 * GROUPS, 3 * GROUPS)))


def out_weights(ids, mixed, gbranch, pieces):
    tokens, width = mixed.shape
    blocks = sum(piece.shape[0] for piece in pieces)
    full = pl.BlockSpec((tokens, width), lambda i: (0, 0))
    return pl.pallas_call(
        out_weights_kernel,
        grid=(1,),
        out_shape=store_shapes(pieces, FIRST_TILES),
        in_specs=[SMEM_SPEC, full, full],
        out_specs=(HBM_SPEC,) * len(pieces),
        scratch_shapes=[
            pltpu.VMEM((2, GROUPS, width, 128), jnp.bfloat16),
            pltpu.SemaphoreType.DMA((blocks,)),
        ],
        cost_estimate=cost(4),
        compiler_params=params(("arbitrary",), FULL),
        name="out_weights",
    )(ids, mixed, gbranch)


def attend_back_kernel(ids_rows, base, steps, ids, lengths, order, mask, bias, q, k, v, mixed, gmixed, lse, sums,
                       up_sums, xs_far, gres, *rest):
    scratch = rest[-17:]
    done = base + steps == GROUPS
    count = (len(rest) - 17 - 2) // (2 if done else 3)
    pieces = rest[:count]
    if done:
        own, send, *gw_outs = rest[count:-17]
    else:
        gx_out, vectors_out, *gw_outs = rest[2 * count : -17]
    (vectors, turned, vector_sems, gk, gv, gdist, gx, gq, inner, weights, buffer, xs, rows_out, sems, in_sems, out_sems,
     row_sems) = scratch
    step = pl.program_id(0)
    group = base + step
    tiles = slice(3 * base, 3 * (base + steps))
    length = mask.shape[1]
    rows = xs.shape[1] // (2 * gw_outs[0].shape[0]) if count > 2 else ids_rows
    loads = block_copies(ids, pieces, weights, sems, tiles) + [
        pltpu.make_async_copy(xs_far, xs, in_sems.at[0]),
        pltpu.make_async_copy(gres, gx, in_sems.at[1]),
    ]

    def stores(index):
        return block_stores(
            ids, buffer.at[index], gw_outs, out_sems.at[index],
            slice(0, 3) if done else pl.ds(3 * (base + index), 3),
        )

    @pl.when(step == 0)
    def _():
        for copy in loads:
            copy.start()
        if base:
            vectors[0:16, :] = sums[8:24, :]

    gdist[...] = jnp.zeros_like(gdist)
    gk[...] = jnp.zeros_like(gk)
    gv[...] = jnp.zeros_like(gv)

    lane = lax.broadcasted_iota(jnp.int32, (LANES, GROUP * 128), 0) // HEAD_DIM
    head = lax.broadcasted_iota(jnp.int32, (LANES, GROUP * 128), 1) // 128
    adder = jnp.where(lane == head, 1.0, 0.0).astype(jnp.bfloat16)
    crossed = mixed[...].astype(jnp.float32) * gmixed[...].astype(jnp.float32)
    inner[...] = product(crossed.astype(jnp.bfloat16), adder)

    def tile_step(tile, carry):
        def body(first, keys):
            there = pl.ds(first, keys)
            near = pl.ds(pl.multiple_of((2 - tile) * TILE + first, TILE), keys)
            here = pl.ds(pl.multiple_of(tile * TILE, TILE), TILE)
            key = k[there, :]
            value = v[there, :]
            at = [
                pl.ds(pl.multiple_of(stream * length + tile * TILE, TILE), TILE)
                for stream in range(2)
            ]
            query = jnp.concatenate([head_stack(q[at[s], :] * jnp.bfloat16(0.125)) for s in range(2)])
            gmix = jnp.concatenate([head_stack(gmixed[at[s], :]) for s in range(2)])
            scores = product(query, key, NT)
            gprobs = product(gmix, value, NT)
            masked = [mask[s, here, there].astype(jnp.float32) for s in range(2)]
            probs_low = [None] * (2 * GROUP)
            gscores_low = [None] * (2 * GROUP)
            for h in range(GROUP):
                both = None
                near_bias = bias[h, :, near].astype(jnp.float32)
                for stream in range(2):
                    index = stream * GROUP + h
                    part = slice(index * TILE, (index + 1) * TILE)
                    score = scores[part, :] + near_bias + masked[stream]
                    probs = jnp.exp(score - lse[0, at[stream], h : h + 1])
                    lanes = slice(h * 128, (h + 1) * 128)
                    gscores = probs * (gprobs[part, :] - widen(inner[at[stream], lanes], keys))
                    probs_low[index] = probs.astype(jnp.bfloat16)
                    gscores_low[index] = gscores.astype(jnp.bfloat16)
                    both = gscores if both is None else both + gscores
                gdist[h, :, near] += both
            probs_low = jnp.concatenate(probs_low)
            gscores_low = jnp.concatenate(gscores_low)
            gv[there, :] += product(probs_low, gmix, TN)
            gk[there, :] += product(gscores_low, query, TN)
            back = product(gscores_low, key)
            for stream in range(2):
                part = slice(stream * GROUP * TILE, (stream + 1) * GROUP * TILE)
                gq[at[stream], :] = head_merge(back[part, :], TILE)

        by_width(ids, lengths, tile, body)
        return carry

    lax.fori_loop(0, length // TILE, tile_step, 0)
    gq_low = (gq[...] * 0.125).astype(jnp.bfloat16)
    gk_low = gk[...].astype(jnp.bfloat16)
    gv_low = gv[...].astype(jnp.bfloat16)

    @pl.when(step == 0)
    def _():
        for copy in loads:
            copy.wait()

    for index, grad in enumerate((
        product(xs[...], gq_low, TN),
        product(xs[0:length, :], gk_low, TN),
        product(xs[0:length, :], gv_low, TN),
    )):
        grad = grad.astype(jnp.bfloat16)
        buffer[step, 0, index] = grad[:, :128]
        buffer[step, 1, index] = grad[:, 128:]
    for index in range(steps):
        @pl.when(step == index)
        def _():
            for copy in stores(index):
                copy.start()

    gx[...] += product(gq_low, joined(weights, 3 * step), NT)
    gx[0:length, :] += product(gk_low, joined(weights, 3 * step + 1), NT) + product(
        gv_low, joined(weights, 3 * step + 2), NT
    )
    if done:
        sends = put_back(
            ids, order_onehot(ids, order),
            lambda s: gx[s * length : (s + 1) * length, :].astype(jnp.bfloat16),
            rows_out, own, send, row_sems,
        )
    else:
        sends = [pltpu.make_async_copy(gx, gx_out, in_sems.at[0])]
    for copy in sends:
        copy.start()
    lanes = pl.ds(pl.multiple_of(group * LANES, LANES), LANES)
    vectors[0:1, lanes] = column_sum(gq_low.astype(jnp.float32))
    vectors[1:2, lanes] = column_sum(gv_low.astype(jnp.float32))
    span = TURN
    pieces_sum = []
    row_index = lax.broadcasted_iota(jnp.int32, (8, span), 0)
    for h in range(GROUP):
        wide = jnp.concatenate([gdist[h], jnp.zeros((TILE, TILE), jnp.float32)], axis=1)
        size = TILE // 2
        while size >= 8:
            wide = wide[size:, :] + pltpu.roll(wide[:size, :], size, 1)
            size //= 2
        for bit in (4, 2, 1):
            wide = jnp.where(row_index & bit == 0, pltpu.roll(wide, bit, 1), wide)
        pieces_sum.append(column_sum(wide))
    pieces_sum.append(jnp.zeros((8 - GROUP, span), jnp.float32))
    onehot = jnp.where(bucket_onehot(), 1.0, 0.0)
    by_bucket = lax.dot_general(
        jnp.concatenate(pieces_sum, axis=0), onehot, NT, precision=lax.Precision.HIGHEST,
        preferred_element_type=jnp.float32,
    )
    width = xs.shape[1]
    parts = width // rows
    each = BUCKETS * HEADS // parts
    lane = lax.broadcasted_iota(jnp.int32, (BUCKETS, width), 1)
    entry = lane // rows * each + lane % rows
    bucket = lax.broadcasted_iota(jnp.int32, (BUCKETS, width), 0)
    chosen = (entry // HEADS == bucket) & (lane % rows < each)
    table = lax.dot_general(
        by_bucket, jnp.where(chosen, 1.0, 0.0), NN, precision=lax.Precision.HIGHEST,
        preferred_element_type=jnp.float32,
    )
    head = lax.broadcasted_iota(jnp.int32, table.shape, 0)
    lane = lax.broadcasted_iota(jnp.int32, table.shape, 1)
    entry = lane // rows * each + lane % rows
    right = (head < GROUP) & (entry % HEADS == GROUP * group + head)
    table = column_sum(jnp.where(right, table, 0.0))

    if base:
        vectors[12:13, :] += table
    else:
        vectors[12:13, :] = table

    if not done:
        for copy in stores(0):
            copy.wait()
        vectors_out[...] = vectors[0:16, :]
        for copy in sends:
            copy.wait()
        return

    vectors[2:8, :] = sums[0:6, :]
    vectors[8:12, :] = up_slots(ids, up_sums, rows, parts // 2)
    vectors[13:, :] = jnp.zeros((128 - 13, width), jnp.float32)
    tile = jnp.transpose(vectors[...]).astype(jnp.bfloat16)
    turned[0, 0] = tile
    turned[1, 0] = tile
    last = block_stores(ids, turned, gw_outs, vector_sems, slice(3, LAST_TILES))
    for copy in last:
        copy.start()
    for copy in stores(0) + last + sends:
        copy.wait()


def up_slots(ids, up_sums, rows, blocks):
    width = up_sums.shape[1] // 4
    share = 2 * rows
    slot = lax.broadcasted_iota(jnp.int32, (8, width), 0)
    lane = lax.broadcasted_iota(jnp.int32, (8, width), 1)
    total = jnp.zeros((8, width), jnp.float32)
    for index in range(4):
        own = index % 2 == 0
        place = ids[HALF] if own else 1 - ids[HALF]
        part = jnp.broadcast_to(up_sums[:, index * width : (index + 1) * width], (8, width))
        for block in range(blocks):
            chip = ids[ME] ^ block_flip(ids, own, index >= 2, block, blocks)
            for quarter in range(2):
                shift = (width - block * share - quarter * rows) % width
                values = pltpu.roll(part, shift, 1) if shift else part
                keep = (lane < rows) & (slot == 2 * place + quarter)
                total = total + pltpu.roll(jnp.where(keep, values, 0.0), chip * rows, 1)
    return total[0:4, :]


def attend_back(base, steps, ids, lengths, order, xs, mask, bias, q, k, v, mixed, gmixed, lse,
                sums, up_sums, gres, pieces, grads, rows_each):
    tokens, width = xs.shape
    length = mask.shape[1]
    blocks = sum(piece.shape[0] for piece in pieces)
    done = base + steps == GROUPS
    column = lambda g: (0, base + g)
    rows = SDS((2, length // 2, width), jnp.bfloat16)
    first = 15 + len(pieces)
    if done:
        outs, out_specs = (rows, rows), (HBM_SPEC, HBM_SPEC)
    else:
        outs = (SDS((tokens, width), jnp.float32), SDS((16, width), jnp.float32))
        out_specs = (HBM_SPEC, pl.BlockSpec((16, width), lambda g: (0, 0)))
    return pl.pallas_call(
        functools.partial(attend_back_kernel, rows_each, base, steps),
        grid=(steps,),
        out_shape=outs + store_shapes(pieces, LAST_TILES if done else FIRST_TILES),
        input_output_aliases={first + index: 2 + index for index in range(len(grads))},
        in_specs=[
            SMEM_SPEC,
            SMEM_SPEC,
            VMEM_SPEC,
            pl.BlockSpec((2, length, length), lambda g: (0, 0, 0), pipeline_mode=pl.Buffered(1)),
            pl.BlockSpec((GROUP, TILE, SPAN), lambda g: (base + g, 0, 0)),
            pl.BlockSpec((tokens, LANES), column),
            pl.BlockSpec((length, LANES), column),
            pl.BlockSpec((length, LANES), column),
            pl.BlockSpec((tokens, LANES), column),
            pl.BlockSpec((tokens, LANES), column),
            pl.BlockSpec((1, tokens, 128), lambda g: (base + g, 0, 0)),
            pl.BlockSpec(sums.shape, lambda g: (0, 0)),
            pl.BlockSpec((1, 4 * width), lambda g: (0, 0)),
        ] + [HBM_SPEC] * (2 + len(pieces) + len(grads)),
        out_specs=out_specs + (HBM_SPEC,) * len(pieces),
        scratch_shapes=[
            pltpu.VMEM((128, width), jnp.float32),
            pltpu.VMEM((2, 1, width, 128), jnp.bfloat16),
            pltpu.SemaphoreType.DMA((blocks,)),
            pltpu.VMEM((length, LANES), jnp.float32),
            pltpu.VMEM((length, LANES), jnp.float32),
            pltpu.VMEM((GROUP, TILE, SPAN), jnp.float32),
            pltpu.VMEM((tokens, width), jnp.float32),
            pltpu.VMEM((tokens, LANES), jnp.float32),
            pltpu.VMEM((tokens, GROUP * 128), jnp.float32),
            pltpu.VMEM((2, 3 * steps, width, 128), jnp.bfloat16),
            pltpu.VMEM((steps, 2, 3, width, 128), jnp.bfloat16),
            pltpu.VMEM((tokens, width), jnp.bfloat16),
            pltpu.VMEM((2, 2, length // 2, width), jnp.bfloat16),
            pltpu.SemaphoreType.DMA((blocks,)),
            pltpu.SemaphoreType.DMA((2,)),
            pltpu.SemaphoreType.DMA((steps, blocks)),
            pltpu.SemaphoreType.DMA((2,)),
        ],
        cost_estimate=cost(14 * steps),
        compiler_params=params(("arbitrary",), FULL),
        name="attend_back",
    )(ids, lengths, order, mask, bias, q, k, v, mixed, gmixed, lse, sums, up_sums,
      *in_hbm(xs, gres, *pieces, *grads))


def grad_tile(index, group):
    if index == 3:
        return 2 * GROUPS + group
    return index + (3 * group if group < GROUPS - 1 else FIRST_TILES)


def finish_kernel(ids, own, came, wq, wk, wv, wo, *vectors):
    half = ids[HALF]
    for place in range(2):
        mine = half == place
        for index, out in enumerate((wq, wk, wv, wo)):
            for group in range(GROUPS):
                tile = grad_tile(index, group)
                lane = group * LANES + place * 128
                out[:, lane : lane + 128] = jnp.where(mine, own[tile], came[tile])
    turned = jnp.transpose(own[FIRST_TILES + 3])
    rows = own.shape[1]
    for index, out in enumerate(vectors):
        if index == UP_SLOT:
            for quarter in range(4):
                out[:, quarter * rows : (quarter + 1) * rows] = turned[8 + quarter : 9 + quarter, :]
        else:
            at = 12 if index == TABLE_SLOT else index
            out[...] = turned[at : at + 1, : out.shape[1]]


def finish(ids, own, came, sizes):
    rows = own.shape[1]
    width = LANES * GROUPS
    outs = (SDS((rows, width), jnp.float32),) * 4
    outs += tuple(SDS((1, size), jnp.float32) for size in sizes)
    return pl.pallas_call(
        finish_kernel,
        out_shape=outs,
        in_specs=[SMEM_SPEC, VMEM_SPEC, VMEM_SPEC],
        out_specs=(VMEM_SPEC,) * len(outs),
        cost_estimate=cost(2),
        compiler_params=params(None, FULL),
        name="finish",
    )(ids, own, came)


BOTH = ("dp", "seq")


def xor_pairs(count, by_half):
    halves = len(by_half)
    return [
        (device * halves + half, (device ^ flip) * halves + half)
        for device in range(count)
        for half, flip in enumerate(by_half)
    ]


def swap(value):
    return lax.ppermute(value, "seq", [(0, 1), (1, 0)])


def high_part(value, high, count):
    return lax.ppermute(value, BOTH, xor_pairs(count, (4 * high, 4 * high)))


def high_parts(value, count):
    return [high_part(value, high, count) for high in range(1, count // 4)]


def low_round(value, count):
    return jnp.concatenate([value, lax.ppermute(value, BOTH, xor_pairs(count, (1, 2)))])


def last_round(value, count):
    return lax.ppermute(value, BOTH, xor_pairs(count, (2, 1)))


def offsets(count, half):
    first = jnp.where(half == 0, 1, 2)
    highs = 4 * jnp.arange(count // 4)
    near = jnp.concatenate([highs, highs ^ first])
    return jnp.concatenate([near, near ^ (3 - first)])


def after(value, *others):
    return lax.optimization_barrier((value,) + others)[0]


def wide(value):
    return value.astype(jnp.float32)


def low(value):
    return value.astype(jnp.bfloat16)


def in_order(half, own, other):
    return jnp.where(half == 0, jnp.stack([own, other]), jnp.stack([other, own]))


def shards(count, content, query_in, content_cot, query_cot, lengths, order, query_weight,
           query_bias, key_weight, value_weight, value_bias, out_weight, out_bias, mixer_gain,
           mixer_shift, up_weight, up_bias, down_weight, down_bias, final_gain, final_shift,
           position_bias):
    _, block, width = content.shape
    length = order.shape[1]
    half = lax.axis_index("seq")
    me = lax.axis_index("dp")
    rows = query_weight.shape[0]
    hidden = up_weight.shape[1]
    share = hidden // 2
    near_count = count // 2

    ids = jnp.stack([me, half]).astype(jnp.int32)
    vectors = (query_bias, value_bias, out_bias, mixer_gain, mixer_shift, down_bias, final_gain,
               final_shift, up_bias, position_bias)
    sizes = [vector.shape[0] for vector in vectors]
    theirs, square, feed_own, slots = pack(
        ids, content, query_in, content_cot, query_cot, query_weight, key_weight, value_weight,
        out_weight, jnp.transpose(up_weight), down_weight, vectors,
    )

    square_parts = high_parts(square, count)
    came = swap(theirs)
    xs, cs, mask = sort_rows(
        ids, lengths, (content, query_in, content_cot, query_cot), came, order
    )
    slots = after(slots, xs)
    slots_high = jnp.stack([slots] + high_parts(slots, count))
    feed_early = high_part(after(feed_own, came), 2, count)
    square_parts, xs = lax.optimization_barrier((square_parts, xs))
    square_near = low_round(jnp.stack([square] + square_parts), count)
    square_near, slots_high, feed_early = lax.optimization_barrier(
        (square_near, slots_high, feed_early)
    )
    slots_near = low_round(slots_high, count)
    square_far = last_round(square_near, count)
    near_swapped = swap(square_near)
    square_far = after(square_far, slots_near, near_swapped)
    slots_far = last_round(slots_near, count)
    far_swapped = swap(square_far)
    feed_later = after(feed_own, square_near)
    feed_parts = [
        feed_early if high == 2 else high_part(feed_later, high, count)
        for high in range(1, count // 4)
    ]
    feed_parts = lax.optimization_barrier((feed_parts, square_far))[0]
    feed_near = low_round(jnp.stack([feed_own] + feed_parts), count)
    vector_rows, up_biases, bias = vectors_to_all(ids, slots_near, slots_far, width, sizes)
    feed_near = after(feed_near, far_swapped, bias)
    pieces = (square_near, square_far, near_swapped, far_swapped)

    flips = offsets(count, half)
    other_flips = offsets(count, 1 - half)
    chips, other_chips = me ^ flips, me ^ other_flips
    aligned = rows % 16 == 0
    if not aligned:
        ordered = []
        for side, places in ((pieces[:2], chips), (pieces[2:], other_chips)):
            joint = jnp.take(jnp.concatenate(side), jnp.argsort(places), axis=0)
            ordered.append(
                jnp.transpose(joint, (1, 0, 2, 3)).reshape(1, 4 * GROUPS, width, 128)
            )
        pieces = tuple(ordered)

    q, k, v, mixed, lse = attend(ids, lengths, xs, mask, bias, vector_rows, pieces)
    feed_far = last_round(feed_near, count)
    feed_far = after(feed_far, mixed)

    feeds = (feed_near, swap(feed_near), feed_far, swap(feed_far))
    out, act, gup, first, gdown, gres, gbranch, gmixed, sums, up_sums = feed(
        ids, xs, mixed, cs, vector_rows, up_biases, feeds, pieces
    )
    shape = (near_count, 2, share, width)
    far_own, far_other = feed_weights(1, act, gup, first, gdown, shape)

    def by_device(grads):
        if aligned:
            return grads
        result = []
        for grad, places in zip(grads, (chips, other_chips)):
            parts = grad[0].reshape(grad.shape[1], count, rows, 128)
            parts = jnp.take(jnp.transpose(parts, (1, 0, 2, 3)), places, axis=0)
            result += [parts[:near_count], parts[near_count:]]
        return result

    def swapped_sum(own, other):
        return wide(own) + wide(swap(other))

    def halved(total):
        return total.reshape((2, total.shape[0] // 2) + total.shape[1:])

    def high_parts_of(total, count):
        return [
            lax.ppermute(low(total[high]), BOTH, xor_pairs(count, (4 * high, 4 * high)))
            for high in range(1, count // 4)
        ]

    def own_sum(total, parts):
        total = total[0]
        for part in parts:
            total = total + wide(part)
        return total

    gwo = out_weights(ids, after(mixed, far_own), gbranch, pieces)
    far_came, _ = lax.optimization_barrier((swap(far_other), gwo[0]))
    cut = near_count // 2 + max(1, near_count // 8)
    far_first = low(wide(far_own[:cut]) + wide(far_came[:cut]))
    gmixed, far_first = lax.optimization_barrier((gmixed, far_first))
    far_first = last_round(far_first, count)
    heads = functools.partial(
        attend_back, ids=ids, lengths=lengths, order=order, xs=xs, mask=mask, bias=bias, q=q, k=k,
        v=v, mixed=mixed, lse=lse, up_sums=up_sums, pieces=pieces, rows_each=rows,
    )
    gx, head_sums, *gws = heads(0, 1, gmixed=gmixed, sums=sums, gres=gres, grads=gwo)
    far_own, far_came, gx = lax.optimization_barrier((far_own, far_came, gx))
    far_second = low(wide(far_own[cut:]) + wide(far_came[cut:]))
    gdown, far_first, far_second, gx = lax.optimization_barrier(
        (gdown, far_first, far_second, gx)
    )
    far_second = last_round(far_second, count)
    near_own, near_other = feed_weights(0, act, gup, first, gdown, shape)
    far_second, near_own, near_other = lax.optimization_barrier(
        (far_second, near_own, near_other)
    )
    near_came = swap(near_other)
    outs = unsort_rows(ids, order, after(out, far_second))
    near_came, near_own, _ = lax.optimization_barrier((near_came, near_own, outs[0]))
    to_send = low(
        wide(halved(near_own)[1]) + wide(halved(near_came)[1])
        + wide(jnp.concatenate([far_first[near_count // 2 :], far_second]))
    )
    gx, to_send = lax.optimization_barrier((gx, to_send))
    gfeed_came = lax.ppermute(to_send, BOTH, xor_pairs(count, (1, 2)))
    gx, head_sums, *gws = result = heads(
        1, 1, gmixed=gmixed, sums=jnp.concatenate([sums, head_sums]), gres=gx, grads=gws
    )
    near_parts = [near_own, near_came, far_first, gfeed_came]
    near_parts, gx = lax.optimization_barrier((near_parts, gx))
    early = low(sum(wide(part[2]) for part in near_parts))
    gx, early = lax.optimization_barrier((gx, early))
    early = high_part(early, 2, count)
    most = by_device(result[2:])
    most_came = [swap(part) for part in most[2:]]
    grad_own, grad_send, *gws = heads(
        2, 1, gmixed=gmixed, sums=jnp.concatenate([sums, head_sums]), gres=gx, grads=()
    )
    early, most_came, gws, near_parts = lax.optimization_barrier(
        (early, most_came, gws, near_parts)
    )
    gfeed = sum(wide(part[: near_count // 2]) for part in near_parts)
    last = by_device(gws)
    most_far = last_round(low(wide(most[1]) + wide(most_came[1])), count)
    last_came = [swap(part) for part in last[2:]]
    last_far = last_round(low(wide(last[1]) + wide(last_came[1])), count)
    gfeed_parts = [
        early if high == 2 else high_part(low(gfeed[high]), high, count)
        for high in range(1, count // 4)
    ]
    outs = place_rows(half, *outs)
    grads = place_rows(half, grad_own, grad_send)
    most_far, last_far, last_came, gfeed_parts = lax.optimization_barrier(
        (most_far, last_far, last_came, gfeed_parts)
    )
    gw = jnp.concatenate([
        wide(most[0]) + wide(most_came[0]) + wide(most_far),
        wide(last[0]) + wide(last_came[0]) + wide(last_far),
    ], axis=1)
    gw_came = lax.ppermute(low(halved(gw)[1]), BOTH, xor_pairs(count, (1, 2)))
    gw = halved(gw)[0] + wide(gw_came)
    gw_parts = high_parts_of(gw, count)
    gfeed = own_sum(gfeed, gfeed_parts)
    gfeed = in_order(half, gfeed, swap(gfeed))
    up_grad = jnp.transpose(gfeed[:, 0].reshape(hidden, width))
    down_grad = gfeed[:, 1].reshape(hidden, width)
    gw = own_sum(gw, gw_parts)
    query_grad, key_grad, value_grad, out_grad, *ends = finish(ids, gw, swap(gw), sizes)
    ends = [end.reshape(-1) for end in ends]
    return (
        outs[0], outs[1], grads[0], grads[1],
        query_grad, ends[0], key_grad, value_grad, ends[1], out_grad, ends[2], ends[3], ends[4],
        up_grad, ends[8], down_grad, ends[5], ends[6], ends[7], ends[9],
    )


def place_rows(half, own, send):
    came = swap(send)
    return [
        jnp.where(half == 0, jnp.stack([own[i], came[i]]), jnp.stack([came[i], own[i]]))
        for i in range(2)
    ]


def solution(mesh):
    rows3 = P("dp", "seq", None)
    flat, first, last = P("dp"), P("dp", None), P(None, "dp")
    in_specs = (
        rows3, rows3, rows3, rows3, first, first, first, flat, first, first, flat, first, flat,
        flat, flat, last, flat, first, flat, flat, flat, flat,
    )
    out_specs = (
        rows3, rows3, rows3, rows3, first, flat, first, first, flat, first, flat, flat, flat,
        last, flat, first, flat, flat, flat, flat,
    )
    body = functools.partial(shards, mesh.shape["dp"])
    return jax.shard_map(
        body, mesh=mesh, in_specs=in_specs, out_specs=out_specs, check_vma=False
    )
```

```python
import functools
import math

import jax
import jax.numpy as jnp
from jax import lax
from jax.experimental import pallas as pl
from jax.experimental.pallas import tpu as pltpu
from jax.sharding import PartitionSpec as P

HEADS = 12
HEAD_DIM = 64
BUCKETS = 32
GROUP = 4
LANES = GROUP * HEAD_DIM
GROUPS = HEADS // GROUP
TILE = 128
TILES = 4
NEG = -1e30
FLOOR = -1e29
EPS = 1e-05

limits = (1, 2, 3, 4, 5, 6, 7, 8, 12, 16, 23, 32, 46, 64, 91)

NN = (((1,), (0,)), ((), ()))
NT = (((1,), (1,)), ((), ()))
TN = (((0,), (0,)), ((), ()))
VMEM_SPEC = pl.BlockSpec(memory_space=pltpu.VMEM)
ANY_SPEC = pl.BlockSpec(memory_space=pl.ANY)
HBM_SPEC = pl.BlockSpec(memory_space=pltpu.HBM)
SCALE = 1.6e6
SMEM_SPEC = pl.BlockSpec(memory_space=pltpu.SMEM)
SDS = jax.ShapeDtypeStruct


def cost(micros):
    return pl.CostEstimate(
        flops=0, bytes_accessed=int(micros * SCALE), transcendentals=0
    )


def product(left, right, dims=NN):
    return lax.dot_general(left, right, dims, preferred_element_type=jnp.float32)


def params(semantics=None, limit=56):
    return pltpu.CompilerParams(dimension_semantics=semantics, vmem_limit_bytes=limit << 20)


def row_sum(values):
    return jnp.sum(values, axis=-1, keepdims=True)


ME, HALF = 0, 1
VECTORS, UP_SLOT, TABLE_SLOT = 10, 8, 9
FIRST_TILES, LAST_TILES = 3 * GROUPS, 4
FULL = 60


def in_hbm(*values):
    return [pltpu.with_memory_space_constraint(value, pltpu.HBM) for value in values]


def run_copies(copies):
    for copy in copies:
        copy.start()
    for copy in copies:
        copy.wait()


def pack_kernel(ids, content, query, ccot, qcot, wq, wk, wv, wo, up, down, *rest):
    vectors, rest = rest[:VECTORS], rest[VECTORS:]
    (theirs, square, feed, slots, tokens, squares, feeds, in_sems, out_sems) = rest
    half = ids[HALF]
    share = feed.shape[1]
    loads = []

    def load(source, target):
        copy = pltpu.make_async_copy(source, target, in_sems.at[len(loads)])
        copy.start()
        loads.append(copy)

    for index, weight in enumerate((wq, wk, wv, wo)):
        for group in range(GROUPS):
            lane = pl.multiple_of(group * LANES + half * 128, 128)
            place = 3 * group + index if index < 3 else 3 * GROUPS + group
            load(weight.at[:, pl.ds(lane, 128)], squares.at[place])
    for index, source in enumerate((content, query, ccot, qcot)):
        load(source.at[1 - half], tokens.at[index])
    rows = pl.ds(pl.multiple_of(half * share, share), share)
    load(up.at[rows, :], feeds.at[0])
    load(down.at[rows, :], feeds.at[1])
    slots[...] = jnp.zeros_like(slots)
    for index, vector in enumerate(vectors):
        slots[index : index + 1, : vector.shape[1]] = vector[...]
    for copy in loads[: 4 * GROUPS]:
        copy.wait()
    stores = [
        pltpu.make_async_copy(squares, square, out_sems.at[0]),
        pltpu.make_async_copy(tokens, theirs, out_sems.at[1]),
        pltpu.make_async_copy(feeds, feed, out_sems.at[2]),
    ]
    stores[0].start()
    for copy in loads[4 * GROUPS :]:
        copy.wait()
    stores[1].start()
    stores[2].start()
    for copy in stores:
        copy.wait()


def pack(ids, content, query, ccot, qcot, wq, wk, wv, wo, up, down, vectors):
    _, block, width = content.shape
    rows = wq.shape[0]
    hidden = up.shape[0]
    return pl.pallas_call(
        pack_kernel,
        out_shape=(
            SDS((4, block, width), jnp.bfloat16),
            SDS((4 * GROUPS, rows, 128), jnp.bfloat16),
            SDS((2, hidden // 2, width), jnp.bfloat16),
            SDS((16, 256), jnp.bfloat16),
        ),
        in_specs=[SMEM_SPEC] + [HBM_SPEC] * 10 + [VMEM_SPEC] * VECTORS,
        out_specs=(HBM_SPEC,) * 3 + (VMEM_SPEC,),
        scratch_shapes=[
            pltpu.VMEM((4, block, width), jnp.bfloat16),
            pltpu.VMEM((4 * GROUPS, rows, 128), jnp.bfloat16),
            pltpu.VMEM((2, hidden // 2, width), jnp.bfloat16),
            pltpu.SemaphoreType.DMA((4 * GROUPS + 6,)),
            pltpu.SemaphoreType.DMA((3,)),
        ],
        cost_estimate=cost(4),
        compiler_params=params(None, FULL),
        name="pack",
    )(ids, *in_hbm(content, query, ccot, qcot, wq, wk, wv, wo, up, down),
      *(vector.reshape(1, -1) for vector in vectors))


def order_onehot(ids, order):
    length = order.shape[1]
    row = order[pl.ds(ids[HALF], 1), :]
    down = lax.broadcasted_iota(jnp.int32, (length, length), 0)
    return jnp.where(row == down, 1.0, 0.0).astype(jnp.bfloat16)


def sort_kernel(ids, lengths, content, query, ccot, qcot, came, order,
                xs_out, cs_out, mask_out, held, sems):
    length = order.shape[1]
    block = content.shape[1]
    half = ids[HALF]
    copies = []
    for index, source in enumerate((content, query, ccot, qcot)):
        for place, rows in ((half, source.at[half]), (1 - half, came.at[index])):
            here = pl.ds(pl.multiple_of(place * block, block), block)
            copies.append(
                pltpu.make_async_copy(rows, held.at[index, here], sems.at[len(copies)])
            )
    for copy in copies:
        copy.start()
    onehot = order_onehot(ids, order)
    lane = lax.broadcasted_iota(jnp.int32, (8, length), 1)
    line = lax.broadcasted_iota(jnp.int32, (8, length), 0)
    digits = jnp.where(line == 0, lane // 16, jnp.where(line == 1, lane % 16, 0))
    digits = product(digits.astype(jnp.float32).astype(jnp.bfloat16), onehot, NT)
    rank_row = digits[0:1, :] * 16.0 + digits[1:2, :]
    across = lax.broadcasted_iota(jnp.int32, (length, length), 1).astype(jnp.float32)
    rank_col = row_sum(onehot.astype(jnp.float32) * across)
    place_col = lax.broadcasted_iota(jnp.int32, (length, 1), 0)
    place_row = lax.broadcasted_iota(jnp.int32, (1, length), 1)
    segment_col = jnp.zeros((length, 1), jnp.int32)
    segment_row = jnp.zeros((1, length), jnp.int32)
    bound = jnp.int32(0)
    for index in range(lengths.shape[1] - 1):
        bound = bound + lengths[half, index]
        segment_col = segment_col + (place_col >= bound).astype(jnp.int32)
        segment_row = segment_row + (place_row >= bound).astype(jnp.int32)
    same = segment_col == segment_row
    mask_out[0] = jnp.where(same & (rank_row <= rank_col), 0.0, NEG).astype(jnp.bfloat16)
    mask_out[1] = jnp.where(same & (rank_row < rank_col), 0.0, NEG).astype(jnp.bfloat16)
    for copy in copies:
        copy.wait()
    for source, target, at in ((0, xs_out, 0), (1, xs_out, 1), (2, cs_out, 0), (3, cs_out, 1)):
        target[at * length : (at + 1) * length, :] = product(onehot, held[source]).astype(
            jnp.bfloat16
        )


def sort_rows(ids, lengths, tokens, came, order):
    length = order.shape[1]
    width = came.shape[2]
    return pl.pallas_call(
        sort_kernel,
        out_shape=(
            SDS((2 * length, width), jnp.bfloat16),
            SDS((2 * length, width), jnp.bfloat16),
            SDS((2, length, length), jnp.bfloat16),
        ),
        in_specs=[SMEM_SPEC] * 2 + [HBM_SPEC] * 5 + [VMEM_SPEC],
        out_specs=(VMEM_SPEC,) * 3,
        scratch_shapes=[
            pltpu.VMEM((4, length, width), jnp.bfloat16),
            pltpu.SemaphoreType.DMA((8,)),
        ],
        cost_estimate=cost(5),
        compiler_params=params(None, FULL),
        name="sort_rows",
    )(ids, lengths, *in_hbm(*tokens, came), order)


def put_back(ids, onehot, source, scratch, own, send, sems):
    length = onehot.shape[0]
    block = own.shape[1]
    for stream in range(2):
        rows = product(onehot, source(stream), TN).astype(jnp.bfloat16)
        scratch[0, stream] = rows[:block, :]
        scratch[1, stream] = rows[block:, :]
    return [
        pltpu.make_async_copy(scratch.at[ids[HALF]], own, sems.at[0]),
        pltpu.make_async_copy(scratch.at[1 - ids[HALF]], send, sems.at[1]),
    ]


def unsort_kernel(ids, order, values, own, send, held, scratch, sems):
    length = order.shape[1]
    copy = pltpu.make_async_copy(values, held, sems.at[2])
    copy.start()
    onehot = order_onehot(ids, order)
    copy.wait()
    run_copies(put_back(
        ids, onehot, lambda s: held[s * length : (s + 1) * length, :], scratch, own, send, sems
    ))


def unsort_rows(ids, order, values):
    length = order.shape[1]
    width = values.shape[1]
    shape = SDS((2, length // 2, width), jnp.bfloat16)
    return pl.pallas_call(
        unsort_kernel,
        out_shape=(shape, shape),
        in_specs=[SMEM_SPEC, VMEM_SPEC, HBM_SPEC],
        out_specs=(HBM_SPEC, HBM_SPEC),
        scratch_shapes=[
            pltpu.VMEM((2 * length, width), jnp.bfloat16),
            pltpu.VMEM((2, 2, length // 2, width), jnp.bfloat16),
            pltpu.SemaphoreType.DMA((3,)),
        ],
        cost_estimate=cost(3),
        compiler_params=params(None, FULL),
        name="unsort_rows",
    )(ids, order, *in_hbm(values))


SPAN = 5 * TILE
TURN = 6 * TILE


def bucket_onehot():
    distance = lax.broadcasted_iota(jnp.int32, (BUCKETS, TURN), 1) - (3 * TILE - 1)
    magnitude = jnp.abs(distance)
    counted = jnp.zeros(distance.shape, jnp.int32)
    for limit in limits:
        counted = counted + (magnitude >= limit).astype(jnp.int32)
    bucket = counted + 16 * (distance > 0).astype(jnp.int32)
    return bucket == lax.broadcasted_iota(jnp.int32, distance.shape, 0)


def block_flip(ids, own, far, block, count):
    place = ids[HALF] if own else 1 - ids[HALF]
    first = jnp.where(place == 0, 1, 2)
    high = count // 2
    flip = jnp.int32(4 * (block % high))
    if block >= high:
        flip = flip ^ first
    return flip ^ (3 - first) if far else flip


def block_places(ids, pieces):
    places = []
    for index, piece in enumerate(pieces):
        own = index < len(pieces) // 2
        place = ids[HALF] if own else 1 - ids[HALF]
        for block in range(piece.shape[0]):
            if len(pieces) == 2:
                places.append((index, block, place, 0))
            else:
                flip = block_flip(ids, own, index % 2 == 1, block, piece.shape[0])
                places.append((index, block, place, ids[ME] ^ flip))
    return places


def block_copies(ids, pieces, target, sems, tiles):
    copies = []
    for index, block, place, chip in block_places(ids, pieces):
        rows = pieces[index].shape[2]
        here = pl.ds(pl.multiple_of(chip * rows, rows), rows)
        copies.append(
            pltpu.make_async_copy(
                pieces[index].at[block, tiles], target.at[place, :, here, :],
                sems.at[len(copies)],
            )
        )
    return copies


def block_stores(ids, source, outs, sems, tiles):
    copies = []
    for index, block, place, chip in block_places(ids, outs):
        rows = outs[index].shape[2]
        here = pl.ds(pl.multiple_of(chip * rows, rows), rows)
        copies.append(
            pltpu.make_async_copy(
                source.at[place, :, here, :], outs[index].at[block, tiles],
                sems.at[len(copies)],
            )
        )
    return copies


def joined(weights, index):
    return jnp.concatenate([weights[0, index], weights[1, index]], axis=1)


def store_shapes(pieces, tiles):
    return tuple(SDS((p.shape[0], tiles) + p.shape[2:], jnp.bfloat16) for p in pieces)


def vectors_kernel(width, sizes, ids, near, far, rows_out, up_out, bias_out):
    count = 2 * near.shape[0]
    half = ids[HALF]
    high = count // 4
    total = jnp.zeros((16, width), jnp.float32)
    table = jnp.zeros((16, width), jnp.float32)
    blank = jnp.zeros((16, width - 256), jnp.float32)
    slot = lax.broadcasted_iota(jnp.int32, (16, width), 0)
    blocks = [[], []]
    for side, part in enumerate((near, far)):
        for block in range(part.shape[0]):
            chip = ids[ME] ^ block_flip(ids, True, side == 1, block, part.shape[0])
            values = jnp.concatenate([part[block].astype(jnp.float32), blank], axis=1)
            blocks[side].append(values)
            total = total + pltpu.roll(
                jnp.where(slot < UP_SLOT, values, 0.0), chip * sizes[0], 1
            )
            table = table + pltpu.roll(
                jnp.where(slot == TABLE_SLOT, values, 0.0), chip * sizes[TABLE_SLOT], 1
            )
    rows_out[...] = total[2:10, :]
    rows_out[6:8, :] = total[0:2, :]
    share = sizes[UP_SLOT] // 2
    lane = lax.broadcasted_iota(jnp.int32, (16, width), 1)
    keep = (slot == UP_SLOT) & (lane < share)
    near_blocks, far_blocks = blocks
    order = (
        (half, near_blocks[:high] + near_blocks[high:]),
        (1 - half, near_blocks[:high] + far_blocks[:high]),
        (half, far_blocks[:high] + far_blocks[high:]),
        (1 - half, near_blocks[high:] + far_blocks[high:]),
    )
    for index, (place, parts) in enumerate(order):
        joint = jnp.zeros((16, width), jnp.float32)
        for block, values in enumerate(parts):
            values = pltpu.roll(values, lax.rem(width - place * share, width), 1)
            joint = joint + pltpu.roll(jnp.where(keep, values, 0.0), block * share, 1)
        up_out[:, index * width : (index + 1) * width] = joint[UP_SLOT : UP_SLOT + 1, :]
    flat = table[TABLE_SLOT : TABLE_SLOT + 1, : BUCKETS * HEADS]
    entry = lax.broadcasted_iota(jnp.int32, (16, BUCKETS * HEADS), 1)
    head = lax.broadcasted_iota(jnp.int32, (16, BUCKETS * HEADS), 0)
    spread_heads = jnp.where(entry % HEADS == head, flat, 0.0).astype(jnp.bfloat16)
    place = lax.broadcasted_iota(jnp.int32, (BUCKETS, BUCKETS * HEADS), 1) // HEADS
    bucket = lax.broadcasted_iota(jnp.int32, (BUCKETS, BUCKETS * HEADS), 0)
    folded = product(spread_heads, jnp.where(place == bucket, 1.0, 0.0).astype(jnp.bfloat16), NT)
    onehot = jnp.where(bucket_onehot(), 1.0, 0.0).astype(jnp.bfloat16)
    rows = product(folded.astype(jnp.bfloat16), onehot)
    for head in range(HEADS):
        spread = jnp.broadcast_to(rows[head : head + 1, :], (TILE, TURN))
        turned = pltpu.roll(spread, TURN - (TILE - 1), 1, stride=1, stride_axis=0)
        bias_out[head] = turned[:, :SPAN].astype(jnp.bfloat16)


def vectors_to_all(ids, near, far, width, sizes):
    return pl.pallas_call(
        functools.partial(vectors_kernel, width, sizes),
        out_shape=(
            SDS((8, width), jnp.float32),
            SDS((1, 4 * width), jnp.float32),
            SDS((HEADS, TILE, SPAN), jnp.bfloat16),
        ),
        in_specs=[SMEM_SPEC] + [VMEM_SPEC] * 2,
        out_specs=(VMEM_SPEC,) * 3,
        cost_estimate=cost(6),
        compiler_params=params(None, FULL),
        name="vectors",
    )(ids, near, far)


def head_lanes(head, shape):
    lane = lax.broadcasted_iota(jnp.int32, shape, 1)
    return (lane >= head * HEAD_DIM) & (lane < (head + 1) * HEAD_DIM)


def head_stack(values):
    low = jnp.zeros((), values.dtype)
    return jnp.concatenate(
        [jnp.where(head_lanes(h, values.shape), values, low) for h in range(GROUP)]
    )


def head_merge(stack, rows):
    total = stack[(GROUP - 1) * rows :, :]
    for h in range(GROUP - 1):
        part = stack[h * rows : (h + 1) * rows, :]
        total = jnp.where(head_lanes(h, part.shape), part, total)
    return total


def widen(values, lanes):
    return jnp.concatenate([values] * (lanes // 128), axis=1)


def by_width(ids, lengths, tile, body):
    half = ids[HALF]
    begin, end = tile * TILE, (tile + 1) * TILE
    bound = jnp.int32(0)
    low, high = jnp.int32(0), jnp.int32(TILES * TILE)
    for index in range(lengths.shape[1] - 1):
        bound = bound + lengths[half, index]
        low = jnp.where(bound <= begin, bound, low)
        high = jnp.where(bound >= end, jnp.minimum(bound, high), high)
    first = low // TILE
    width = jnp.maximum((high + TILE - 1) // TILE - first, 2)
    first = pl.multiple_of(jnp.minimum(first, TILES - width) * TILE, TILE)
    for count in range(2, TILES + 1):
        pl.when(width == count)(functools.partial(body, first, count * TILE))


def attend_kernel(ids, lengths, xs, mask, bias, rows, *rest):
    pieces, rest = rest[:-8], rest[-8:]
    q_out, k_out, v_out, mixed_out, lse_out, weights, values, sems = rest
    length = mask.shape[1]
    group = pl.program_id(0)

    def weight_copies(index):
        tiles = pl.ds(3 * index, 3)
        return block_copies(ids, pieces, weights.at[:, tiles], sems.at[index], tiles)

    @pl.when(group == 0)
    def _():
        for index in range(GROUPS):
            for copy in weight_copies(index):
                copy.start()

    for index in range(GROUPS):
        @pl.when(group == index)
        def _():
            for copy in weight_copies(index):
                copy.wait()

    q = product(xs[...], joined(weights, 3 * group)) + rows[6:7, :]
    q_out[...] = q.astype(jnp.bfloat16)
    k = product(xs[0:length, :], joined(weights, 3 * group + 1))
    k_out[...] = k.astype(jnp.bfloat16)
    v = product(xs[0:length, :], joined(weights, 3 * group + 2)) + rows[7:8, :]
    v_out[...] = v.astype(jnp.bfloat16)

    wide_lanes = lax.broadcasted_iota(jnp.int32, v.shape, 1) < 128
    one = jnp.ones((), jnp.bfloat16)
    values[0] = jnp.where(wide_lanes, v_out[...], one)
    values[1] = jnp.where(wide_lanes, one, v_out[...])

    def tile_step(tile, carry):
        def body(first, keys):
            there = pl.ds(first, keys)
            near = pl.ds(pl.multiple_of((2 - tile) * TILE + first, TILE), keys)
            here = pl.ds(pl.multiple_of(tile * TILE, TILE), TILE)
            key = k_out[there, :]
            for stream in range(2):
                at = pl.ds(pl.multiple_of(stream * length + tile * TILE, TILE), TILE)
                scores = product(head_stack(q_out[at, :] * jnp.bfloat16(0.125)), key, NT)
                masked = mask[stream, here, there].astype(jnp.float32)
                weights, peaks, logs = [], [], []
                for h in range(GROUP):
                    part = scores[h * TILE : (h + 1) * TILE, :] + bias[h, :, near].astype(jnp.float32) + masked
                    peak = jnp.maximum(jnp.max(part, axis=-1, keepdims=True), FLOOR)
                    weights.append(jnp.exp(part - peak).astype(jnp.bfloat16))
                    peaks.append(peak)
                for pair in range(2):
                    both = jnp.concatenate(weights[2 * pair : 2 * pair + 2])
                    both = product(both, values[pair, there, :])
                    top = slice(pair * 128, pair * 128 + 128)
                    low = slice(128 - pair * 128, 256 - pair * 128)
                    parts = []
                    for h in range(2):
                        rows = slice(h * TILE, (h + 1) * TILE)
                        summed = both[rows, low]
                        alive = summed > 0
                        inverse = jnp.where(alive, 1.0 / summed, 0.0)
                        parts.append(both[rows, top] * inverse)
                        logs.append(
                            jnp.where(alive, peaks[2 * pair + h] + jnp.log(summed), 0.0)
                        )
                    lane = lax.broadcasted_iota(jnp.int32, parts[0].shape, 1)
                    mixed = jnp.where(lane < HEAD_DIM, parts[0], parts[1])
                    mixed_out[at, top] = mixed.astype(jnp.bfloat16)
                packed = logs[0]
                for h in range(1, GROUP):
                    packed = jnp.where(lane == h, logs[h], packed)
                lse_out[0, at, :] = packed

        by_width(ids, lengths, tile, body)
        return carry

    lax.fori_loop(0, length // TILE, tile_step, 0)


def attend(ids, lengths, xs, mask, bias, rows, pieces):
    tokens, width = xs.shape
    length = mask.shape[1]
    blocks = sum(piece.shape[0] for piece in pieces)
    full = lambda g: (0, 0)
    column = lambda g: (0, g)
    once = pl.Buffered(1)
    return pl.pallas_call(
        attend_kernel,
        grid=(GROUPS,),
        out_shape=(
            SDS((tokens, width), jnp.bfloat16),
            SDS((length, width), jnp.bfloat16),
            SDS((length, width), jnp.bfloat16),
            SDS((tokens, width), jnp.bfloat16),
            SDS((GROUPS, tokens, 128), jnp.float32),
        ),
        in_specs=[
            SMEM_SPEC,
            SMEM_SPEC,
            pl.BlockSpec((tokens, width), full, pipeline_mode=once),
            pl.BlockSpec((2, length, length), lambda g: (0, 0, 0), pipeline_mode=once),
            pl.BlockSpec((GROUP, TILE, SPAN), lambda g: (g, 0, 0)),
            pl.BlockSpec((8, LANES), column),
        ] + [HBM_SPEC] * len(pieces),
        out_specs=(
            pl.BlockSpec((tokens, LANES), column),
            pl.BlockSpec((length, LANES), column),
            pl.BlockSpec((length, LANES), column),
            pl.BlockSpec((tokens, LANES), column),
            pl.BlockSpec((1, tokens, 128), lambda g: (g, 0, 0)),
        ),
        scratch_shapes=[
            pltpu.VMEM((2, 3 * GROUPS, width, 128), jnp.bfloat16),
            pltpu.VMEM((2, length, LANES), jnp.bfloat16),
            pltpu.SemaphoreType.DMA((GROUPS, blocks)),
        ],
        cost_estimate=cost(18),
        compiler_params=params(("arbitrary",), FULL),
        name="attend",
    )(ids, lengths, xs, mask, bias, rows, *in_hbm(*pieces))


def norm_parts(values):
    mean = jnp.mean(values, axis=-1, keepdims=True)
    center = values - mean
    spread = jnp.mean(center * center, axis=-1, keepdims=True)
    scale = lax.rsqrt(spread + EPS)
    return center * scale, scale


def norm_back(normal, scale, grad):
    mean = jnp.mean(grad, axis=-1, keepdims=True)
    inner = jnp.mean(grad * normal, axis=-1, keepdims=True)
    return scale * (grad - mean - normal * inner)


def column_sum(values):
    return jnp.sum(values, axis=0, keepdims=True)


BLOCK = 256


def feed_kernel(ids, xs, mixed, cot, rows, up_bias, near_own, near_other, far_own, far_other,
                *rest):
    pieces, rest = rest[:-14], rest[-14:]
    (out, act_out, gup_out, first_out, gdown_out, gres_out, gbranch_out, gmixed_out,
     sums, up_sums, up_all, down_all, wo_all, sems) = rest
    step = pl.program_id(0)
    units = up_all.shape[0] // 4
    parts = (near_own, near_other, far_own, far_other)
    held = sum(piece.shape[0] for piece in pieces)

    def weight_copies():
        copies = []
        share = near_own.shape[2]
        for index, part in enumerate(parts):
            for block in range(part.shape[0]):
                here = slice(index * units + block * share, index * units + (block + 1) * share)
                for which, target in ((0, up_all), (1, down_all)):
                    copies.append(
                        pltpu.make_async_copy(
                            part.at[block, which], target.at[here, :],
                            sems.at[held + len(copies)],
                        )
                    )
        return copies

    @pl.when(step == 0)
    def _():
        sums[...] = jnp.zeros_like(sums)
        up_sums[...] = jnp.zeros_like(up_sums)
        copies = block_copies(ids, pieces, wo_all, sems, slice(3 * GROUPS, 4 * GROUPS))
        copies += weight_copies()
        run_copies(copies)

    wo = jnp.concatenate([joined(wo_all, index) for index in range(GROUPS)], axis=1)
    branch = product(mixed[...], wo) + rows[0:1, :]

    normal1, scale1 = norm_parts(xs[...].astype(jnp.float32) + branch)
    first = normal1 * rows[1:2, :] + rows[2:3, :]
    first_low = first.astype(jnp.bfloat16)
    first_out[...] = first_low
    slopes = []
    second = first + rows[3:4, :]
    for index in range(2):
        here = slice(2 * index * units, 2 * (index + 1) * units)
        up = product(first_low, up_all[here, :], NT) + up_bias[:, here]
        gate = 0.5 + 0.5 * lax.erf(up * math.sqrt(0.5))
        act = (up * gate).astype(jnp.bfloat16)
        act_out[:, here] = act
        slopes.append(gate + up * jnp.exp(-0.5 * up * up) * (1.0 / math.sqrt(2.0 * math.pi)))
        second = second + product(act, down_all[here, :])
    normal2, scale2 = norm_parts(second)
    gain = rows[4:5, :]
    out[...] = (normal2 * gain + rows[5:6, :]).astype(jnp.bfloat16)
    cots = cot[...].astype(jnp.float32)
    gsecond = norm_back(normal2, scale2, cots * gain)
    gdown = gsecond.astype(jnp.bfloat16)
    gdown_out[...] = gdown
    gfirst = gsecond
    for index in range(2):
        here = slice(2 * index * units, 2 * (index + 1) * units)
        gup = (product(gdown, down_all[here, :], NT) * slopes[index]).astype(jnp.bfloat16)
        gup_out[:, here] = gup
        up_sums[:, here] += column_sum(gup.astype(jnp.float32))
        gfirst = gfirst + product(gup, up_all[here, :])
    gres = norm_back(normal1, scale1, gfirst * rows[1:2, :])
    gres_out[...] = gres
    gbranch = gres.astype(jnp.bfloat16)
    gbranch_out[...] = gbranch
    gmixed_out[...] = product(gbranch, wo, NT).astype(jnp.bfloat16)
    sums[0:1, :] += column_sum(gbranch.astype(jnp.float32))
    sums[1:2, :] += column_sum(gfirst * normal1)
    sums[2:3, :] += column_sum(gfirst)
    sums[3:4, :] += column_sum(gdown.astype(jnp.float32))
    sums[4:5, :] += column_sum(cots * normal2)
    sums[5:6, :] += column_sum(cots)


def feed(ids, xs, mixed, cot, rows, up_bias, feeds, pieces):
    tokens, width = xs.shape
    hidden = up_bias.shape[1]
    token = pl.BlockSpec((BLOCK, width), lambda i: (i, 0))
    wide = pl.BlockSpec((BLOCK, hidden), lambda i: (i, 0))
    held = sum(piece.shape[0] for piece in pieces) + 2 * sum(part.shape[0] for part in feeds)
    low = SDS((tokens, width), jnp.bfloat16)
    return pl.pallas_call(
        feed_kernel,
        grid=(tokens // BLOCK,),
        out_shape=(
            low,
            SDS((tokens, hidden), jnp.bfloat16),
            SDS((tokens, hidden), jnp.bfloat16),
            low,
            low,
            SDS((tokens, width), jnp.float32),
            low,
            low,
            SDS((8, width), jnp.float32),
            SDS((1, hidden), jnp.float32),
        ),
        in_specs=[
            SMEM_SPEC, token, token, token,
            pl.BlockSpec((8, width), lambda i: (0, 0)),
            pl.BlockSpec((1, hidden), lambda i: (0, 0)),
        ] + [ANY_SPEC] * 4 + [HBM_SPEC] * len(pieces),
        out_specs=(token, wide, wide, token, token, token, token, token,
                   pl.BlockSpec((8, width), lambda i: (0, 0)),
                   pl.BlockSpec((1, hidden), lambda i: (0, 0))),
        scratch_shapes=[
            pltpu.VMEM((hidden, width), jnp.bfloat16),
            pltpu.VMEM((hidden, width), jnp.bfloat16),
            pltpu.VMEM((2, GROUPS, width, 128), jnp.bfloat16),
            pltpu.SemaphoreType.DMA((held,)),
        ],
        cost_estimate=cost(36),
        compiler_params=params(("arbitrary",), FULL),
        name="feed",
    )(ids, xs, mixed, cot, rows, up_bias, *feeds, *in_hbm(*pieces))


def feed_weights_kernel(part, act, gup, first, gdown, own, other, left, right, grads, in_sems,
                        out_sems):
    tokens, units = left.shape[1:]
    share = own.shape[2]
    loads, uses = [], []

    def load(source, target):
        copy = pltpu.make_async_copy(source, target, in_sems.at[len(loads)])
        copy.start()
        loads.append(copy)

    for side in range(2):
        lanes = slice((2 * part + 1 - side) * units, (2 * part + 2 - side) * units)
        for which, (source, other_side) in enumerate(((gup, first), (act, gdown))):
            load(source.at[:, lanes], left.at[2 * side + which])
            if side == 0:
                load(other_side, right.at[which])
            uses.append(len(loads))
    stores = []
    done = 0
    for index in range(4):
        for copy in loads[done : uses[index]]:
            copy.wait()
        done = uses[index]
        which = index % 2
        grad = product(left[index], right[which], TN).astype(jnp.bfloat16)
        for block in range(own.shape[0]):
            grads[index, block] = grad[block * share : (block + 1) * share, :]
        out = other if index < 2 else own
        stores.append(
            pltpu.make_async_copy(grads.at[index], out.at[:, which], out_sems.at[index])
        )
        stores[-1].start()
    for copy in stores:
        copy.wait()


def feed_weights(part, act, gup, first, gdown, shape):
    tokens, width = first.shape
    units = shape[0] * shape[2]
    return pl.pallas_call(
        functools.partial(feed_weights_kernel, part),
        out_shape=(SDS(shape, jnp.bfloat16),) * 2,
        in_specs=[HBM_SPEC] * 4,
        out_specs=(HBM_SPEC,) * 2,
        scratch_shapes=[
            pltpu.VMEM((4, tokens, units), jnp.bfloat16),
            pltpu.VMEM((2, tokens, width), jnp.bfloat16),
            pltpu.VMEM((4, shape[0], shape[2], width), jnp.bfloat16),
            pltpu.SemaphoreType.DMA((6,)),
            pltpu.SemaphoreType.DMA((4,)),
        ],
        cost_estimate=cost(9),
        compiler_params=params(None, FULL),
        name="feed_weights",
    )(*in_hbm(act, gup, first, gdown))


def out_weights_kernel(ids, mixed, gbranch, *rest):
    outs, (buffer, sems) = rest[:-2], rest[-2:]
    grad = product(mixed[...], gbranch[...], TN).astype(jnp.bfloat16)
    for index in range(GROUPS):
        for half in range(2):
            lane = index * LANES + half * 128
            buffer[half, index] = grad[:, lane : lane + 128]
    run_copies(block_stores(ids, buffer, outs, sems, slice(2 * GROUPS, 3 * GROUPS)))


def out_weights(ids, mixed, gbranch, pieces):
    tokens, width = mixed.shape
    blocks = sum(piece.shape[0] for piece in pieces)
    full = pl.BlockSpec((tokens, width), lambda i: (0, 0))
    return pl.pallas_call(
        out_weights_kernel,
        grid=(1,),
        out_shape=store_shapes(pieces, FIRST_TILES),
        in_specs=[SMEM_SPEC, full, full],
        out_specs=(HBM_SPEC,) * len(pieces),
        scratch_shapes=[
            pltpu.VMEM((2, GROUPS, width, 128), jnp.bfloat16),
            pltpu.SemaphoreType.DMA((blocks,)),
        ],
        cost_estimate=cost(4),
        compiler_params=params(("arbitrary",), FULL),
        name="out_weights",
    )(ids, mixed, gbranch)


def attend_back_kernel(ids_rows, base, steps, ids, lengths, order, mask, bias, q, k, v, mixed, gmixed, lse, sums,
                       up_sums, xs_far, gres, *rest):
    scratch = rest[-17:]
    done = base + steps == GROUPS
    count = (len(rest) - 17 - 2) // (2 if done else 3)
    pieces = rest[:count]
    if done:
        own, send, *gw_outs = rest[count:-17]
    else:
        gx_out, vectors_out, *gw_outs = rest[2 * count : -17]
    (vectors, turned, vector_sems, gk, gv, gdist, gx, gq, inner, weights, buffer, xs, rows_out, sems, in_sems, out_sems,
     row_sems) = scratch
    step = pl.program_id(0)
    group = base + step
    tiles = slice(3 * base, 3 * (base + steps))
    length = mask.shape[1]
    rows = xs.shape[1] // (2 * gw_outs[0].shape[0]) if count > 2 else ids_rows
    loads = block_copies(ids, pieces, weights, sems, tiles) + [
        pltpu.make_async_copy(xs_far, xs, in_sems.at[0]),
        pltpu.make_async_copy(gres, gx, in_sems.at[1]),
    ]

    def stores(index):
        return block_stores(
            ids, buffer.at[index], gw_outs, out_sems.at[index],
            slice(0, 3) if done else pl.ds(3 * (base + index), 3),
        )

    @pl.when(step == 0)
    def _():
        for copy in loads:
            copy.start()
        if base:
            vectors[0:16, :] = sums[8:24, :]

    gdist[...] = jnp.zeros_like(gdist)
    gk[...] = jnp.zeros_like(gk)
    gv[...] = jnp.zeros_like(gv)

    lane = lax.broadcasted_iota(jnp.int32, (LANES, GROUP * 128), 0) // HEAD_DIM
    head = lax.broadcasted_iota(jnp.int32, (LANES, GROUP * 128), 1) // 128
    adder = jnp.where(lane == head, 1.0, 0.0).astype(jnp.bfloat16)
    crossed = mixed[...].astype(jnp.float32) * gmixed[...].astype(jnp.float32)
    inner[...] = product(crossed.astype(jnp.bfloat16), adder)

    def tile_step(tile, carry):
        def body(first, keys):
            there = pl.ds(first, keys)
            near = pl.ds(pl.multiple_of((2 - tile) * TILE + first, TILE), keys)
            here = pl.ds(pl.multiple_of(tile * TILE, TILE), TILE)
            key = k[there, :]
            value = v[there, :]
            at = [
                pl.ds(pl.multiple_of(stream * length + tile * TILE, TILE), TILE)
                for stream in range(2)
            ]
            query = jnp.concatenate([head_stack(q[at[s], :] * jnp.bfloat16(0.125)) for s in range(2)])
            gmix = jnp.concatenate([head_stack(gmixed[at[s], :]) for s in range(2)])
            scores = product(query, key, NT)
            gprobs = product(gmix, value, NT)
            masked = [mask[s, here, there].astype(jnp.float32) for s in range(2)]
            probs_low = [None] * (2 * GROUP)
            gscores_low = [None] * (2 * GROUP)
            for h in range(GROUP):
                both = None
                near_bias = bias[h, :, near].astype(jnp.float32)
                for stream in range(2):
                    index = stream * GROUP + h
                    part = slice(index * TILE, (index + 1) * TILE)
                    score = scores[part, :] + near_bias + masked[stream]
                    probs = jnp.exp(score - lse[0, at[stream], h : h + 1])
                    lanes = slice(h * 128, (h + 1) * 128)
                    gscores = probs * (gprobs[part, :] - widen(inner[at[stream], lanes], keys))
                    probs_low[index] = probs.astype(jnp.bfloat16)
                    gscores_low[index] = gscores.astype(jnp.bfloat16)
                    both = gscores if both is None else both + gscores
                gdist[h, :, near] += both
            probs_low = jnp.concatenate(probs_low)
            gscores_low = jnp.concatenate(gscores_low)
            gv[there, :] += product(probs_low, gmix, TN)
            gk[there, :] += product(gscores_low, query, TN)
            back = product(gscores_low, key)
            for stream in range(2):
                part = slice(stream * GROUP * TILE, (stream + 1) * GROUP * TILE)
                gq[at[stream], :] = head_merge(back[part, :], TILE)

        by_width(ids, lengths, tile, body)
        return carry

    lax.fori_loop(0, length // TILE, tile_step, 0)
    gq_low = (gq[...] * 0.125).astype(jnp.bfloat16)
    gk_low = gk[...].astype(jnp.bfloat16)
    gv_low = gv[...].astype(jnp.bfloat16)

    @pl.when(step == 0)
    def _():
        for copy in loads:
            copy.wait()

    for index, grad in enumerate((
        product(xs[...], gq_low, TN),
        product(xs[0:length, :], gk_low, TN),
        product(xs[0:length, :], gv_low, TN),
    )):
        grad = grad.astype(jnp.bfloat16)
        buffer[step, 0, index] = grad[:, :128]
        buffer[step, 1, index] = grad[:, 128:]
    for index in range(steps):
        @pl.when(step == index)
        def _():
            for copy in stores(index):
                copy.start()

    gx[...] += product(gq_low, joined(weights, 3 * step), NT)
    gx[0:length, :] += product(gk_low, joined(weights, 3 * step + 1), NT) + product(
        gv_low, joined(weights, 3 * step + 2), NT
    )
    if done:
        sends = put_back(
            ids, order_onehot(ids, order),
            lambda s: gx[s * length : (s + 1) * length, :].astype(jnp.bfloat16),
            rows_out, own, send, row_sems,
        )
    else:
        sends = [pltpu.make_async_copy(gx, gx_out, in_sems.at[0])]
    for copy in sends:
        copy.start()
    lanes = pl.ds(pl.multiple_of(group * LANES, LANES), LANES)
    vectors[0:1, lanes] = column_sum(gq_low.astype(jnp.float32))
    vectors[1:2, lanes] = column_sum(gv_low.astype(jnp.float32))
    span = TURN
    pieces_sum = []
    row_index = lax.broadcasted_iota(jnp.int32, (8, span), 0)
    for h in range(GROUP):
        wide = jnp.concatenate([gdist[h], jnp.zeros((TILE, TILE), jnp.float32)], axis=1)
        size = TILE // 2
        while size >= 8:
            wide = wide[size:, :] + pltpu.roll(wide[:size, :], size, 1)
            size //= 2
        for bit in (4, 2, 1):
            wide = jnp.where(row_index & bit == 0, pltpu.roll(wide, bit, 1), wide)
        pieces_sum.append(column_sum(wide))
    pieces_sum.append(jnp.zeros((8 - GROUP, span), jnp.float32))
    onehot = jnp.where(bucket_onehot(), 1.0, 0.0)
    by_bucket = lax.dot_general(
        jnp.concatenate(pieces_sum, axis=0), onehot, NT, precision=lax.Precision.HIGHEST,
        preferred_element_type=jnp.float32,
    )
    width = xs.shape[1]
    parts = width // rows
    each = BUCKETS * HEADS // parts
    lane = lax.broadcasted_iota(jnp.int32, (BUCKETS, width), 1)
    entry = lane // rows * each + lane % rows
    bucket = lax.broadcasted_iota(jnp.int32, (BUCKETS, width), 0)
    chosen = (entry // HEADS == bucket) & (lane % rows < each)
    table = lax.dot_general(
        by_bucket, jnp.where(chosen, 1.0, 0.0), NN, precision=lax.Precision.HIGHEST,
        preferred_element_type=jnp.float32,
    )
    head = lax.broadcasted_iota(jnp.int32, table.shape, 0)
    lane = lax.broadcasted_iota(jnp.int32, table.shape, 1)
    entry = lane // rows * each + lane % rows
    right = (head < GROUP) & (entry % HEADS == GROUP * group + head)
    table = column_sum(jnp.where(right, table, 0.0))

    if base:
        vectors[12:13, :] += table
    else:
        vectors[12:13, :] = table

    if not done:
        for copy in stores(0):
            copy.wait()
        vectors_out[...] = vectors[0:16, :]
        for copy in sends:
            copy.wait()
        return

    vectors[2:8, :] = sums[0:6, :]
    vectors[8:12, :] = up_slots(ids, up_sums, rows, parts // 2)
    vectors[13:, :] = jnp.zeros((128 - 13, width), jnp.float32)
    tile = jnp.transpose(vectors[...]).astype(jnp.bfloat16)
    turned[0, 0] = tile
    turned[1, 0] = tile
    last = block_stores(ids, turned, gw_outs, vector_sems, slice(3, LAST_TILES))
    for copy in last:
        copy.start()
    for copy in stores(0) + last + sends:
        copy.wait()


def up_slots(ids, up_sums, rows, blocks):
    width = up_sums.shape[1] // 4
    share = 2 * rows
    slot = lax.broadcasted_iota(jnp.int32, (8, width), 0)
    lane = lax.broadcasted_iota(jnp.int32, (8, width), 1)
    total = jnp.zeros((8, width), jnp.float32)
    for index in range(4):
        own = index % 2 == 0
        place = ids[HALF] if own else 1 - ids[HALF]
        part = jnp.broadcast_to(up_sums[:, index * width : (index + 1) * width], (8, width))
        for block in range(blocks):
            chip = ids[ME] ^ block_flip(ids, own, index >= 2, block, blocks)
            for quarter in range(2):
                shift = (width - block * share - quarter * rows) % width
                values = pltpu.roll(part, shift, 1) if shift else part
                keep = (lane < rows) & (slot == 2 * place + quarter)
                total = total + pltpu.roll(jnp.where(keep, values, 0.0), chip * rows, 1)
    return total[0:4, :]


def attend_back(base, steps, ids, lengths, order, xs, mask, bias, q, k, v, mixed, gmixed, lse,
                sums, up_sums, gres, pieces, grads, rows_each):
    tokens, width = xs.shape
    length = mask.shape[1]
    blocks = sum(piece.shape[0] for piece in pieces)
    done = base + steps == GROUPS
    column = lambda g: (0, base + g)
    rows = SDS((2, length // 2, width), jnp.bfloat16)
    first = 15 + len(pieces)
    if done:
        outs, out_specs = (rows, rows), (HBM_SPEC, HBM_SPEC)
    else:
        outs = (SDS((tokens, width), jnp.float32), SDS((16, width), jnp.float32))
        out_specs = (HBM_SPEC, pl.BlockSpec((16, width), lambda g: (0, 0)))
    return pl.pallas_call(
        functools.partial(attend_back_kernel, rows_each, base, steps),
        grid=(steps,),
        out_shape=outs + store_shapes(pieces, LAST_TILES if done else FIRST_TILES),
        input_output_aliases={first + index: 2 + index for index in range(len(grads))},
        in_specs=[
            SMEM_SPEC,
            SMEM_SPEC,
            VMEM_SPEC,
            pl.BlockSpec((2, length, length), lambda g: (0, 0, 0), pipeline_mode=pl.Buffered(1)),
            pl.BlockSpec((GROUP, TILE, SPAN), lambda g: (base + g, 0, 0)),
            pl.BlockSpec((tokens, LANES), column),
            pl.BlockSpec((length, LANES), column),
            pl.BlockSpec((length, LANES), column),
            pl.BlockSpec((tokens, LANES), column),
            pl.BlockSpec((tokens, LANES), column),
            pl.BlockSpec((1, tokens, 128), lambda g: (base + g, 0, 0)),
            pl.BlockSpec(sums.shape, lambda g: (0, 0)),
            pl.BlockSpec((1, 4 * width), lambda g: (0, 0)),
        ] + [HBM_SPEC] * (2 + len(pieces) + len(grads)),
        out_specs=out_specs + (HBM_SPEC,) * len(pieces),
        scratch_shapes=[
            pltpu.VMEM((128, width), jnp.float32),
            pltpu.VMEM((2, 1, width, 128), jnp.bfloat16),
            pltpu.SemaphoreType.DMA((blocks,)),
            pltpu.VMEM((length, LANES), jnp.float32),
            pltpu.VMEM((length, LANES), jnp.float32),
            pltpu.VMEM((GROUP, TILE, SPAN), jnp.float32),
            pltpu.VMEM((tokens, width), jnp.float32),
            pltpu.VMEM((tokens, LANES), jnp.float32),
            pltpu.VMEM((tokens, GROUP * 128), jnp.float32),
            pltpu.VMEM((2, 3 * steps, width, 128), jnp.bfloat16),
            pltpu.VMEM((steps, 2, 3, width, 128), jnp.bfloat16),
            pltpu.VMEM((tokens, width), jnp.bfloat16),
            pltpu.VMEM((2, 2, length // 2, width), jnp.bfloat16),
            pltpu.SemaphoreType.DMA((blocks,)),
            pltpu.SemaphoreType.DMA((2,)),
            pltpu.SemaphoreType.DMA((steps, blocks)),
            pltpu.SemaphoreType.DMA((2,)),
        ],
        cost_estimate=cost(14 * steps),
        compiler_params=params(("arbitrary",), FULL),
        name="attend_back",
    )(ids, lengths, order, mask, bias, q, k, v, mixed, gmixed, lse, sums, up_sums,
      *in_hbm(xs, gres, *pieces, *grads))


def grad_tile(index, group):
    if index == 3:
        return 2 * GROUPS + group
    return index + (3 * group if group < GROUPS - 1 else FIRST_TILES)


def finish_kernel(ids, own, came, wq, wk, wv, wo, *vectors):
    half = ids[HALF]
    for place in range(2):
        mine = half == place
        for index, out in enumerate((wq, wk, wv, wo)):
            for group in range(GROUPS):
                tile = grad_tile(index, group)
                lane = group * LANES + place * 128
                out[:, lane : lane + 128] = jnp.where(mine, own[tile], came[tile])
    turned = jnp.transpose(own[FIRST_TILES + 3])
    rows = own.shape[1]
    for index, out in enumerate(vectors):
        if index == UP_SLOT:
            for quarter in range(4):
                out[:, quarter * rows : (quarter + 1) * rows] = turned[8 + quarter : 9 + quarter, :]
        else:
            at = 12 if index == TABLE_SLOT else index
            out[...] = turned[at : at + 1, : out.shape[1]]


def finish(ids, own, came, sizes):
    rows = own.shape[1]
    width = LANES * GROUPS
    outs = (SDS((rows, width), jnp.float32),) * 4
    outs += tuple(SDS((1, size), jnp.float32) for size in sizes)
    return pl.pallas_call(
        finish_kernel,
        out_shape=outs,
        in_specs=[SMEM_SPEC, VMEM_SPEC, VMEM_SPEC],
        out_specs=(VMEM_SPEC,) * len(outs),
        cost_estimate=cost(2),
        compiler_params=params(None, FULL),
        name="finish",
    )(ids, own, came)


BOTH = ("dp", "seq")


def xor_pairs(count, by_half):
    halves = len(by_half)
    return [
        (device * halves + half, (device ^ flip) * halves + half)
        for device in range(count)
        for half, flip in enumerate(by_half)
    ]


def swap(value):
    return lax.ppermute(value, "seq", [(0, 1), (1, 0)])


def high_part(value, high, count):
    return lax.ppermute(value, BOTH, xor_pairs(count, (4 * high, 4 * high)))


def high_parts(value, count):
    return [high_part(value, high, count) for high in range(1, count // 4)]


def low_round(value, count):
    return jnp.concatenate([value, lax.ppermute(value, BOTH, xor_pairs(count, (1, 2)))])


def last_round(value, count):
    return lax.ppermute(value, BOTH, xor_pairs(count, (2, 1)))


def offsets(count, half):
    first = jnp.where(half == 0, 1, 2)
    highs = 4 * jnp.arange(count // 4)
    near = jnp.concatenate([highs, highs ^ first])
    return jnp.concatenate([near, near ^ (3 - first)])


def after(value, *others):
    return lax.optimization_barrier((value,) + others)[0]


def wide(value):
    return value.astype(jnp.float32)


def low(value):
    return value.astype(jnp.bfloat16)


def in_order(half, own, other):
    return jnp.where(half == 0, jnp.stack([own, other]), jnp.stack([other, own]))


def shards(count, content, query_in, content_cot, query_cot, lengths, order, query_weight,
           query_bias, key_weight, value_weight, value_bias, out_weight, out_bias, mixer_gain,
           mixer_shift, up_weight, up_bias, down_weight, down_bias, final_gain, final_shift,
           position_bias):
    _, block, width = content.shape
    length = order.shape[1]
    half = lax.axis_index("seq")
    me = lax.axis_index("dp")
    rows = query_weight.shape[0]
    hidden = up_weight.shape[1]
    share = hidden // 2
    near_count = count // 2

    ids = jnp.stack([me, half]).astype(jnp.int32)
    vectors = (query_bias, value_bias, out_bias, mixer_gain, mixer_shift, down_bias, final_gain,
               final_shift, up_bias, position_bias)
    sizes = [vector.shape[0] for vector in vectors]
    theirs, square, feed_own, slots = pack(
        ids, content, query_in, content_cot, query_cot, query_weight, key_weight, value_weight,
        out_weight, jnp.transpose(up_weight), down_weight, vectors,
    )

    square_parts = high_parts(square, count)
    came = swap(theirs)
    xs, cs, mask = sort_rows(
        ids, lengths, (content, query_in, content_cot, query_cot), came, order
    )
    slots = after(slots, xs)
    slots_high = jnp.stack([slots] + high_parts(slots, count))
    feed_early = high_part(after(feed_own, came), 2, count)
    square_parts, xs = lax.optimization_barrier((square_parts, xs))
    square_near = low_round(jnp.stack([square] + square_parts), count)
    square_near, slots_high, feed_early = lax.optimization_barrier(
        (square_near, slots_high, feed_early)
    )
    slots_near = low_round(slots_high, count)
    square_far = last_round(square_near, count)
    near_swapped = swap(square_near)
    square_far = after(square_far, slots_near, near_swapped)
    slots_far = last_round(slots_near, count)
    far_swapped = swap(square_far)
    feed_later = after(feed_own, square_near)
    feed_parts = [
        feed_early if high == 2 else high_part(feed_later, high, count)
        for high in range(1, count // 4)
    ]
    feed_parts = lax.optimization_barrier((feed_parts, square_far))[0]
    feed_near = low_round(jnp.stack([feed_own] + feed_parts), count)
    vector_rows, up_biases, bias = vectors_to_all(ids, slots_near, slots_far, width, sizes)
    feed_near = after(feed_near, far_swapped, bias)
    pieces = (square_near, square_far, near_swapped, far_swapped)

    flips = offsets(count, half)
    other_flips = offsets(count, 1 - half)
    chips, other_chips = me ^ flips, me ^ other_flips
    aligned = rows % 16 == 0
    if not aligned:
        ordered = []
        for side, places in ((pieces[:2], chips), (pieces[2:], other_chips)):
            joint = jnp.take(jnp.concatenate(side), jnp.argsort(places), axis=0)
            ordered.append(
                jnp.transpose(joint, (1, 0, 2, 3)).reshape(1, 4 * GROUPS, width, 128)
            )
        pieces = tuple(ordered)

    q, k, v, mixed, lse = attend(ids, lengths, xs, mask, bias, vector_rows, pieces)
    feed_far = last_round(feed_near, count)
    feed_far = after(feed_far, mixed)

    feeds = (feed_near, swap(feed_near), feed_far, swap(feed_far))
    out, act, gup, first, gdown, gres, gbranch, gmixed, sums, up_sums = feed(
        ids, xs, mixed, cs, vector_rows, up_biases, feeds, pieces
    )
    shape = (near_count, 2, share, width)
    far_own, far_other = feed_weights(1, act, gup, first, gdown, shape)

    def by_device(grads):
        if aligned:
            return grads
        result = []
        for grad, places in zip(grads, (chips, other_chips)):
            parts = grad[0].reshape(grad.shape[1], count, rows, 128)
            parts = jnp.take(jnp.transpose(parts, (1, 0, 2, 3)), places, axis=0)
            result += [parts[:near_count], parts[near_count:]]
        return result

    def swapped_sum(own, other):
        return wide(own) + wide(swap(other))

    def halved(total):
        return total.reshape((2, total.shape[0] // 2) + total.shape[1:])

    def high_parts_of(total, count):
        return [
            lax.ppermute(low(total[high]), BOTH, xor_pairs(count, (4 * high, 4 * high)))
            for high in range(1, count // 4)
        ]

    def own_sum(total, parts):
        total = total[0]
        for part in parts:
            total = total + wide(part)
        return total

    gwo = out_weights(ids, after(mixed, far_own), gbranch, pieces)
    far_came, _ = lax.optimization_barrier((swap(far_other), gwo[0]))
    cut = near_count // 2 + max(1, near_count // 8)
    far_first = low(wide(far_own[:cut]) + wide(far_came[:cut]))
    gmixed, far_first = lax.optimization_barrier((gmixed, far_first))
    far_first = last_round(far_first, count)
    heads = functools.partial(
        attend_back, ids=ids, lengths=lengths, order=order, xs=xs, mask=mask, bias=bias, q=q, k=k,
        v=v, mixed=mixed, lse=lse, up_sums=up_sums, pieces=pieces, rows_each=rows,
    )
    gx, head_sums, *gws = heads(0, 1, gmixed=gmixed, sums=sums, gres=gres, grads=gwo)
    far_own, far_came, gx = lax.optimization_barrier((far_own, far_came, gx))
    far_second = low(wide(far_own[cut:]) + wide(far_came[cut:]))
    gdown, far_first, far_second, gx = lax.optimization_barrier(
        (gdown, far_first, far_second, gx)
    )
    far_second = last_round(far_second, count)
    near_own, near_other = feed_weights(0, act, gup, first, gdown, shape)
    far_second, near_own, near_other = lax.optimization_barrier(
        (far_second, near_own, near_other)
    )
    near_came = swap(near_other)
    outs = unsort_rows(ids, order, after(out, far_second))
    near_came, near_own, _ = lax.optimization_barrier((near_came, near_own, outs[0]))
    to_send = low(
        wide(halved(near_own)[1]) + wide(halved(near_came)[1])
        + wide(jnp.concatenate([far_first[near_count // 2 :], far_second]))
    )
    gx, to_send = lax.optimization_barrier((gx, to_send))
    gfeed_came = lax.ppermute(to_send, BOTH, xor_pairs(count, (1, 2)))
    gx, head_sums, *gws = result = heads(
        1, 1, gmixed=gmixed, sums=jnp.concatenate([sums, head_sums]), gres=gx, grads=gws
    )
    near_parts = [near_own, near_came, far_first, gfeed_came]
    near_parts, gx = lax.optimization_barrier((near_parts, gx))
    gfeed_low = [
        low(sum(wide(part[high]) for part in near_parts)) for high in range(1, count // 4)
    ]
    gx, gfeed_low = lax.optimization_barrier((gx, gfeed_low))
    early = high_part(gfeed_low[1], 2, count)
    most = by_device(result[2:])
    most_came = [swap(part) for part in most[2:]]
    grad_own, grad_send, *gws = heads(
        2, 1, gmixed=gmixed, sums=jnp.concatenate([sums, head_sums]), gres=gx, grads=()
    )
    early, most_came, gws, near_parts = lax.optimization_barrier(
        (early, most_came, gws, near_parts)
    )
    last = by_device(gws)
    most_far = last_round(low(wide(most[1]) + wide(most_came[1])), count)
    last_came = [swap(part) for part in last[2:]]
    last_far = last_round(low(wide(last[1]) + wide(last_came[1])), count)
    gfeed_parts = [
        early if high == 2 else high_part(gfeed_low[high - 1], high, count)
        for high in range(1, count // 4)
    ]
    outs = place_rows(half, *outs)
    grads = place_rows(half, grad_own, grad_send)
    most_far, last_far, last_came, gfeed_parts = lax.optimization_barrier(
        (most_far, last_far, last_came, gfeed_parts)
    )
    gw = jnp.concatenate([
        wide(most[0]) + wide(most_came[0]) + wide(most_far),
        wide(last[0]) + wide(last_came[0]) + wide(last_far),
    ], axis=1)
    gw_came = lax.ppermute(low(halved(gw)[1]), BOTH, xor_pairs(count, (1, 2)))
    gw = halved(gw)[0] + wide(gw_came)
    gw_parts = high_parts_of(gw, count)
    gfeed = sum(wide(part[0]) for part in near_parts) + sum(wide(part) for part in gfeed_parts)
    gfeed = in_order(half, gfeed, swap(gfeed))
    up_grad = jnp.transpose(gfeed[:, 0].reshape(hidden, width))
    down_grad = gfeed[:, 1].reshape(hidden, width)
    gw = own_sum(gw, gw_parts)
    query_grad, key_grad, value_grad, out_grad, *ends = finish(ids, gw, swap(gw), sizes)
    ends = [end.reshape(-1) for end in ends]
    return (
        outs[0], outs[1], grads[0], grads[1],
        query_grad, ends[0], key_grad, value_grad, ends[1], out_grad, ends[2], ends[3], ends[4],
        up_grad, ends[8], down_grad, ends[5], ends[6], ends[7], ends[9],
    )


def place_rows(half, own, send):
    came = swap(send)
    return [
        jnp.where(half == 0, jnp.stack([own[i], came[i]]), jnp.stack([came[i], own[i]]))
        for i in range(2)
    ]


def solution(mesh):
    rows3 = P("dp", "seq", None)
    flat, first, last = P("dp"), P("dp", None), P(None, "dp")
    in_specs = (
        rows3, rows3, rows3, rows3, first, first, first, flat, first, first, flat, first, flat,
        flat, flat, last, flat, first, flat, flat, flat, flat,
    )
    out_specs = (
        rows3, rows3, rows3, rows3, first, flat, first, first, flat, first, flat, flat, flat,
        last, flat, first, flat, flat, flat, flat,
    )
    body = functools.partial(shards, mesh.shape["dp"])
    return jax.shard_map(
        body, mesh=mesh, in_specs=in_specs, out_specs=out_specs, check_vma=False
    )
```

```python
import functools
import math

import jax
import jax.numpy as jnp
from jax import lax
from jax.experimental import pallas as pl
from jax.experimental.pallas import tpu as pltpu
from jax.sharding import PartitionSpec as P

HEADS = 12
HEAD_DIM = 64
BUCKETS = 32
GROUP = 4
LANES = GROUP * HEAD_DIM
GROUPS = HEADS // GROUP
TILE = 128
TILES = 4
NEG = -1e30
FLOOR = -1e29
EPS = 1e-05

limits = (1, 2, 3, 4, 5, 6, 7, 8, 12, 16, 23, 32, 46, 64, 91)

NN = (((1,), (0,)), ((), ()))
NT = (((1,), (1,)), ((), ()))
TN = (((0,), (0,)), ((), ()))
VMEM_SPEC = pl.BlockSpec(memory_space=pltpu.VMEM)
ANY_SPEC = pl.BlockSpec(memory_space=pl.ANY)
HBM_SPEC = pl.BlockSpec(memory_space=pltpu.HBM)
SCALE = 1.6e6
SMEM_SPEC = pl.BlockSpec(memory_space=pltpu.SMEM)
SDS = jax.ShapeDtypeStruct


def cost(micros):
    return pl.CostEstimate(
        flops=0, bytes_accessed=int(micros * SCALE), transcendentals=0
    )


def product(left, right, dims=NN):
    return lax.dot_general(left, right, dims, preferred_element_type=jnp.float32)


def params(semantics=None, limit=56):
    return pltpu.CompilerParams(dimension_semantics=semantics, vmem_limit_bytes=limit << 20)


def row_sum(values):
    return jnp.sum(values, axis=-1, keepdims=True)


ME, HALF = 0, 1
VECTORS, UP_SLOT, TABLE_SLOT = 10, 8, 9
FIRST_TILES, LAST_TILES = 3 * GROUPS, 4
FULL = 60


def in_hbm(*values):
    return [pltpu.with_memory_space_constraint(value, pltpu.HBM) for value in values]


def run_copies(copies):
    for copy in copies:
        copy.start()
    for copy in copies:
        copy.wait()


def pack_kernel(ids, content, query, ccot, qcot, wq, wk, wv, wo, up, down, *rest):
    vectors, rest = rest[:VECTORS], rest[VECTORS:]
    (theirs, square, feed, slots, tokens, squares, feeds, in_sems, out_sems) = rest
    half = ids[HALF]
    share = feed.shape[1]
    loads = []

    def load(source, target):
        copy = pltpu.make_async_copy(source, target, in_sems.at[len(loads)])
        copy.start()
        loads.append(copy)

    for index, weight in enumerate((wq, wk, wv, wo)):
        for group in range(GROUPS):
            lane = pl.multiple_of(group * LANES + half * 128, 128)
            place = 3 * group + index if index < 3 else 3 * GROUPS + group
            load(weight.at[:, pl.ds(lane, 128)], squares.at[place])
    for index, source in enumerate((content, query, ccot, qcot)):
        load(source.at[1 - half], tokens.at[index])
    rows = pl.ds(pl.multiple_of(half * share, share), share)
    load(up.at[rows, :], feeds.at[0])
    load(down.at[rows, :], feeds.at[1])
    slots[...] = jnp.zeros_like(slots)
    for index, vector in enumerate(vectors):
        slots[index : index + 1, : vector.shape[1]] = vector[...]
    for copy in loads[: 4 * GROUPS]:
        copy.wait()
    stores = [
        pltpu.make_async_copy(squares, square, out_sems.at[0]),
        pltpu.make_async_copy(tokens, theirs, out_sems.at[1]),
        pltpu.make_async_copy(feeds, feed, out_sems.at[2]),
    ]
    stores[0].start()
    for copy in loads[4 * GROUPS :]:
        copy.wait()
    stores[1].start()
    stores[2].start()
    for copy in stores:
        copy.wait()


def pack(ids, content, query, ccot, qcot, wq, wk, wv, wo, up, down, vectors):
    _, block, width = content.shape
    rows = wq.shape[0]
    hidden = up.shape[0]
    return pl.pallas_call(
        pack_kernel,
        out_shape=(
            SDS((4, block, width), jnp.bfloat16),
            SDS((4 * GROUPS, rows, 128), jnp.bfloat16),
            SDS((2, hidden // 2, width), jnp.bfloat16),
            SDS((16, 256), jnp.bfloat16),
        ),
        in_specs=[SMEM_SPEC] + [HBM_SPEC] * 10 + [VMEM_SPEC] * VECTORS,
        out_specs=(HBM_SPEC,) * 3 + (VMEM_SPEC,),
        scratch_shapes=[
            pltpu.VMEM((4, block, width), jnp.bfloat16),
            pltpu.VMEM((4 * GROUPS, rows, 128), jnp.bfloat16),
            pltpu.VMEM((2, hidden // 2, width), jnp.bfloat16),
            pltpu.SemaphoreType.DMA((4 * GROUPS + 6,)),
            pltpu.SemaphoreType.DMA((3,)),
        ],
        cost_estimate=cost(4),
        compiler_params=params(None, FULL),
        name="pack",
    )(ids, *in_hbm(content, query, ccot, qcot, wq, wk, wv, wo, up, down),
      *(vector.reshape(1, -1) for vector in vectors))


def order_onehot(ids, order):
    length = order.shape[1]
    row = order[pl.ds(ids[HALF], 1), :]
    down = lax.broadcasted_iota(jnp.int32, (length, length), 0)
    return jnp.where(row == down, 1.0, 0.0).astype(jnp.bfloat16)


def sort_kernel(ids, lengths, content, query, ccot, qcot, came, order,
                xs_out, cs_out, mask_out, held, sems):
    length = order.shape[1]
    block = content.shape[1]
    half = ids[HALF]
    copies = []
    for index, source in enumerate((content, query, ccot, qcot)):
        for place, rows in ((half, source.at[half]), (1 - half, came.at[index])):
            here = pl.ds(pl.multiple_of(place * block, block), block)
            copies.append(
                pltpu.make_async_copy(rows, held.at[index, here], sems.at[len(copies)])
            )
    for copy in copies:
        copy.start()
    onehot = order_onehot(ids, order)
    lane = lax.broadcasted_iota(jnp.int32, (8, length), 1)
    line = lax.broadcasted_iota(jnp.int32, (8, length), 0)
    digits = jnp.where(line == 0, lane // 16, jnp.where(line == 1, lane % 16, 0))
    digits = product(digits.astype(jnp.float32).astype(jnp.bfloat16), onehot, NT)
    rank_row = digits[0:1, :] * 16.0 + digits[1:2, :]
    across = lax.broadcasted_iota(jnp.int32, (length, length), 1).astype(jnp.float32)
    rank_col = row_sum(onehot.astype(jnp.float32) * across)
    place_col = lax.broadcasted_iota(jnp.int32, (length, 1), 0)
    place_row = lax.broadcasted_iota(jnp.int32, (1, length), 1)
    segment_col = jnp.zeros((length, 1), jnp.int32)
    segment_row = jnp.zeros((1, length), jnp.int32)
    bound = jnp.int32(0)
    for index in range(lengths.shape[1] - 1):
        bound = bound + lengths[half, index]
        segment_col = segment_col + (place_col >= bound).astype(jnp.int32)
        segment_row = segment_row + (place_row >= bound).astype(jnp.int32)
    same = segment_col == segment_row
    mask_out[0] = jnp.where(same & (rank_row <= rank_col), 0.0, NEG).astype(jnp.bfloat16)
    mask_out[1] = jnp.where(same & (rank_row < rank_col), 0.0, NEG).astype(jnp.bfloat16)
    for copy in copies:
        copy.wait()
    for source, target, at in ((0, xs_out, 0), (1, xs_out, 1), (2, cs_out, 0), (3, cs_out, 1)):
        target[at * length : (at + 1) * length, :] = product(onehot, held[source]).astype(
            jnp.bfloat16
        )


def sort_rows(ids, lengths, tokens, came, order):
    length = order.shape[1]
    width = came.shape[2]
    return pl.pallas_call(
        sort_kernel,
        out_shape=(
            SDS((2 * length, width), jnp.bfloat16),
            SDS((2 * length, width), jnp.bfloat16),
            SDS((2, length, length), jnp.bfloat16),
        ),
        in_specs=[SMEM_SPEC] * 2 + [HBM_SPEC] * 5 + [VMEM_SPEC],
        out_specs=(VMEM_SPEC,) * 3,
        scratch_shapes=[
            pltpu.VMEM((4, length, width), jnp.bfloat16),
            pltpu.SemaphoreType.DMA((8,)),
        ],
        cost_estimate=cost(5),
        compiler_params=params(None, FULL),
        name="sort_rows",
    )(ids, lengths, *in_hbm(*tokens, came), order)


def put_back(ids, onehot, source, scratch, own, send, sems):
    length = onehot.shape[0]
    block = own.shape[1]
    for stream in range(2):
        rows = product(onehot, source(stream), TN).astype(jnp.bfloat16)
        scratch[0, stream] = rows[:block, :]
        scratch[1, stream] = rows[block:, :]
    return [
        pltpu.make_async_copy(scratch.at[ids[HALF]], own, sems.at[0]),
        pltpu.make_async_copy(scratch.at[1 - ids[HALF]], send, sems.at[1]),
    ]


def unsort_kernel(ids, order, values, own, send, held, scratch, sems):
    length = order.shape[1]
    copy = pltpu.make_async_copy(values, held, sems.at[2])
    copy.start()
    onehot = order_onehot(ids, order)
    copy.wait()
    run_copies(put_back(
        ids, onehot, lambda s: held[s * length : (s + 1) * length, :], scratch, own, send, sems
    ))


def unsort_rows(ids, order, values):
    length = order.shape[1]
    width = values.shape[1]
    shape = SDS((2, length // 2, width), jnp.bfloat16)
    return pl.pallas_call(
        unsort_kernel,
        out_shape=(shape, shape),
        in_specs=[SMEM_SPEC, VMEM_SPEC, HBM_SPEC],
        out_specs=(HBM_SPEC, HBM_SPEC),
        scratch_shapes=[
            pltpu.VMEM((2 * length, width), jnp.bfloat16),
            pltpu.VMEM((2, 2, length // 2, width), jnp.bfloat16),
            pltpu.SemaphoreType.DMA((3,)),
        ],
        cost_estimate=cost(3),
        compiler_params=params(None, FULL),
        name="unsort_rows",
    )(ids, order, *in_hbm(values))


SPAN = 5 * TILE
TURN = 6 * TILE


def bucket_onehot():
    distance = lax.broadcasted_iota(jnp.int32, (BUCKETS, TURN), 1) - (3 * TILE - 1)
    magnitude = jnp.abs(distance)
    counted = jnp.zeros(distance.shape, jnp.int32)
    for limit in limits:
        counted = counted + (magnitude >= limit).astype(jnp.int32)
    bucket = counted + 16 * (distance > 0).astype(jnp.int32)
    return bucket == lax.broadcasted_iota(jnp.int32, distance.shape, 0)


def block_flip(ids, own, far, block, count):
    place = ids[HALF] if own else 1 - ids[HALF]
    first = jnp.where(place == 0, 1, 2)
    high = count // 2
    flip = jnp.int32(4 * (block % high))
    if block >= high:
        flip = flip ^ first
    return flip ^ (3 - first) if far else flip


def block_places(ids, pieces):
    places = []
    for index, piece in enumerate(pieces):
        own = index < len(pieces) // 2
        place = ids[HALF] if own else 1 - ids[HALF]
        for block in range(piece.shape[0]):
            if len(pieces) == 2:
                places.append((index, block, place, 0))
            else:
                flip = block_flip(ids, own, index % 2 == 1, block, piece.shape[0])
                places.append((index, block, place, ids[ME] ^ flip))
    return places


def block_copies(ids, pieces, target, sems, tiles):
    copies = []
    for index, block, place, chip in block_places(ids, pieces):
        rows = pieces[index].shape[2]
        here = pl.ds(pl.multiple_of(chip * rows, rows), rows)
        copies.append(
            pltpu.make_async_copy(
                pieces[index].at[block, tiles], target.at[place, :, here, :],
                sems.at[len(copies)],
            )
        )
    return copies


def block_stores(ids, source, outs, sems, tiles):
    copies = []
    for index, block, place, chip in block_places(ids, outs):
        rows = outs[index].shape[2]
        here = pl.ds(pl.multiple_of(chip * rows, rows), rows)
        copies.append(
            pltpu.make_async_copy(
                source.at[place, :, here, :], outs[index].at[block, tiles],
                sems.at[len(copies)],
            )
        )
    return copies


def joined(weights, index):
    return jnp.concatenate([weights[0, index], weights[1, index]], axis=1)


def store_shapes(pieces, tiles):
    return tuple(SDS((p.shape[0], tiles) + p.shape[2:], jnp.bfloat16) for p in pieces)


def vectors_kernel(width, sizes, ids, near, far, rows_out, up_out, bias_out):
    count = 2 * near.shape[0]
    half = ids[HALF]
    high = count // 4
    total = jnp.zeros((16, width), jnp.float32)
    table = jnp.zeros((16, width), jnp.float32)
    blank = jnp.zeros((16, width - 256), jnp.float32)
    slot = lax.broadcasted_iota(jnp.int32, (16, width), 0)
    blocks = [[], []]
    for side, part in enumerate((near, far)):
        for block in range(part.shape[0]):
            chip = ids[ME] ^ block_flip(ids, True, side == 1, block, part.shape[0])
            values = jnp.concatenate([part[block].astype(jnp.float32), blank], axis=1)
            blocks[side].append(values)
            total = total + pltpu.roll(
                jnp.where(slot < UP_SLOT, values, 0.0), chip * sizes[0], 1
            )
            table = table + pltpu.roll(
                jnp.where(slot == TABLE_SLOT, values, 0.0), chip * sizes[TABLE_SLOT], 1
            )
    rows_out[...] = total[2:10, :]
    rows_out[6:8, :] = total[0:2, :]
    share = sizes[UP_SLOT] // 2
    lane = lax.broadcasted_iota(jnp.int32, (16, width), 1)
    keep = (slot == UP_SLOT) & (lane < share)
    near_blocks, far_blocks = blocks
    order = (
        (half, near_blocks[:high] + near_blocks[high:]),
        (1 - half, near_blocks[:high] + far_blocks[:high]),
        (half, far_blocks[:high] + far_blocks[high:]),
        (1 - half, near_blocks[high:] + far_blocks[high:]),
    )
    for index, (place, parts) in enumerate(order):
        joint = jnp.zeros((16, width), jnp.float32)
        for block, values in enumerate(parts):
            values = pltpu.roll(values, lax.rem(width - place * share, width), 1)
            joint = joint + pltpu.roll(jnp.where(keep, values, 0.0), block * share, 1)
        up_out[:, index * width : (index + 1) * width] = joint[UP_SLOT : UP_SLOT + 1, :]
    flat = table[TABLE_SLOT : TABLE_SLOT + 1, : BUCKETS * HEADS]
    entry = lax.broadcasted_iota(jnp.int32, (16, BUCKETS * HEADS), 1)
    head = lax.broadcasted_iota(jnp.int32, (16, BUCKETS * HEADS), 0)
    spread_heads = jnp.where(entry % HEADS == head, flat, 0.0).astype(jnp.bfloat16)
    place = lax.broadcasted_iota(jnp.int32, (BUCKETS, BUCKETS * HEADS), 1) // HEADS
    bucket = lax.broadcasted_iota(jnp.int32, (BUCKETS, BUCKETS * HEADS), 0)
    folded = product(spread_heads, jnp.where(place == bucket, 1.0, 0.0).astype(jnp.bfloat16), NT)
    onehot = jnp.where(bucket_onehot(), 1.0, 0.0).astype(jnp.bfloat16)
    rows = product(folded.astype(jnp.bfloat16), onehot)
    for head in range(HEADS):
        spread = jnp.broadcast_to(rows[head : head + 1, :], (TILE, TURN))
        turned = pltpu.roll(spread, TURN - (TILE - 1), 1, stride=1, stride_axis=0)
        bias_out[head] = turned[:, :SPAN].astype(jnp.bfloat16)


def vectors_to_all(ids, near, far, width, sizes):
    return pl.pallas_call(
        functools.partial(vectors_kernel, width, sizes),
        out_shape=(
            SDS((8, width), jnp.float32),
            SDS((1, 4 * width), jnp.float32),
            SDS((HEADS, TILE, SPAN), jnp.bfloat16),
        ),
        in_specs=[SMEM_SPEC] + [VMEM_SPEC] * 2,
        out_specs=(VMEM_SPEC,) * 3,
        cost_estimate=cost(6),
        compiler_params=params(None, FULL),
        name="vectors",
    )(ids, near, far)


def head_lanes(head, shape):
    lane = lax.broadcasted_iota(jnp.int32, shape, 1)
    return (lane >= head * HEAD_DIM) & (lane < (head + 1) * HEAD_DIM)


def head_stack(values):
    low = jnp.zeros((), values.dtype)
    return jnp.concatenate(
        [jnp.where(head_lanes(h, values.shape), values, low) for h in range(GROUP)]
    )


def head_merge(stack, rows):
    total = stack[(GROUP - 1) * rows :, :]
    for h in range(GROUP - 1):
        part = stack[h * rows : (h + 1) * rows, :]
        total = jnp.where(head_lanes(h, part.shape), part, total)
    return total


def widen(values, lanes):
    return jnp.concatenate([values] * (lanes // 128), axis=1)


def by_width(ids, lengths, tile, body):
    half = ids[HALF]
    begin, end = tile * TILE, (tile + 1) * TILE
    bound = jnp.int32(0)
    low, high = jnp.int32(0), jnp.int32(TILES * TILE)
    for index in range(lengths.shape[1] - 1):
        bound = bound + lengths[half, index]
        low = jnp.where(bound <= begin, bound, low)
        high = jnp.where(bound >= end, jnp.minimum(bound, high), high)
    first = low // TILE
    width = jnp.maximum((high + TILE - 1) // TILE - first, 2)
    first = pl.multiple_of(jnp.minimum(first, TILES - width) * TILE, TILE)
    for count in range(2, TILES + 1):
        pl.when(width == count)(functools.partial(body, first, count * TILE))


def attend_kernel(ids, lengths, xs, mask, bias, rows, *rest):
    pieces, rest = rest[:-8], rest[-8:]
    q_out, k_out, v_out, mixed_out, lse_out, weights, values, sems = rest
    length = mask.shape[1]
    group = pl.program_id(0)

    def weight_copies(index):
        tiles = pl.ds(3 * index, 3)
        return block_copies(ids, pieces, weights.at[:, tiles], sems.at[index], tiles)

    @pl.when(group == 0)
    def _():
        for index in range(GROUPS):
            for copy in weight_copies(index):
                copy.start()

    for index in range(GROUPS):
        @pl.when(group == index)
        def _():
            for copy in weight_copies(index):
                copy.wait()

    q = product(xs[...], joined(weights, 3 * group)) + rows[6:7, :]
    q_out[...] = q.astype(jnp.bfloat16)
    k = product(xs[0:length, :], joined(weights, 3 * group + 1))
    k_out[...] = k.astype(jnp.bfloat16)
    v = product(xs[0:length, :], joined(weights, 3 * group + 2)) + rows[7:8, :]
    v_out[...] = v.astype(jnp.bfloat16)

    wide_lanes = lax.broadcasted_iota(jnp.int32, v.shape, 1) < 128
    one = jnp.ones((), jnp.bfloat16)
    values[0] = jnp.where(wide_lanes, v_out[...], one)
    values[1] = jnp.where(wide_lanes, one, v_out[...])

    def tile_step(tile, carry):
        def body(first, keys):
            there = pl.ds(first, keys)
            near = pl.ds(pl.multiple_of((2 - tile) * TILE + first, TILE), keys)
            here = pl.ds(pl.multiple_of(tile * TILE, TILE), TILE)
            key = k_out[there, :]
            for stream in range(2):
                at = pl.ds(pl.multiple_of(stream * length + tile * TILE, TILE), TILE)
                scores = product(head_stack(q_out[at, :] * jnp.bfloat16(0.125)), key, NT)
                masked = mask[stream, here, there].astype(jnp.float32)
                weights, peaks, logs = [], [], []
                for h in range(GROUP):
                    part = scores[h * TILE : (h + 1) * TILE, :] + bias[h, :, near].astype(jnp.float32) + masked
                    peak = jnp.maximum(jnp.max(part, axis=-1, keepdims=True), FLOOR)
                    weights.append(jnp.exp(part - peak).astype(jnp.bfloat16))
                    peaks.append(peak)
                for pair in range(2):
                    both = jnp.concatenate(weights[2 * pair : 2 * pair + 2])
                    both = product(both, values[pair, there, :])
                    top = slice(pair * 128, pair * 128 + 128)
                    low = slice(128 - pair * 128, 256 - pair * 128)
                    parts = []
                    for h in range(2):
                        rows = slice(h * TILE, (h + 1) * TILE)
                        summed = both[rows, low]
                        alive = summed > 0
                        inverse = jnp.where(alive, 1.0 / summed, 0.0)
                        parts.append(both[rows, top] * inverse)
                        logs.append(
                            jnp.where(alive, peaks[2 * pair + h] + jnp.log(summed), 0.0)
                        )
                    lane = lax.broadcasted_iota(jnp.int32, parts[0].shape, 1)
                    mixed = jnp.where(lane < HEAD_DIM, parts[0], parts[1])
                    mixed_out[at, top] = mixed.astype(jnp.bfloat16)
                packed = logs[0]
                for h in range(1, GROUP):
                    packed = jnp.where(lane == h, logs[h], packed)
                lse_out[0, at, :] = packed

        by_width(ids, lengths, tile, body)
        return carry

    lax.fori_loop(0, length // TILE, tile_step, 0)


def attend(ids, lengths, xs, mask, bias, rows, pieces):
    tokens, width = xs.shape
    length = mask.shape[1]
    blocks = sum(piece.shape[0] for piece in pieces)
    full = lambda g: (0, 0)
    column = lambda g: (0, g)
    once = pl.Buffered(1)
    return pl.pallas_call(
        attend_kernel,
        grid=(GROUPS,),
        out_shape=(
            SDS((tokens, width), jnp.bfloat16),
            SDS((length, width), jnp.bfloat16),
            SDS((length, width), jnp.bfloat16),
            SDS((tokens, width), jnp.bfloat16),
            SDS((GROUPS, tokens, 128), jnp.float32),
        ),
        in_specs=[
            SMEM_SPEC,
            SMEM_SPEC,
            pl.BlockSpec((tokens, width), full, pipeline_mode=once),
            pl.BlockSpec((2, length, length), lambda g: (0, 0, 0), pipeline_mode=once),
            pl.BlockSpec((GROUP, TILE, SPAN), lambda g: (g, 0, 0)),
            pl.BlockSpec((8, LANES), column),
        ] + [HBM_SPEC] * len(pieces),
        out_specs=(
            pl.BlockSpec((tokens, LANES), column),
            pl.BlockSpec((length, LANES), column),
            pl.BlockSpec((length, LANES), column),
            pl.BlockSpec((tokens, LANES), column),
            pl.BlockSpec((1, tokens, 128), lambda g: (g, 0, 0)),
        ),
        scratch_shapes=[
            pltpu.VMEM((2, 3 * GROUPS, width, 128), jnp.bfloat16),
            pltpu.VMEM((2, length, LANES), jnp.bfloat16),
            pltpu.SemaphoreType.DMA((GROUPS, blocks)),
        ],
        cost_estimate=cost(18),
        compiler_params=params(("arbitrary",), FULL),
        name="attend",
    )(ids, lengths, xs, mask, bias, rows, *in_hbm(*pieces))


def norm_parts(values):
    mean = jnp.mean(values, axis=-1, keepdims=True)
    center = values - mean
    spread = jnp.mean(center * center, axis=-1, keepdims=True)
    scale = lax.rsqrt(spread + EPS)
    return center * scale, scale


def norm_back(normal, scale, grad):
    mean = jnp.mean(grad, axis=-1, keepdims=True)
    inner = jnp.mean(grad * normal, axis=-1, keepdims=True)
    return scale * (grad - mean - normal * inner)


def column_sum(values):
    return jnp.sum(values, axis=0, keepdims=True)


BLOCK = 256


def feed_kernel(ids, xs, mixed, cot, rows, up_bias, *rest):
    feeds, rest = rest[:8], rest[8:]
    pieces, rest = rest[:-14], rest[-14:]
    (out, act_out, gup_out, first_out, gdown_out, gres_out, gbranch_out, gmixed_out,
     sums, up_sums, up_all, down_all, wo_all, sems) = rest
    step = pl.program_id(0)
    units = up_all.shape[0] // 4
    parts = [feeds[index : index + 2] for index in range(0, 8, 2)]
    held = sum(piece.shape[0] for piece in pieces)

    def weight_copies():
        copies = []
        share = feeds[0].shape[2]
        for index, pair in enumerate(parts):
            blocks = [(part, block) for part in pair for block in range(part.shape[0])]
            for at, (part, block) in enumerate(blocks):
                here = slice(index * units + at * share, index * units + (at + 1) * share)
                for which, target in ((0, up_all), (1, down_all)):
                    copies.append(
                        pltpu.make_async_copy(
                            part.at[block, which], target.at[here, :],
                            sems.at[held + len(copies)],
                        )
                    )
        return copies

    @pl.when(step == 0)
    def _():
        sums[...] = jnp.zeros_like(sums)
        up_sums[...] = jnp.zeros_like(up_sums)
        copies = block_copies(ids, pieces, wo_all, sems, slice(3 * GROUPS, 4 * GROUPS))
        copies += weight_copies()
        run_copies(copies)

    wo = jnp.concatenate([joined(wo_all, index) for index in range(GROUPS)], axis=1)
    branch = product(mixed[...], wo) + rows[0:1, :]

    normal1, scale1 = norm_parts(xs[...].astype(jnp.float32) + branch)
    first = normal1 * rows[1:2, :] + rows[2:3, :]
    first_low = first.astype(jnp.bfloat16)
    first_out[...] = first_low
    slopes = []
    second = first + rows[3:4, :]
    for index in range(2):
        here = slice(2 * index * units, 2 * (index + 1) * units)
        up = product(first_low, up_all[here, :], NT) + up_bias[:, here]
        gate = 0.5 + 0.5 * lax.erf(up * math.sqrt(0.5))
        act = (up * gate).astype(jnp.bfloat16)
        act_out[:, here] = act
        slopes.append(gate + up * jnp.exp(-0.5 * up * up) * (1.0 / math.sqrt(2.0 * math.pi)))
        second = second + product(act, down_all[here, :])
    normal2, scale2 = norm_parts(second)
    gain = rows[4:5, :]
    out[...] = (normal2 * gain + rows[5:6, :]).astype(jnp.bfloat16)
    cots = cot[...].astype(jnp.float32)
    gsecond = norm_back(normal2, scale2, cots * gain)
    gdown = gsecond.astype(jnp.bfloat16)
    gdown_out[...] = gdown
    gfirst = gsecond
    for index in range(2):
        here = slice(2 * index * units, 2 * (index + 1) * units)
        gup = (product(gdown, down_all[here, :], NT) * slopes[index]).astype(jnp.bfloat16)
        gup_out[:, here] = gup
        up_sums[:, here] += column_sum(gup.astype(jnp.float32))
        gfirst = gfirst + product(gup, up_all[here, :])
    gres = norm_back(normal1, scale1, gfirst * rows[1:2, :])
    gres_out[...] = gres
    gbranch = gres.astype(jnp.bfloat16)
    gbranch_out[...] = gbranch
    gmixed_out[...] = product(gbranch, wo, NT).astype(jnp.bfloat16)
    sums[0:1, :] += column_sum(gbranch.astype(jnp.float32))
    sums[1:2, :] += column_sum(gfirst * normal1)
    sums[2:3, :] += column_sum(gfirst)
    sums[3:4, :] += column_sum(gdown.astype(jnp.float32))
    sums[4:5, :] += column_sum(cots * normal2)
    sums[5:6, :] += column_sum(cots)


def feed(ids, xs, mixed, cot, rows, up_bias, feeds, pieces):
    tokens, width = xs.shape
    hidden = up_bias.shape[1]
    token = pl.BlockSpec((BLOCK, width), lambda i: (i, 0))
    wide = pl.BlockSpec((BLOCK, hidden), lambda i: (i, 0))
    held = sum(piece.shape[0] for piece in pieces) + 2 * sum(part.shape[0] for part in feeds)
    low = SDS((tokens, width), jnp.bfloat16)
    return pl.pallas_call(
        feed_kernel,
        grid=(tokens // BLOCK,),
        out_shape=(
            low,
            SDS((tokens, hidden), jnp.bfloat16),
            SDS((tokens, hidden), jnp.bfloat16),
            low,
            low,
            SDS((tokens, width), jnp.float32),
            low,
            low,
            SDS((8, width), jnp.float32),
            SDS((1, hidden), jnp.float32),
        ),
        in_specs=[
            SMEM_SPEC, token, token, token,
            pl.BlockSpec((8, width), lambda i: (0, 0)),
            pl.BlockSpec((1, hidden), lambda i: (0, 0)),
        ] + [ANY_SPEC] * len(feeds) + [HBM_SPEC] * len(pieces),
        out_specs=(token, wide, wide, token, token, token, token, token,
                   pl.BlockSpec((8, width), lambda i: (0, 0)),
                   pl.BlockSpec((1, hidden), lambda i: (0, 0))),
        scratch_shapes=[
            pltpu.VMEM((hidden, width), jnp.bfloat16),
            pltpu.VMEM((hidden, width), jnp.bfloat16),
            pltpu.VMEM((2, GROUPS, width, 128), jnp.bfloat16),
            pltpu.SemaphoreType.DMA((held,)),
        ],
        cost_estimate=cost(36),
        compiler_params=params(("arbitrary",), FULL),
        name="feed",
    )(ids, xs, mixed, cot, rows, up_bias, *feeds, *in_hbm(*pieces))


def feed_weights_kernel(part, act, gup, first, gdown, own, other, left, right, grads, in_sems,
                        out_sems):
    tokens, units = left.shape[1:]
    share = own.shape[2]
    loads, uses = [], []

    def load(source, target):
        copy = pltpu.make_async_copy(source, target, in_sems.at[len(loads)])
        copy.start()
        loads.append(copy)

    for side in range(2):
        lanes = slice((2 * part + 1 - side) * units, (2 * part + 2 - side) * units)
        for which, (source, other_side) in enumerate(((gup, first), (act, gdown))):
            load(source.at[:, lanes], left.at[2 * side + which])
            if side == 0:
                load(other_side, right.at[which])
            uses.append(len(loads))
    stores = []
    done = 0
    for index in range(4):
        for copy in loads[done : uses[index]]:
            copy.wait()
        done = uses[index]
        which = index % 2
        grad = product(left[index], right[which], TN).astype(jnp.bfloat16)
        for block in range(own.shape[0]):
            grads[index, block] = grad[block * share : (block + 1) * share, :]
        out = other if index < 2 else own
        stores.append(
            pltpu.make_async_copy(grads.at[index], out.at[:, which], out_sems.at[index])
        )
        stores[-1].start()
    for copy in stores:
        copy.wait()


def feed_weights(part, act, gup, first, gdown, shape):
    tokens, width = first.shape
    units = shape[0] * shape[2]
    return pl.pallas_call(
        functools.partial(feed_weights_kernel, part),
        out_shape=(SDS(shape, jnp.bfloat16),) * 2,
        in_specs=[HBM_SPEC] * 4,
        out_specs=(HBM_SPEC,) * 2,
        scratch_shapes=[
            pltpu.VMEM((4, tokens, units), jnp.bfloat16),
            pltpu.VMEM((2, tokens, width), jnp.bfloat16),
            pltpu.VMEM((4, shape[0], shape[2], width), jnp.bfloat16),
            pltpu.SemaphoreType.DMA((6,)),
            pltpu.SemaphoreType.DMA((4,)),
        ],
        cost_estimate=cost(9),
        compiler_params=params(None, FULL),
        name="feed_weights",
    )(*in_hbm(act, gup, first, gdown))


def out_weights_kernel(ids, mixed, gbranch, *rest):
    outs, (buffer, sems) = rest[:-2], rest[-2:]
    grad = product(mixed[...], gbranch[...], TN).astype(jnp.bfloat16)
    for index in range(GROUPS):
        for half in range(2):
            lane = index * LANES + half * 128
            buffer[half, index] = grad[:, lane : lane + 128]
    run_copies(block_stores(ids, buffer, outs, sems, slice(2 * GROUPS, 3 * GROUPS)))


def out_weights(ids, mixed, gbranch, pieces):
    tokens, width = mixed.shape
    blocks = sum(piece.shape[0] for piece in pieces)
    full = pl.BlockSpec((tokens, width), lambda i: (0, 0))
    return pl.pallas_call(
        out_weights_kernel,
        grid=(1,),
        out_shape=store_shapes(pieces, FIRST_TILES),
        in_specs=[SMEM_SPEC, full, full],
        out_specs=(HBM_SPEC,) * len(pieces),
        scratch_shapes=[
            pltpu.VMEM((2, GROUPS, width, 128), jnp.bfloat16),
            pltpu.SemaphoreType.DMA((blocks,)),
        ],
        cost_estimate=cost(4),
        compiler_params=params(("arbitrary",), FULL),
        name="out_weights",
    )(ids, mixed, gbranch)


def attend_back_kernel(ids_rows, base, steps, ids, lengths, order, mask, bias, q, k, v, mixed, gmixed, lse, sums,
                       up_sums, xs_far, gres, *rest):
    scratch = rest[-17:]
    done = base + steps == GROUPS
    count = (len(rest) - 17 - 2) // (2 if done else 3)
    pieces = rest[:count]
    if done:
        own, send, *gw_outs = rest[count:-17]
    else:
        gx_out, vectors_out, *gw_outs = rest[2 * count : -17]
    (vectors, turned, vector_sems, gk, gv, gdist, gx, gq, inner, weights, buffer, xs, rows_out, sems, in_sems, out_sems,
     row_sems) = scratch
    step = pl.program_id(0)
    group = base + step
    tiles = slice(3 * base, 3 * (base + steps))
    length = mask.shape[1]
    rows = xs.shape[1] // (2 * gw_outs[0].shape[0]) if count > 2 else ids_rows
    loads = block_copies(ids, pieces, weights, sems, tiles) + [
        pltpu.make_async_copy(xs_far, xs, in_sems.at[0]),
        pltpu.make_async_copy(gres, gx, in_sems.at[1]),
    ]

    def stores(index):
        return block_stores(
            ids, buffer.at[index], gw_outs, out_sems.at[index],
            slice(0, 3) if done else pl.ds(3 * (base + index), 3),
        )

    @pl.when(step == 0)
    def _():
        for copy in loads:
            copy.start()
        if base:
            vectors[0:16, :] = sums[8:24, :]

    gdist[...] = jnp.zeros_like(gdist)
    gk[...] = jnp.zeros_like(gk)
    gv[...] = jnp.zeros_like(gv)

    lane = lax.broadcasted_iota(jnp.int32, (LANES, GROUP * 128), 0) // HEAD_DIM
    head = lax.broadcasted_iota(jnp.int32, (LANES, GROUP * 128), 1) // 128
    adder = jnp.where(lane == head, 1.0, 0.0).astype(jnp.bfloat16)
    crossed = mixed[...].astype(jnp.float32) * gmixed[...].astype(jnp.float32)
    inner[...] = product(crossed.astype(jnp.bfloat16), adder)

    def tile_step(tile, carry):
        def body(first, keys):
            there = pl.ds(first, keys)
            near = pl.ds(pl.multiple_of((2 - tile) * TILE + first, TILE), keys)
            here = pl.ds(pl.multiple_of(tile * TILE, TILE), TILE)
            key = k[there, :]
            value = v[there, :]
            at = [
                pl.ds(pl.multiple_of(stream * length + tile * TILE, TILE), TILE)
                for stream in range(2)
            ]
            query = jnp.concatenate([head_stack(q[at[s], :] * jnp.bfloat16(0.125)) for s in range(2)])
            gmix = jnp.concatenate([head_stack(gmixed[at[s], :]) for s in range(2)])
            scores = product(query, key, NT)
            gprobs = product(gmix, value, NT)
            masked = [mask[s, here, there].astype(jnp.float32) for s in range(2)]
            probs_low = [None] * (2 * GROUP)
            gscores_low = [None] * (2 * GROUP)
            for h in range(GROUP):
                both = None
                near_bias = bias[h, :, near].astype(jnp.float32)
                for stream in range(2):
                    index = stream * GROUP + h
                    part = slice(index * TILE, (index + 1) * TILE)
                    score = scores[part, :] + near_bias + masked[stream]
                    probs = jnp.exp(score - lse[0, at[stream], h : h + 1])
                    lanes = slice(h * 128, (h + 1) * 128)
                    gscores = probs * (gprobs[part, :] - widen(inner[at[stream], lanes], keys))
                    probs_low[index] = probs.astype(jnp.bfloat16)
                    gscores_low[index] = gscores.astype(jnp.bfloat16)
                    both = gscores if both is None else both + gscores
                gdist[h, :, near] += both
            probs_low = jnp.concatenate(probs_low)
            gscores_low = jnp.concatenate(gscores_low)
            gv[there, :] += product(probs_low, gmix, TN)
            gk[there, :] += product(gscores_low, query, TN)
            back = product(gscores_low, key)
            for stream in range(2):
                part = slice(stream * GROUP * TILE, (stream + 1) * GROUP * TILE)
                gq[at[stream], :] = head_merge(back[part, :], TILE)

        by_width(ids, lengths, tile, body)
        return carry

    lax.fori_loop(0, length // TILE, tile_step, 0)
    gq_low = (gq[...] * 0.125).astype(jnp.bfloat16)
    gk_low = gk[...].astype(jnp.bfloat16)
    gv_low = gv[...].astype(jnp.bfloat16)

    @pl.when(step == 0)
    def _():
        for copy in loads:
            copy.wait()

    for index, grad in enumerate((
        product(xs[...], gq_low, TN),
        product(xs[0:length, :], gk_low, TN),
        product(xs[0:length, :], gv_low, TN),
    )):
        grad = grad.astype(jnp.bfloat16)
        buffer[step, 0, index] = grad[:, :128]
        buffer[step, 1, index] = grad[:, 128:]
    for index in range(steps):
        @pl.when(step == index)
        def _():
            for copy in stores(index):
                copy.start()

    gx[...] += product(gq_low, joined(weights, 3 * step), NT)
    gx[0:length, :] += product(gk_low, joined(weights, 3 * step + 1), NT) + product(
        gv_low, joined(weights, 3 * step + 2), NT
    )
    if done:
        sends = put_back(
            ids, order_onehot(ids, order),
            lambda s: gx[s * length : (s + 1) * length, :].astype(jnp.bfloat16),
            rows_out, own, send, row_sems,
        )
    else:
        sends = [pltpu.make_async_copy(gx, gx_out, in_sems.at[0])]
    for copy in sends:
        copy.start()
    lanes = pl.ds(pl.multiple_of(group * LANES, LANES), LANES)
    vectors[0:1, lanes] = column_sum(gq_low.astype(jnp.float32))
    vectors[1:2, lanes] = column_sum(gv_low.astype(jnp.float32))
    span = TURN
    pieces_sum = []
    row_index = lax.broadcasted_iota(jnp.int32, (8, span), 0)
    for h in range(GROUP):
        wide = jnp.concatenate([gdist[h], jnp.zeros((TILE, TILE), jnp.float32)], axis=1)
        size = TILE // 2
        while size >= 8:
            wide = wide[size:, :] + pltpu.roll(wide[:size, :], size, 1)
            size //= 2
        for bit in (4, 2, 1):
            wide = jnp.where(row_index & bit == 0, pltpu.roll(wide, bit, 1), wide)
        pieces_sum.append(column_sum(wide))
    pieces_sum.append(jnp.zeros((8 - GROUP, span), jnp.float32))
    onehot = jnp.where(bucket_onehot(), 1.0, 0.0)
    by_bucket = lax.dot_general(
        jnp.concatenate(pieces_sum, axis=0), onehot, NT, precision=lax.Precision.HIGHEST,
        preferred_element_type=jnp.float32,
    )
    width = xs.shape[1]
    parts = width // rows
    each = BUCKETS * HEADS // parts
    lane = lax.broadcasted_iota(jnp.int32, (BUCKETS, width), 1)
    entry = lane // rows * each + lane % rows
    bucket = lax.broadcasted_iota(jnp.int32, (BUCKETS, width), 0)
    chosen = (entry // HEADS == bucket) & (lane % rows < each)
    table = lax.dot_general(
        by_bucket, jnp.where(chosen, 1.0, 0.0), NN, precision=lax.Precision.HIGHEST,
        preferred_element_type=jnp.float32,
    )
    head = lax.broadcasted_iota(jnp.int32, table.shape, 0)
    lane = lax.broadcasted_iota(jnp.int32, table.shape, 1)
    entry = lane // rows * each + lane % rows
    right = (head < GROUP) & (entry % HEADS == GROUP * group + head)
    table = column_sum(jnp.where(right, table, 0.0))

    if base:
        vectors[12:13, :] += table
    else:
        vectors[12:13, :] = table

    if not done:
        for copy in stores(0):
            copy.wait()
        vectors_out[...] = vectors[0:16, :]
        for copy in sends:
            copy.wait()
        return

    vectors[2:8, :] = sums[0:6, :]
    vectors[8:12, :] = up_slots(ids, up_sums, rows, parts // 2)
    vectors[13:, :] = jnp.zeros((128 - 13, width), jnp.float32)
    tile = jnp.transpose(vectors[...]).astype(jnp.bfloat16)
    turned[0, 0] = tile
    turned[1, 0] = tile
    last = block_stores(ids, turned, gw_outs, vector_sems, slice(3, LAST_TILES))
    for copy in last:
        copy.start()
    for copy in stores(0) + last + sends:
        copy.wait()


def up_slots(ids, up_sums, rows, blocks):
    width = up_sums.shape[1] // 4
    share = 2 * rows
    slot = lax.broadcasted_iota(jnp.int32, (8, width), 0)
    lane = lax.broadcasted_iota(jnp.int32, (8, width), 1)
    total = jnp.zeros((8, width), jnp.float32)
    for index in range(4):
        own = index % 2 == 0
        place = ids[HALF] if own else 1 - ids[HALF]
        part = jnp.broadcast_to(up_sums[:, index * width : (index + 1) * width], (8, width))
        for block in range(blocks):
            chip = ids[ME] ^ block_flip(ids, own, index >= 2, block, blocks)
            for quarter in range(2):
                shift = (width - block * share - quarter * rows) % width
                values = pltpu.roll(part, shift, 1) if shift else part
                keep = (lane < rows) & (slot == 2 * place + quarter)
                total = total + pltpu.roll(jnp.where(keep, values, 0.0), chip * rows, 1)
    return total[0:4, :]


def attend_back(base, steps, ids, lengths, order, xs, mask, bias, q, k, v, mixed, gmixed, lse,
                sums, up_sums, gres, pieces, grads, rows_each):
    tokens, width = xs.shape
    length = mask.shape[1]
    blocks = sum(piece.shape[0] for piece in pieces)
    done = base + steps == GROUPS
    column = lambda g: (0, base + g)
    rows = SDS((2, length // 2, width), jnp.bfloat16)
    first = 15 + len(pieces)
    if done:
        outs, out_specs = (rows, rows), (HBM_SPEC, HBM_SPEC)
    else:
        outs = (SDS((tokens, width), jnp.float32), SDS((16, width), jnp.float32))
        out_specs = (HBM_SPEC, pl.BlockSpec((16, width), lambda g: (0, 0)))
    return pl.pallas_call(
        functools.partial(attend_back_kernel, rows_each, base, steps),
        grid=(steps,),
        out_shape=outs + store_shapes(pieces, LAST_TILES if done else FIRST_TILES),
        input_output_aliases={first + index: 2 + index for index in range(len(grads))},
        in_specs=[
            SMEM_SPEC,
            SMEM_SPEC,
            VMEM_SPEC,
            pl.BlockSpec((2, length, length), lambda g: (0, 0, 0), pipeline_mode=pl.Buffered(1)),
            pl.BlockSpec((GROUP, TILE, SPAN), lambda g: (base + g, 0, 0)),
            pl.BlockSpec((tokens, LANES), column),
            pl.BlockSpec((length, LANES), column),
            pl.BlockSpec((length, LANES), column),
            pl.BlockSpec((tokens, LANES), column),
            pl.BlockSpec((tokens, LANES), column),
            pl.BlockSpec((1, tokens, 128), lambda g: (base + g, 0, 0)),
            pl.BlockSpec(sums.shape, lambda g: (0, 0)),
            pl.BlockSpec((1, 4 * width), lambda g: (0, 0)),
        ] + [HBM_SPEC] * (2 + len(pieces) + len(grads)),
        out_specs=out_specs + (HBM_SPEC,) * len(pieces),
        scratch_shapes=[
            pltpu.VMEM((128, width), jnp.float32),
            pltpu.VMEM((2, 1, width, 128), jnp.bfloat16),
            pltpu.SemaphoreType.DMA((blocks,)),
            pltpu.VMEM((length, LANES), jnp.float32),
            pltpu.VMEM((length, LANES), jnp.float32),
            pltpu.VMEM((GROUP, TILE, SPAN), jnp.float32),
            pltpu.VMEM((tokens, width), jnp.float32),
            pltpu.VMEM((tokens, LANES), jnp.float32),
            pltpu.VMEM((tokens, GROUP * 128), jnp.float32),
            pltpu.VMEM((2, 3 * steps, width, 128), jnp.bfloat16),
            pltpu.VMEM((steps, 2, 3, width, 128), jnp.bfloat16),
            pltpu.VMEM((tokens, width), jnp.bfloat16),
            pltpu.VMEM((2, 2, length // 2, width), jnp.bfloat16),
            pltpu.SemaphoreType.DMA((blocks,)),
            pltpu.SemaphoreType.DMA((2,)),
            pltpu.SemaphoreType.DMA((steps, blocks)),
            pltpu.SemaphoreType.DMA((2,)),
        ],
        cost_estimate=cost(14 * steps),
        compiler_params=params(("arbitrary",), FULL),
        name="attend_back",
    )(ids, lengths, order, mask, bias, q, k, v, mixed, gmixed, lse, sums, up_sums,
      *in_hbm(xs, gres, *pieces, *grads))


def grad_tile(index, group):
    if index == 3:
        return 2 * GROUPS + group
    return index + (3 * group if group < GROUPS - 1 else FIRST_TILES)


def finish_kernel(ids, own, came, wq, wk, wv, wo, *vectors):
    half = ids[HALF]
    for place in range(2):
        mine = half == place
        for index, out in enumerate((wq, wk, wv, wo)):
            for group in range(GROUPS):
                tile = grad_tile(index, group)
                lane = group * LANES + place * 128
                out[:, lane : lane + 128] = jnp.where(mine, own[tile], came[tile])
    turned = jnp.transpose(own[FIRST_TILES + 3])
    rows = own.shape[1]
    for index, out in enumerate(vectors):
        if index == UP_SLOT:
            for quarter in range(4):
                out[:, quarter * rows : (quarter + 1) * rows] = turned[8 + quarter : 9 + quarter, :]
        else:
            at = 12 if index == TABLE_SLOT else index
            out[...] = turned[at : at + 1, : out.shape[1]]


def finish(ids, own, came, sizes):
    rows = own.shape[1]
    width = LANES * GROUPS
    outs = (SDS((rows, width), jnp.float32),) * 4
    outs += tuple(SDS((1, size), jnp.float32) for size in sizes)
    return pl.pallas_call(
        finish_kernel,
        out_shape=outs,
        in_specs=[SMEM_SPEC, VMEM_SPEC, VMEM_SPEC],
        out_specs=(VMEM_SPEC,) * len(outs),
        cost_estimate=cost(2),
        compiler_params=params(None, FULL),
        name="finish",
    )(ids, own, came)


BOTH = ("dp", "seq")


def xor_pairs(count, by_half):
    halves = len(by_half)
    return [
        (device * halves + half, (device ^ flip) * halves + half)
        for device in range(count)
        for half, flip in enumerate(by_half)
    ]


def swap(value):
    return lax.ppermute(value, "seq", [(0, 1), (1, 0)])


def high_part(value, high, count):
    return lax.ppermute(value, BOTH, xor_pairs(count, (4 * high, 4 * high)))


def high_parts(value, count):
    return [high_part(value, high, count) for high in range(1, count // 4)]


def low_round(value, count):
    return jnp.concatenate([value, lax.ppermute(value, BOTH, xor_pairs(count, (1, 2)))])


def last_round(value, count):
    return lax.ppermute(value, BOTH, xor_pairs(count, (2, 1)))


def offsets(count, half):
    first = jnp.where(half == 0, 1, 2)
    highs = 4 * jnp.arange(count // 4)
    near = jnp.concatenate([highs, highs ^ first])
    return jnp.concatenate([near, near ^ (3 - first)])


def after(value, *others):
    return lax.optimization_barrier((value,) + others)[0]


def wide(value):
    return value.astype(jnp.float32)


def low(value):
    return value.astype(jnp.bfloat16)


def in_order(half, own, other):
    return jnp.where(half == 0, jnp.stack([own, other]), jnp.stack([other, own]))


def shards(count, content, query_in, content_cot, query_cot, lengths, order, query_weight,
           query_bias, key_weight, value_weight, value_bias, out_weight, out_bias, mixer_gain,
           mixer_shift, up_weight, up_bias, down_weight, down_bias, final_gain, final_shift,
           position_bias):
    _, block, width = content.shape
    length = order.shape[1]
    half = lax.axis_index("seq")
    me = lax.axis_index("dp")
    rows = query_weight.shape[0]
    hidden = up_weight.shape[1]
    share = hidden // 2
    near_count = count // 2

    ids = jnp.stack([me, half]).astype(jnp.int32)
    vectors = (query_bias, value_bias, out_bias, mixer_gain, mixer_shift, down_bias, final_gain,
               final_shift, up_bias, position_bias)
    sizes = [vector.shape[0] for vector in vectors]
    theirs, square, feed_own, slots = pack(
        ids, content, query_in, content_cot, query_cot, query_weight, key_weight, value_weight,
        out_weight, jnp.transpose(up_weight), down_weight, vectors,
    )

    square_parts = high_parts(square, count)
    came = swap(theirs)
    xs, cs, mask = sort_rows(
        ids, lengths, (content, query_in, content_cot, query_cot), came, order
    )
    slots = after(slots, xs)
    slots_high = jnp.stack([slots] + high_parts(slots, count))
    feed_early = high_part(after(feed_own, came), 2, count)
    square_parts, xs = lax.optimization_barrier((square_parts, xs))
    square_near = low_round(jnp.stack([square] + square_parts), count)
    square_near, slots_high, feed_early = lax.optimization_barrier(
        (square_near, slots_high, feed_early)
    )
    slots_near = low_round(slots_high, count)
    square_far = last_round(square_near, count)
    near_swapped = swap(square_near)
    square_far = after(square_far, slots_near, near_swapped)
    slots_far = last_round(slots_near, count)
    far_swapped = swap(square_far)
    feed_later = after(feed_own, square_near)
    feed_parts = [
        feed_early if high == 2 else high_part(feed_later, high, count)
        for high in range(1, count // 4)
    ]
    feed_parts = lax.optimization_barrier((feed_parts, square_far))[0]
    feed_high = jnp.stack([feed_own] + feed_parts)
    feed_near = lax.ppermute(feed_high, BOTH, xor_pairs(count, (1, 2)))
    vector_rows, up_biases, bias = vectors_to_all(ids, slots_near, slots_far, width, sizes)
    feed_near, feed_high = lax.optimization_barrier(
        (feed_near, feed_high, far_swapped, bias)
    )[:2]
    feed_near = (feed_high, feed_near)
    pieces = (square_near, square_far, near_swapped, far_swapped)

    flips = offsets(count, half)
    other_flips = offsets(count, 1 - half)
    chips, other_chips = me ^ flips, me ^ other_flips
    aligned = rows % 16 == 0
    if not aligned:
        ordered = []
        for side, places in ((pieces[:2], chips), (pieces[2:], other_chips)):
            joint = jnp.take(jnp.concatenate(side), jnp.argsort(places), axis=0)
            ordered.append(
                jnp.transpose(joint, (1, 0, 2, 3)).reshape(1, 4 * GROUPS, width, 128)
            )
        pieces = tuple(ordered)

    q, k, v, mixed, lse = attend(ids, lengths, xs, mask, bias, vector_rows, pieces)
    feed_far = [last_round(part, count) for part in feed_near]
    feed_far = lax.optimization_barrier((feed_far, mixed))[0]

    feeds = [
        part for pair in (feed_near, map(swap, feed_near), feed_far, map(swap, feed_far))
        for part in pair
    ]
    out, act, gup, first, gdown, gres, gbranch, gmixed, sums, up_sums = feed(
        ids, xs, mixed, cs, vector_rows, up_biases, feeds, pieces
    )
    shape = (near_count, 2, share, width)
    far_own, far_other = feed_weights(1, act, gup, first, gdown, shape)

    def by_device(grads):
        if aligned:
            return grads
        result = []
        for grad, places in zip(grads, (chips, other_chips)):
            parts = grad[0].reshape(grad.shape[1], count, rows, 128)
            parts = jnp.take(jnp.transpose(parts, (1, 0, 2, 3)), places, axis=0)
            result += [parts[:near_count], parts[near_count:]]
        return result

    def swapped_sum(own, other):
        return wide(own) + wide(swap(other))

    def halved(total):
        return total.reshape((2, total.shape[0] // 2) + total.shape[1:])

    def high_parts_of(total, count):
        return [
            lax.ppermute(low(total[high]), BOTH, xor_pairs(count, (4 * high, 4 * high)))
            for high in range(1, count // 4)
        ]

    def own_sum(total, parts):
        total = total[0]
        for part in parts:
            total = total + wide(part)
        return total

    gwo = out_weights(ids, after(mixed, far_own), gbranch, pieces)
    far_came, _ = lax.optimization_barrier((swap(far_other), gwo[0]))
    cut = near_count // 2 + max(1, near_count // 8)
    far_first = low(wide(far_own[:cut]) + wide(far_came[:cut]))
    gmixed, far_first = lax.optimization_barrier((gmixed, far_first))
    far_first = last_round(far_first, count)
    heads = functools.partial(
        attend_back, ids=ids, lengths=lengths, order=order, xs=xs, mask=mask, bias=bias, q=q, k=k,
        v=v, mixed=mixed, lse=lse, up_sums=up_sums, pieces=pieces, rows_each=rows,
    )
    gx, head_sums, *gws = heads(0, 1, gmixed=gmixed, sums=sums, gres=gres, grads=gwo)
    far_own, far_came, gx = lax.optimization_barrier((far_own, far_came, gx))
    far_second = low(wide(far_own[cut:]) + wide(far_came[cut:]))
    gdown, far_first, far_second, gx = lax.optimization_barrier(
        (gdown, far_first, far_second, gx)
    )
    far_second = last_round(far_second, count)
    near_own, near_other = feed_weights(0, act, gup, first, gdown, shape)
    far_second, near_own, near_other = lax.optimization_barrier(
        (far_second, near_own, near_other)
    )
    near_came = swap(near_other)
    outs = unsort_rows(ids, order, after(out, far_second))
    near_came, near_own, _ = lax.optimization_barrier((near_came, near_own, outs[0]))
    to_send = low(
        wide(halved(near_own)[1]) + wide(halved(near_came)[1])
        + wide(jnp.concatenate([far_first[near_count // 2 :], far_second]))
    )
    gx, to_send = lax.optimization_barrier((gx, to_send))
    gfeed_came = lax.ppermute(to_send, BOTH, xor_pairs(count, (1, 2)))
    gx, head_sums, *gws = result = heads(
        1, 1, gmixed=gmixed, sums=jnp.concatenate([sums, head_sums]), gres=gx, grads=gws
    )
    near_parts = [near_own, near_came, far_first, gfeed_came]
    near_parts, gx = lax.optimization_barrier((near_parts, gx))
    gfeed_low = [
        low(sum(wide(part[high]) for part in near_parts)) for high in range(1, count // 4)
    ]
    gx, gfeed_low = lax.optimization_barrier((gx, gfeed_low))
    early = high_part(gfeed_low[1], 2, count)
    most = by_device(result[2:])
    most_came = [swap(part) for part in most[2:]]
    grad_own, grad_send, *gws = heads(
        2, 1, gmixed=gmixed, sums=jnp.concatenate([sums, head_sums]), gres=gx, grads=()
    )
    early, most_came, gws, near_parts = lax.optimization_barrier(
        (early, most_came, gws, near_parts)
    )
    last = by_device(gws)
    most_far = last_round(low(wide(most[1]) + wide(most_came[1])), count)
    last_came = [swap(part) for part in last[2:]]
    last_far = last_round(low(wide(last[1]) + wide(last_came[1])), count)
    gfeed_parts = [
        early if high == 2 else high_part(gfeed_low[high - 1], high, count)
        for high in range(1, count // 4)
    ]
    outs = place_rows(half, *outs)
    grads = place_rows(half, grad_own, grad_send)
    most_far, last_far, last_came, gfeed_parts = lax.optimization_barrier(
        (most_far, last_far, last_came, gfeed_parts)
    )
    gw = jnp.concatenate([
        wide(most[0]) + wide(most_came[0]) + wide(most_far),
        wide(last[0]) + wide(last_came[0]) + wide(last_far),
    ], axis=1)
    gw_came = lax.ppermute(low(halved(gw)[1]), BOTH, xor_pairs(count, (1, 2)))
    gw = halved(gw)[0] + wide(gw_came)
    gw_parts = high_parts_of(gw, count)
    gfeed = sum(wide(part[0]) for part in near_parts) + sum(wide(part) for part in gfeed_parts)
    gfeed = in_order(half, gfeed, swap(gfeed))
    up_grad = jnp.transpose(gfeed[:, 0].reshape(hidden, width))
    down_grad = gfeed[:, 1].reshape(hidden, width)
    gw = own_sum(gw, gw_parts)
    query_grad, key_grad, value_grad, out_grad, *ends = finish(ids, gw, swap(gw), sizes)
    ends = [end.reshape(-1) for end in ends]
    return (
        outs[0], outs[1], grads[0], grads[1],
        query_grad, ends[0], key_grad, value_grad, ends[1], out_grad, ends[2], ends[3], ends[4],
        up_grad, ends[8], down_grad, ends[5], ends[6], ends[7], ends[9],
    )


def place_rows(half, own, send):
    came = swap(send)
    return [
        jnp.where(half == 0, jnp.stack([own[i], came[i]]), jnp.stack([came[i], own[i]]))
        for i in range(2)
    ]


def solution(mesh):
    rows3 = P("dp", "seq", None)
    flat, first, last = P("dp"), P("dp", None), P(None, "dp")
    in_specs = (
        rows3, rows3, rows3, rows3, first, first, first, flat, first, first, flat, first, flat,
        flat, flat, last, flat, first, flat, flat, flat, flat,
    )
    out_specs = (
        rows3, rows3, rows3, rows3, first, flat, first, first, flat, first, flat, flat, flat,
        last, flat, first, flat, flat, flat, flat,
    )
    body = functools.partial(shards, mesh.shape["dp"])
    return jax.shard_map(
        body, mesh=mesh, in_specs=in_specs, out_specs=out_specs, check_vma=False
    )
```
